256 devices in a mesh: tm: 128 (over y, x, z), dp: 2 (over core).
Axes of the slice: x: 4, y: 4, z: 8, core: 2. Of those that a mesh axis runs over, the one named last changes fastest.
Arguments:
- state_feats: bfloat16 [128, 512, 256], P('dp', 'tm'), may hold values from -24 to 24
- achieved: bfloat16 [128, 512, 512], P('dp', 'tm'), may hold values from -24 to 24
- offsets: int32 [128, 512], P('dp', 'tm'), may hold values from 0 to 511, as said below
- w_in: bfloat16 [768, 2048], replicated, may hold values from -0.21875 to 0.21875
- b_in: float32 [2048], replicated, may hold values from -3 to 3
- w_out: float32 [2048], replicated, may hold values from -0.75 to 0.75
- b_out: float32 [1], replicated, may hold values from -1 to 1
Outputs:
- td_error: float32 [128, 512], P('dp', 'tm')
- grad_w_in: float32 [768, 2048], P(('tm', 'dp'))
- grad_b_in: float32 [2048], replicated
- grad_w_out: float32 [2048], replicated
- grad_b_out: float32 [1], replicated
The draws below stay inside these ranges and needn't reach their ends.
Inputs may be any that keep to these rules, and one draw needn't show every extreme that they name: t + offsets[e, t] <= 511. The transitions held by one device (one index of dp and of tm) ask at most 4 of their goals from any other single index of tm; every device whose tm index is below the last asks exactly 4 goals from the last index, all of them at time 512 - 1.
All inputs are finite; a program needn't handle non-finite values.
Results may differ from the reference program's by a relative error of at most 0.0024.
The reference program's roundings to bfloat16 on the way (of `goal`, `inputs`, `hidden` and `grad_low`) count: a program that leaves them out, or rounds other values in their place, can miss the bound.
Values may be sent and summed in bfloat16 or wider, within the bound.
No kernel may reach another device: no remote copies, remote signals or barrier semaphores. Data moves between devices by JAX's collectives and lax.ppermute only.
A program may use at most 64 MiB of HBM per device.

```python
import math
import jax
import jax.numpy as jnp
from jax import lax

S = 256
G = 512
H = 2048
STEPS = 4
EP_DEV = 64
CAP = 4
EP_LEN = 512
EPISODES = 128


def draw_offsets(key, part):
    tm_count = EP_LEN // STEPS
    dp_count = EPISODES // EP_DEV
    rows = EP_DEV * STEPS
    key_far, key_near, key_final = jax.random.split(key, 3)
    shape = (EPISODES, EP_LEN)
    times = jnp.broadcast_to(jnp.arange(EP_LEN, dtype=jnp.int32)[None, :], shape)
    future = times + jax.random.randint(key_far, shape, 0, EP_LEN - times)
    home = times // STEPS
    nearby = times + jax.random.randint(key_near, shape, 0, (home + 1) * STEPS - times)

    def blocks(values):
        return values.reshape(dp_count, EP_DEV, tm_count, STEPS).transpose(0, 2, 1, 3).reshape(dp_count, tm_count, rows)

    def unblock(values):
        return values.reshape(dp_count, tm_count, EP_DEV, STEPS).transpose(0, 2, 1, 3).reshape(EPISODES, EP_LEN)
    owner_rows = blocks(future // STEPS)
    home_rows = blocks(home)
    remote = (owner_rows != home_rows) & (owner_rows != tm_count - 1)
    peers = jnp.arange(tm_count, dtype=jnp.int32)
    hits = ((owner_rows[..., None] == peers) & remote[..., None]).astype(jnp.int32)
    rank = jnp.sum((jnp.cumsum(hits, axis=2) - 1) * hits, axis=3)
    keep = remote & (rank < CAP)
    scores = jax.random.randint(key_final, (dp_count, tm_count, rows), 0, 1 << 20) * rows + jnp.arange(rows, dtype=jnp.int32)
    order = jnp.argsort(jnp.argsort(scores, axis=2), axis=2)
    final = (order < CAP) & (home_rows < tm_count - 1)
    chosen = jnp.where(final, EP_LEN - 1, jnp.where(keep, blocks(future), blocks(nearby)))
    return (unblock(chosen) - times).astype(jnp.int32)


def with_spikes(array, key, source, target, blocks, factor):
    def block_of(axis_at):
        return (jnp.arange(array.shape[axis_at]) // (array.shape[axis_at] // blocks)).reshape((-1,) + (1,) * (array.ndim - 1 - axis_at))

    one_side = jax.random.permutation(key, blocks)[block_of(target)]
    second = (block_of(target) + blocks // 2) % blocks
    return jnp.where((block_of(source) == one_side) | (block_of(source) == second), factor * array, array)


def shard_levels(stream_key, shape, cuts, least, high):
    def one(position, blocks):
        heights = jax.random.uniform(jax.random.fold_in(jax.random.fold_in(stream_key, 6), position), (blocks,), jnp.float32, least / len(cuts), high / len(cuts))
        return jnp.repeat(jnp.exp(heights), shape[position] // blocks).reshape((-1,) + (1,) * (len(shape) - position - 1))

    loudness = one(*cuts[0])
    for cut in cuts[1:]:
        loudness = loudness * one(*cut)
    return loudness


def normal_values(stream_key, dims, spread, bound, shards=(), kind=jnp.bfloat16):
    result = jax.random.normal(stream_key, dims, jnp.float32) * spread
    if len(shards) > 0:
        result = shard_levels(stream_key, dims, shards, -0.22, 0.18) * result
    return jnp.clip(result, min=-bound, max=bound).astype(kind)


def bell_draw_with(stream_key, extent, deviation, reach, shards, heavy, kind=jnp.bfloat16):
    drawn = deviation * jax.random.normal(stream_key, extent, jnp.float32)
    if shards:
        drawn = drawn * shard_levels(stream_key, extent, shards, -0.22, 0.18)
    return jnp.clip(with_spikes(drawn, jax.random.fold_in(stream_key, 3), *heavy), -reach, reach).astype(kind)


def setup_inputs(seed: int = 0) -> dict:
    streams_of = jax.random.split(jax.random.key(seed), 8)
    return {
        "state_feats": bell_draw_with(streams_of[0], (EPISODES, EP_LEN, S), 1.0, 24.0, ((0, 2), (1, 128)), (1, 2, 128, 5.5)),
        "achieved": bell_draw_with(streams_of[1], (EPISODES, EP_LEN, G), 1.0, 24.0, ((0, 2), (1, 128)), (1, 2, 128, 5.5)),
        "offsets": draw_offsets(jax.random.fold_in(streams_of[7], 71), 0),
        "w_in": normal_values(streams_of[3], (S + G, H), (S + G) ** -0.5, 0.21875),
        "b_in": normal_values(streams_of[4], (H,), 0.5, 3.0, (), jnp.float32),
        "w_out": normal_values(streams_of[5], (H,), 64 ** -0.5, 0.75, (), jnp.float32),
        "b_out": jnp.clip(jax.random.uniform(streams_of[6], (1,), jnp.float32, -1.0, 1.0), -1.0, 1.0),
    }


def reference(state_feats, achieved, offsets, w_in, b_in, w_out, b_out):
    times = jnp.arange(EP_LEN, dtype=jnp.int32)
    target = (times[None, :] + offsets).astype(jnp.int32)
    goal = jnp.take_along_axis(achieved, target[:, :, None], axis=1)
    scale = 1.0 / math.sqrt(EPISODES * EP_LEN)

    def episode_step(carry, parts):
        feats, reached, wanted = parts
        inputs = jnp.concatenate([feats, wanted], axis=1)
        pre = jnp.dot(inputs, w_in, preferred_element_type=jnp.float32) + b_in
        hidden = jax.nn.silu(pre).astype(jnp.bfloat16)
        hidden_wide = hidden.astype(jnp.float32)
        value = jnp.dot(hidden_wide, w_out, precision=lax.Precision.HIGHEST) + b_out[0]
        diff = reached.astype(jnp.float32) - wanted.astype(jnp.float32)
        reward = -lax.optimization_barrier(jnp.mean(diff * diff, axis=1))
        error = value - reward
        grad_value = error * scale
        sig = jax.nn.sigmoid(pre)
        grad_pre = grad_value[:, None] * w_out[None, :] * (sig * (1.0 + pre * (1.0 - sig)))
        grad_low = grad_pre.astype(jnp.bfloat16)
        gw_in = lax.dot_general(inputs, grad_low, (((0,), (0,)), ((), ())), preferred_element_type=jnp.float32)
        gb_in = lax.optimization_barrier(jnp.sum(grad_pre, axis=0))
        gw_out = jnp.dot(grad_value, hidden_wide, precision=lax.Precision.HIGHEST)
        gb_out = lax.optimization_barrier(jnp.sum(grad_value, keepdims=True))
        return ((carry[0] + gw_in, carry[1] + gb_in, carry[2] + gw_out, carry[3] + gb_out), error)
    start = (jnp.zeros((S + G, H), jnp.float32), jnp.zeros((H,), jnp.float32), jnp.zeros((H,), jnp.float32), jnp.zeros((1,), jnp.float32))
    totals, errors = lax.scan(episode_step, start, (state_feats, achieved, goal))
    return (errors, totals[0], totals[1], totals[2], totals[3])
```

```python
import functools
import math

import jax
import jax.numpy as jnp
from jax import lax
from jax.experimental import pallas as pl
from jax.experimental.pallas import tpu as pltpu
from jax.sharding import Mesh
from jax.sharding import PartitionSpec as P

CAP = 4
TM = ("tm_0", "tm_1", "tm_2")
TM_DP = ("tm_0", "tm_1", "tm_2", "dp")
PLANE = ("tm_0", "tm_1")
LINE = "tm_2"
N_TM = 128
N_PLANE = 16
N_LINE = 8
ROWS = 256
STEPS = 4
S = 256
G = 512
H = 2048
LANES = 128
HALF = (S + G) // 2
SLAB = HALF // N_PLANE
CHUNK = 256
F32 = jnp.float32
BF16 = jnp.bfloat16
I32 = jnp.int32


def iota(shape, dim):
    return lax.broadcasted_iota(I32, shape, dim)


def dot(a, b, dims=(((1,), (0,)), ((), ()))):
    return lax.dot_general(a, b, dims, preferred_element_type=F32)


def flag(mask):
    return jnp.where(mask, 1.0, 0.0)


def pick_kernel(place_ref, offs_ref, table_ref, out_ref, wide_ref):
    me = place_ref[0]
    offs = offs_ref[...].reshape(N_TM, ROWS)
    peer = iota((N_TM, ROWS), 0)
    row = iota((N_TM, ROWS), 1)
    target = peer * STEPS + (row & (STEPS - 1)) + offs
    hit = ((target >> 2) == me) & (peer != me)
    earlier = flag(iota((ROWS, ROWS), 0) < iota((ROWS, ROWS), 1)).astype(BF16)
    rank = dot(flag(hit).astype(BF16), earlier)
    position = ((row - (row & (STEPS - 1))) + (target & (STEPS - 1)) + 1).astype(F32)
    table = table_ref[...]
    for c in range(CAP):
        place = jnp.sum(
            jnp.where(hit & (rank == float(c)), position, 0.0), axis=1, keepdims=True
        )
        wanted = flag(row.astype(F32) + 1.0 == place).astype(BF16)
        picked = dot(wanted, table)
        for j in range(G // LANES):
            wide_ref[pl.ds(c * (G // LANES) + j, N_TM, stride=16), :] = picked[
                :, j * LANES : (j + 1) * LANES
            ]
    out_ref[...] = wide_ref[...].astype(BF16)


def half_rows(core):
    k = iota((HALF, S + G), 0)
    eighth = k >> 3
    plane = (eighth * 171) >> 9
    within = eighth - plane * 3
    feature = (plane * N_LINE + (k & 7)) * 6 + core * 3 + within
    return flag(iota((HALF, S + G), 1) == feature).astype(BF16)


def three(x):
    high = x.astype(BF16).astype(F32)
    rest = x - high
    middle = rest.astype(BF16).astype(F32)
    return high, middle, rest - middle


def stack_rows(rows, count):
    width = rows[0].shape[1]
    at = iota((count, width), 0)
    total = jnp.zeros((count, width), F32)
    for n, r in enumerate(rows):
        total = jnp.where(at == n, jnp.broadcast_to(r, (count, width)), total)
    return total


def main_kernel(
    scale,
    place_ref,
    b_out_ref,
    offs_ref,
    fetched_ref,
    table_ref,
    state_ref,
    w_in_ref,
    b_in_ref,
    w_out_ref,
    td_ref,
    send_ref,
    keep_ref,
    slope_ref,
    hidden_ref,
    inputs_ref,
):
    me = place_ref[0]
    core = place_ref[1]
    row = iota((ROWS, ROWS), 1)
    col = iota((ROWS, ROWS), 0)
    offs = offs_ref[...]
    lane = iota((1, ROWS), 1)
    target = me * STEPS + (lane & (STEPS - 1)) + offs
    owner_lane = (target >> 2).astype(F32)
    position_lane = ((lane - (lane & (STEPS - 1))) + (target & (STEPS - 1))).astype(F32)

    def to_column(x):
        return jnp.sum(
            jnp.where(row == col, jnp.broadcast_to(x, (ROWS, ROWS)), 0.0),
            axis=1,
            keepdims=True,
        )

    owner = to_column(owner_lane)
    position = to_column(position_lane)
    slot = jnp.sum(flag((owner == owner_lane) & (row < col)), axis=1, keepdims=True)
    remote = owner != me.astype(F32)
    near_at = jnp.where(remote, -1.0, position)
    far_at = jnp.where(remote, owner * 16.0 + slot * 4.0, -100.0).astype(I32)
    near = flag(row.astype(F32) == near_at).astype(BF16)
    spot = iota((ROWS, N_TM * 16), 1)
    inputs_ref[:, :S] = state_ref[...]
    fetched = fetched_ref[...]
    gap = jnp.zeros((ROWS, LANES), F32)
    for j in range(G // LANES):
        far = flag(spot == far_at + j).astype(BF16)
        part = table_ref[:, j * LANES : (j + 1) * LANES]
        goal = dot(far, fetched) + dot(near, part)
        diff = part.astype(F32) - goal
        gap = gap + diff * diff
        inputs_ref[:, S + j * LANES : S + (j + 1) * LANES] = goal.astype(BF16)
    reward = -(jnp.sum(gap, axis=1, keepdims=True) * (1.0 / G))
    inputs = inputs_ref[...]

    def forward(n, total):
        at = pl.ds(pl.multiple_of(n * CHUNK, CHUNK), CHUNK)
        pre = dot(inputs, w_in_ref[:, at]) + b_in_ref[:, at]
        sig = 1.0 / (1.0 + jnp.exp(-pre))
        head = w_out_ref[:, at]
        hidden = (pre * sig).astype(BF16)
        hidden_ref[:, at] = hidden
        slope_ref[:, at] = head * (sig * (1.0 + pre * (1.0 - sig)))
        term = hidden.astype(F32) * head
        return total + term[:, :LANES] + term[:, LANES:]

    total = lax.fori_loop(0, H // CHUNK, forward, jnp.zeros((ROWS, LANES), F32))
    value = jnp.sum(total, axis=1, keepdims=True) + b_out_ref[0]
    error = value - reward
    grad_value = error * scale

    error_lane = jnp.sum(jnp.where(row == col, error, 0.0), axis=0, keepdims=True)
    td = jnp.zeros((ROWS // STEPS, STEPS), F32)
    for s in range(STEPS):
        mine = iota((ROWS // STEPS, ROWS), 1) == iota((ROWS // STEPS, ROWS), 0) * STEPS + s
        column = jnp.sum(jnp.where(mine, error_lane, 0.0), axis=1, keepdims=True)
        td = jnp.where(iota((ROWS // STEPS, STEPS), 1) == s, column, td)
    td_ref[...] = td

    kept = dot(half_rows(core), inputs, (((1,), (1,)), ((), ())))
    keep_ref[...] = kept.astype(BF16)
    sent = dot(half_rows(1 - core), inputs, (((1,), (1,)), ((), ()))).astype(BF16)
    for b in range(H // ROWS):
        send_ref[ROWS : ROWS + 48, b * ROWS : (b + 1) * ROWS] = sent[b * 48 : (b + 1) * 48, :]

    total_value = jnp.sum(grad_value, axis=0, keepdims=True)

    def backward(n, carry):
        at = pl.ds(pl.multiple_of(n * CHUNK, CHUNK), CHUNK)
        grad_pre = grad_value * slope_ref[:, at]
        send_ref[:ROWS, at] = grad_pre.astype(BF16)
        first = jnp.sum(grad_pre, axis=0, keepdims=True)
        second = jnp.sum(grad_value * hidden_ref[:, at].astype(F32), axis=0, keepdims=True)
        third = jnp.broadcast_to(total_value, (1, CHUNK))
        rows = stack_rows(three(first) + three(second) + three(third), 16)
        send_ref[ROWS + 48 : ROWS + 64, at] = rows.astype(BF16)
        return carry

    lax.fori_loop(0, H // CHUNK, backward, 0)


def product_kernel(own_ref, other_ref, keep_ref, out_ref, left_ref):
    for b in range(H // ROWS):
        left_ref[b * 48 : (b + 1) * 48, :] = other_ref[
            ROWS : ROWS + 48, b * ROWS : (b + 1) * ROWS
        ]

    def step(n, carry):
        at = pl.ds(pl.multiple_of(n * CHUNK, CHUNK), CHUNK)
        part = dot(keep_ref[...], own_ref[:ROWS, at]) + dot(left_ref[...], other_ref[:ROWS, at])
        mine = own_ref[ROWS + 48 : ROWS + 64, at].astype(F32)
        theirs = other_ref[ROWS + 48 : ROWS + 64, at].astype(F32)
        sums = []
        for q in range(3):
            a = mine[3 * q : 3 * q + 1] + mine[3 * q + 1 : 3 * q + 2] + mine[3 * q + 2 : 3 * q + 3]
            b = theirs[3 * q : 3 * q + 1] + theirs[3 * q + 1 : 3 * q + 2] + theirs[3 * q + 2 : 3 * q + 3]
            sums.append(three(a + b))
        lane = iota((1, CHUNK), 1)
        last = jnp.where(lane == 0, sums[2][0], jnp.where(lane == 1, sums[2][1], sums[2][2]))
        small = stack_rows(sums[0] + sums[1] + (last,), 8)
        for p in range(N_PLANE):
            slab = jnp.concatenate([part[p * SLAB : (p + 1) * SLAB], small], axis=0)
            out_ref[p * 32 : (p + 1) * 32, at] = slab.astype(BF16)
        return carry

    lax.fori_loop(0, H // CHUNK, step, 0)


BLOCK = 88


def plane_kernel(got_ref, out_ref, sum_ref):
    def step(n, carry):
        at = pl.ds(pl.multiple_of(n * CHUNK, CHUNK), CHUNK)
        total = got_ref[0:32, at].astype(F32)
        for p in range(1, N_PLANE):
            total = total + got_ref[p * 32 : (p + 1) * 32, at].astype(F32)
        sum_ref[:, at] = total
        return carry

    lax.fori_loop(0, H // CHUNK, step, 0)
    for b in range(H // LANES):
        at = slice(b * LANES, (b + 1) * LANES)
        for i in range(3):
            out_ref[pl.ds(i * 16 + b, N_LINE, stride=BLOCK), :] = sum_ref[8 * i : 8 * i + 8, at]
        tail = sum_ref[24:32, at]
        for q in range(2):
            joined = tail[3 * q : 3 * q + 1] + tail[3 * q + 1 : 3 * q + 2] + tail[3 * q + 2 : 3 * q + 3]
            out_ref[pl.ds(48 + q * 16 + b, N_LINE, stride=BLOCK), :] = jnp.broadcast_to(
                joined, (N_LINE, LANES)
            )
    last = sum_ref[30:31, 0:LANES]
    lane = iota((1, LANES), 1)
    whole = jnp.sum(jnp.where(lane < 3, last, 0.0), axis=1, keepdims=True)
    for n in range(80, BLOCK):
        out_ref[pl.ds(n, N_LINE, stride=BLOCK), :] = jnp.broadcast_to(whole, (N_LINE, LANES))


def line_kernel(got_ref, w_ref, b_in_ref, w_out_ref, b_out_ref, sum_ref):
    total = got_ref[0:BLOCK, :]
    for z in range(1, N_LINE):
        total = total + got_ref[z * BLOCK : (z + 1) * BLOCK, :]
    sum_ref[...] = total
    for i in range(3):
        for b in range(H // LANES):
            w_ref[i : i + 1, b * LANES : (b + 1) * LANES] = sum_ref[i * 16 + b : i * 16 + b + 1, :]
    b_in_ref[...] = sum_ref[48:64, :]
    w_out_ref[...] = sum_ref[64:80, :]
    b_out_ref[...] = sum_ref[80:81, :]


def call(kernel, shapes, operands, scratch, flops, in_smem=0):
    specs = [pl.BlockSpec(memory_space=pltpu.SMEM)] * in_smem
    specs += [pl.BlockSpec(memory_space=pltpu.VMEM)] * (len(operands) - in_smem)
    outs = [jax.ShapeDtypeStruct(shape, kind) for shape, kind in shapes]
    return pl.pallas_call(
        kernel,
        out_shape=outs,
        in_specs=specs,
        out_specs=[pl.BlockSpec(memory_space=pltpu.VMEM)] * len(outs),
        scratch_shapes=scratch,
        cost_estimate=pl.CostEstimate(flops=flops, bytes_accessed=1 << 20, transcendentals=0),
    )(*operands)


def body(state_feats, achieved, offsets, w_in, b_in, w_out, b_out):
    place = jnp.stack([lax.axis_index(TM), lax.axis_index("dp")]).astype(I32)
    table = achieved.reshape(ROWS, G)
    state = state_feats.reshape(ROWS, S)
    offs = offsets.reshape(1, ROWS)
    known = lax.all_to_all(
        jnp.broadcast_to(offs[None], (N_TM, 1, ROWS)), TM, split_axis=0, concat_axis=0, tiled=True
    )
    (picked,) = call(
        pick_kernel,
        [((N_TM * 16, LANES), BF16)],
        (place, known, table),
        [pltpu.VMEM((N_TM * 16, LANES), F32)],
        10**8,
        1,
    )
    fetched = lax.all_to_all(
        picked.reshape(N_TM, 16, LANES), TM, split_axis=0, concat_axis=0, tiled=True
    ).reshape(N_TM * 16, LANES)
    scale = 1.0 / math.sqrt(ROWS * N_TM * 2)
    td, send, keep = call(
        functools.partial(main_kernel, scale),
        [((ROWS // STEPS, STEPS), F32), ((ROWS + 64, H), BF16), ((HALF, ROWS), BF16)],
        (place, b_out, offs, fetched, table, state, w_in, b_in.reshape(1, H), w_out.reshape(1, H)),
        [pltpu.VMEM((ROWS, H), F32), pltpu.VMEM((ROWS, H), BF16), pltpu.VMEM((ROWS, S + G), BF16)],
        2 * 10**9,
        2,
    )
    other = lax.ppermute(send, "dp", [(0, 1), (1, 0)])
    (slabs,) = call(
        product_kernel,
        [((N_PLANE * 32, H), BF16)],
        (send, other, keep),
        [pltpu.VMEM((HALF, ROWS), BF16)],
        10**9,
    )
    got = lax.all_to_all(
        slabs.reshape(N_PLANE, 32, H), PLANE, split_axis=0, concat_axis=0, tiled=True
    ).reshape(N_PLANE * 32, H)
    (lines,) = call(
        plane_kernel,
        [((N_LINE * BLOCK, LANES), F32)],
        (got,),
        [pltpu.VMEM((32, H), F32)],
        10**7,
    )
    got = lax.all_to_all(
        lines.reshape(N_LINE, BLOCK, LANES), LINE, split_axis=0, concat_axis=0, tiled=True
    ).reshape(N_LINE * BLOCK, LANES)
    grad_w_in, grad_b_in, grad_w_out, grad_b_out = call(
        line_kernel,
        [((3, H), F32), ((16, LANES), F32), ((16, LANES), F32), ((1, LANES), F32)],
        (got,),
        [pltpu.VMEM((BLOCK, LANES), F32)],
        10**6,
    )
    return td, grad_w_in, grad_b_in.reshape(H), grad_w_out.reshape(H), grad_b_out[0, :1]


def solution(mesh):
    split = Mesh(mesh.devices.reshape(4, 4, 8, mesh.shape["dp"]), TM_DP)
    placed = (P("dp", TM, None), P("dp", TM, None), P("dp", TM), P(), P(), P(), P())
    return jax.shard_map(
        body,
        mesh=split,
        in_specs=placed,
        out_specs=(P("dp", TM), P(TM_DP, None), P(), P(), P()),
        check_vma=False,
    )
```

```python
import functools
import math

import jax
import jax.numpy as jnp
from jax import lax
from jax.experimental import pallas as pl
from jax.experimental.pallas import tpu as pltpu
from jax.sharding import Mesh
from jax.sharding import PartitionSpec as P

CAP = 4
TM = ("tm_0", "tm_1", "tm_2")
TM_DP = ("tm_0", "tm_1", "tm_2", "dp")
PLANE = ("tm_0", "tm_1")
LINE = "tm_2"
N_TM = 128
N_PLANE = 16
N_LINE = 8
ROWS = 256
STEPS = 4
S = 256
G = 512
H = 2048
LANES = 128
HALF = (S + G) // 2
SLAB = HALF // N_PLANE
CHUNK = 256
F32 = jnp.float32
BF16 = jnp.bfloat16
I32 = jnp.int32


def iota(shape, dim):
    return lax.broadcasted_iota(I32, shape, dim)


def dot(a, b, dims=(((1,), (0,)), ((), ()))):
    return lax.dot_general(a, b, dims, preferred_element_type=F32)


def flag(mask):
    return jnp.where(mask, 1.0, 0.0)


def pick_kernel(place_ref, offs_ref, table_ref, out_ref, wide_ref):
    me = place_ref[0]
    offs = offs_ref[...].reshape(N_TM, ROWS)
    peer = iota((N_TM, ROWS), 0)
    row = iota((N_TM, ROWS), 1)
    target = peer * STEPS + (row & (STEPS - 1)) + offs
    hit = ((target >> 2) == me) & (peer != me)
    earlier = flag(iota((ROWS, ROWS), 0) < iota((ROWS, ROWS), 1)).astype(BF16)
    rank = dot(flag(hit).astype(BF16), earlier)
    position = ((row - (row & (STEPS - 1))) + (target & (STEPS - 1)) + 1).astype(F32)
    table = table_ref[...]
    for c in range(CAP):
        place = jnp.sum(
            jnp.where(hit & (rank == float(c)), position, 0.0), axis=1, keepdims=True
        )
        wanted = flag(row.astype(F32) + 1.0 == place).astype(BF16)
        picked = dot(wanted, table)
        for j in range(G // LANES):
            wide_ref[pl.ds(c * (G // LANES) + j, N_TM, stride=16), :] = picked[
                :, j * LANES : (j + 1) * LANES
            ]
    out_ref[...] = wide_ref[...].astype(BF16)


def half_rows(core):
    k = iota((HALF, S + G), 0)
    eighth = k >> 3
    plane = (eighth * 171) >> 9
    within = eighth - plane * 3
    feature = (plane * N_LINE + (k & 7)) * 6 + core * 3 + within
    return flag(iota((HALF, S + G), 1) == feature).astype(BF16)


def three(x):
    high = x.astype(BF16).astype(F32)
    rest = x - high
    middle = rest.astype(BF16).astype(F32)
    return high, middle, rest - middle


def stack_rows(rows, count):
    width = rows[0].shape[1]
    at = iota((count, width), 0)
    total = jnp.zeros((count, width), F32)
    for n, r in enumerate(rows):
        total = jnp.where(at == n, jnp.broadcast_to(r, (count, width)), total)
    return total


def main_kernel(
    scale,
    place_ref,
    b_out_ref,
    offs_ref,
    fetched_ref,
    table_ref,
    state_ref,
    w_in_ref,
    b_in_ref,
    w_out_ref,
    td_ref,
    send_ref,
    keep_ref,
    slope_ref,
    hidden_ref,
    inputs_ref,
):
    me = place_ref[0]
    core = place_ref[1]
    row = iota((ROWS, ROWS), 1)
    col = iota((ROWS, ROWS), 0)
    offs = offs_ref[...]
    lane = iota((1, ROWS), 1)
    target = me * STEPS + (lane & (STEPS - 1)) + offs
    owner_lane = (target >> 2).astype(F32)
    position_lane = ((lane - (lane & (STEPS - 1))) + (target & (STEPS - 1))).astype(F32)

    def to_column(x):
        return jnp.sum(
            jnp.where(row == col, jnp.broadcast_to(x, (ROWS, ROWS)), 0.0),
            axis=1,
            keepdims=True,
        )

    owner = to_column(owner_lane)
    position = to_column(position_lane)
    slot = jnp.sum(flag((owner == owner_lane) & (row < col)), axis=1, keepdims=True)
    remote = owner != me.astype(F32)
    near_at = jnp.where(remote, -1.0, position)
    far_at = jnp.where(remote, owner * 16.0 + slot * 4.0, -100.0).astype(I32)
    near = flag(row.astype(F32) == near_at).astype(BF16)
    spot = iota((ROWS, N_TM * 16), 1)
    inputs_ref[:, :S] = state_ref[...]
    fetched = fetched_ref[...]
    gap = jnp.zeros((ROWS, LANES), F32)
    for j in range(G // LANES):
        far = flag(spot == far_at + j).astype(BF16)
        part = table_ref[:, j * LANES : (j + 1) * LANES]
        goal = dot(far, fetched) + dot(near, part)
        diff = part.astype(F32) - goal
        gap = gap + diff * diff
        inputs_ref[:, S + j * LANES : S + (j + 1) * LANES] = goal.astype(BF16)
    reward = -(jnp.sum(gap, axis=1, keepdims=True) * (1.0 / G))
    inputs = inputs_ref[...]

    def forward(n, total):
        at = pl.ds(pl.multiple_of(n * CHUNK, CHUNK), CHUNK)
        pre = dot(inputs, w_in_ref[:, at]) + b_in_ref[:, at]
        sig = 1.0 / (1.0 + jnp.exp(-pre))
        head = w_out_ref[:, at]
        hidden = (pre * sig).astype(BF16)
        hidden_ref[:, at] = hidden
        slope_ref[:, at] = head * (sig * (1.0 + pre * (1.0 - sig)))
        term = hidden.astype(F32) * head
        return total + term[:, :LANES] + term[:, LANES:]

    total = lax.fori_loop(0, H // CHUNK, forward, jnp.zeros((ROWS, LANES), F32))
    value = jnp.sum(total, axis=1, keepdims=True) + b_out_ref[0]
    error = value - reward
    grad_value = error * scale

    error_lane = jnp.sum(jnp.where(row == col, error, 0.0), axis=0, keepdims=True)
    td = jnp.zeros((ROWS // STEPS, STEPS), F32)
    for s in range(STEPS):
        mine = iota((ROWS // STEPS, ROWS), 1) == iota((ROWS // STEPS, ROWS), 0) * STEPS + s
        column = jnp.sum(jnp.where(mine, error_lane, 0.0), axis=1, keepdims=True)
        td = jnp.where(iota((ROWS // STEPS, STEPS), 1) == s, column, td)
    td_ref[...] = td

    kept = dot(half_rows(core), inputs, (((1,), (1,)), ((), ())))
    keep_ref[...] = kept.astype(BF16)
    sent = dot(half_rows(1 - core), inputs, (((1,), (1,)), ((), ()))).astype(BF16)
    for b in range(H // ROWS):
        send_ref[ROWS : ROWS + 48, b * ROWS : (b + 1) * ROWS] = sent[b * 48 : (b + 1) * 48, :]

    total_value = jnp.sum(grad_value, axis=0, keepdims=True)

    def backward(n, carry):
        at = pl.ds(pl.multiple_of(n * CHUNK, CHUNK), CHUNK)
        grad_pre = grad_value * slope_ref[:, at]
        send_ref[:ROWS, at] = grad_pre.astype(BF16)
        first = jnp.sum(grad_pre, axis=0, keepdims=True)
        second = jnp.sum(grad_value * hidden_ref[:, at].astype(F32), axis=0, keepdims=True)
        third = jnp.broadcast_to(total_value, (1, CHUNK))
        rows = stack_rows(three(first) + three(second) + three(third), 16)
        send_ref[ROWS + 48 : ROWS + 64, at] = rows.astype(BF16)
        return carry

    lax.fori_loop(0, H // CHUNK, backward, 0)


def product_kernel(own_ref, other_ref, keep_ref, out_ref, left_ref):
    for b in range(H // ROWS):
        left_ref[b * 48 : (b + 1) * 48, :] = other_ref[
            ROWS : ROWS + 48, b * ROWS : (b + 1) * ROWS
        ]

    def step(n, carry):
        at = pl.ds(pl.multiple_of(n * CHUNK, CHUNK), CHUNK)
        part = dot(keep_ref[...], own_ref[:ROWS, at]) + dot(left_ref[...], other_ref[:ROWS, at])
        mine = own_ref[ROWS + 48 : ROWS + 64, at].astype(F32)
        theirs = other_ref[ROWS + 48 : ROWS + 64, at].astype(F32)
        sums = []
        for q in range(3):
            a = mine[3 * q : 3 * q + 1] + mine[3 * q + 1 : 3 * q + 2] + mine[3 * q + 2 : 3 * q + 3]
            b = theirs[3 * q : 3 * q + 1] + theirs[3 * q + 1 : 3 * q + 2] + theirs[3 * q + 2 : 3 * q + 3]
            sums.append(three(a + b))
        lane = iota((1, CHUNK), 1)
        last = jnp.where(lane == 0, sums[2][0], jnp.where(lane == 1, sums[2][1], sums[2][2]))
        small = stack_rows(sums[0] + sums[1] + (last,), 8)
        for p in range(N_PLANE):
            slab = jnp.concatenate([part[p * SLAB : (p + 1) * SLAB], small], axis=0)
            out_ref[p * 32 : (p + 1) * 32, at] = slab.astype(BF16)
        return carry

    lax.fori_loop(0, H // CHUNK, step, 0)


BLOCK = 88


def plane_kernel(got_ref, out_ref, sum_ref):
    def step(n, carry):
        at = pl.ds(pl.multiple_of(n * CHUNK, CHUNK), CHUNK)
        total = got_ref[0:32, at].astype(F32)
        for p in range(1, N_PLANE):
            total = total + got_ref[p * 32 : (p + 1) * 32, at].astype(F32)
        sum_ref[:, at] = total
        return carry

    lax.fori_loop(0, H // CHUNK, step, 0)
    for b in range(H // LANES):
        at = slice(b * LANES, (b + 1) * LANES)
        for i in range(3):
            out_ref[pl.ds(i * 16 + b, N_LINE, stride=BLOCK), :] = sum_ref[8 * i : 8 * i + 8, at]
        tail = sum_ref[24:32, at]
        for q in range(2):
            joined = tail[3 * q : 3 * q + 1] + tail[3 * q + 1 : 3 * q + 2] + tail[3 * q + 2 : 3 * q + 3]
            out_ref[pl.ds(48 + q * 16 + b, N_LINE, stride=BLOCK), :] = jnp.broadcast_to(
                joined, (N_LINE, LANES)
            )
    last = sum_ref[30:31, 0:LANES]
    lane = iota((1, LANES), 1)
    whole = jnp.sum(jnp.where(lane < 3, last, 0.0), axis=1, keepdims=True)
    for n in range(80, BLOCK):
        out_ref[pl.ds(n, N_LINE, stride=BLOCK), :] = jnp.broadcast_to(whole, (N_LINE, LANES))


def line_kernel(got_ref, w_ref, b_in_ref, w_out_ref, b_out_ref, sum_ref):
    total = got_ref[0:BLOCK, :]
    for z in range(1, N_LINE):
        total = total + got_ref[z * BLOCK : (z + 1) * BLOCK, :]
    sum_ref[...] = total
    for i in range(3):
        for b in range(H // LANES):
            w_ref[i : i + 1, b * LANES : (b + 1) * LANES] = sum_ref[i * 16 + b : i * 16 + b + 1, :]
    b_in_ref[...] = sum_ref[48:64, :]
    w_out_ref[...] = sum_ref[64:80, :]
    b_out_ref[...] = sum_ref[80:81, :]


def call(kernel, shapes, operands, scratch, flops, grant, in_smem=0):
    specs = [pl.BlockSpec(memory_space=pltpu.SMEM)] * in_smem
    specs += [pl.BlockSpec(memory_space=pltpu.VMEM)] * (len(operands) - in_smem)
    outs = [jax.ShapeDtypeStruct(shape, kind) for shape, kind in shapes]
    return pl.pallas_call(
        kernel,
        out_shape=outs,
        in_specs=specs,
        out_specs=[pl.BlockSpec(memory_space=pltpu.VMEM)] * len(outs),
        scratch_shapes=scratch,
        compiler_params=pltpu.CompilerParams(vmem_limit_bytes=grant << 20),
        cost_estimate=pl.CostEstimate(flops=flops, bytes_accessed=1 << 20, transcendentals=0),
    )(*operands)


def body(state_feats, achieved, offsets, w_in, b_in, w_out, b_out):
    place = jnp.stack([lax.axis_index(TM), lax.axis_index("dp")]).astype(I32)
    table = achieved.reshape(ROWS, G)
    state = state_feats.reshape(ROWS, S)
    offs = offsets.reshape(1, ROWS)
    known = lax.all_to_all(
        jnp.broadcast_to(offs[None], (N_TM, 1, ROWS)), TM, split_axis=0, concat_axis=0, tiled=True
    )
    (picked,) = call(
        pick_kernel,
        [((N_TM * 16, LANES), BF16)],
        (place, known, table),
        [pltpu.VMEM((N_TM * 16, LANES), F32)],
        10**8,
        6,
        1,
    )
    fetched = lax.all_to_all(
        picked.reshape(N_TM, 16, LANES), TM, split_axis=0, concat_axis=0, tiled=True
    ).reshape(N_TM * 16, LANES)
    scale = 1.0 / math.sqrt(ROWS * N_TM * 2)
    td, send, keep = call(
        functools.partial(main_kernel, scale),
        [((ROWS // STEPS, STEPS), F32), ((ROWS + 64, H), BF16), ((HALF, ROWS), BF16)],
        (place, b_out, offs, fetched, table, state, w_in, b_in.reshape(1, H), w_out.reshape(1, H)),
        [pltpu.VMEM((ROWS, H), F32), pltpu.VMEM((ROWS, H), BF16), pltpu.VMEM((ROWS, S + G), BF16)],
        2 * 10**9,
        18,
        2,
    )
    other = lax.ppermute(send, "dp", [(0, 1), (1, 0)])
    (slabs,) = call(
        product_kernel,
        [((N_PLANE * 32, H), BF16)],
        (send, other, keep),
        [pltpu.VMEM((HALF, ROWS), BF16)],
        10**9,
        12,
    )
    got = lax.all_to_all(
        slabs.reshape(N_PLANE, 32, H), PLANE, split_axis=0, concat_axis=0, tiled=True
    ).reshape(N_PLANE * 32, H)
    (lines,) = call(
        plane_kernel,
        [((N_LINE * BLOCK, LANES), F32)],
        (got,),
        [pltpu.VMEM((32, H), F32)],
        10**7,
        6,
    )
    got = lax.all_to_all(
        lines.reshape(N_LINE, BLOCK, LANES), LINE, split_axis=0, concat_axis=0, tiled=True
    ).reshape(N_LINE * BLOCK, LANES)
    grad_w_in, grad_b_in, grad_w_out, grad_b_out = call(
        line_kernel,
        [((3, H), F32), ((16, LANES), F32), ((16, LANES), F32), ((1, LANES), F32)],
        (got,),
        [pltpu.VMEM((BLOCK, LANES), F32)],
        10**6,
        4,
    )
    return td, grad_w_in, grad_b_in.reshape(H), grad_w_out.reshape(H), grad_b_out[0, :1]


def solution(mesh):
    split = Mesh(mesh.devices.reshape(4, 4, 8, mesh.shape["dp"]), TM_DP)
    placed = (P("dp", TM, None), P("dp", TM, None), P("dp", TM), P(), P(), P(), P())
    return jax.shard_map(
        body,
        mesh=split,
        in_specs=placed,
        out_specs=(P("dp", TM), P(TM_DP, None), P(), P(), P()),
        check_vma=False,
    )
```

```python
import functools
import math

import jax
import jax.numpy as jnp
from jax import lax
from jax.experimental import pallas as pl
from jax.experimental.pallas import tpu as pltpu
from jax.sharding import Mesh
from jax.sharding import PartitionSpec as P

CAP = 4
TM = ("tm_0", "tm_1", "tm_2")
TM_DP = ("tm_0", "tm_1", "tm_2", "dp")
PLANE = ("tm_0", "tm_1")
LINE = "tm_2"
N_TM = 128
N_PLANE = 16
N_LINE = 8
ROWS = 256
STEPS = 4
S = 256
G = 512
H = 2048
LANES = 128
HALF = (S + G) // 2
SLAB = HALF // N_PLANE
CHUNK = 256
F32 = jnp.float32
BF16 = jnp.bfloat16
I32 = jnp.int32


def iota(shape, dim):
    return lax.broadcasted_iota(I32, shape, dim)


def dot(a, b, dims=(((1,), (0,)), ((), ()))):
    return lax.dot_general(a, b, dims, preferred_element_type=F32)


def flag(mask):
    return jnp.where(mask, 1.0, 0.0)


def spread_kernel(offs_ref, many_ref, row_ref):
    offs = offs_ref[...]
    parts = jnp.concatenate([offs >> 4, offs & 15], axis=0).astype(F32).astype(BF16)
    episode = flag((iota((ROWS // STEPS, ROWS), 1) >> 2) == iota((ROWS // STEPS, ROWS), 0))
    wide = dot(parts, episode.astype(BF16))
    step = iota((2 * STEPS, ROWS), 1) & (STEPS - 1)
    which = iota((2 * STEPS, ROWS), 0)
    mine = (which & (STEPS - 1)) == step
    weight = jnp.where(which < STEPS, 16.0, 1.0)
    row = jnp.sum(jnp.where(mine, wide * weight, 0.0), axis=0, keepdims=True).astype(I32)
    row_ref[...] = row
    many_ref[...] = jnp.broadcast_to(row[None], (N_TM, 1, ROWS))


def pick_kernel(place_ref, offs_ref, table_ref, out_ref, wide_ref):
    me = place_ref[0]
    offs = offs_ref[...].reshape(N_TM, ROWS)
    peer = iota((N_TM, ROWS), 0)
    row = iota((N_TM, ROWS), 1)
    target = peer * STEPS + (row & (STEPS - 1)) + offs
    hit = ((target >> 2) == me) & (peer != me)
    earlier = flag(iota((ROWS, ROWS), 0) < iota((ROWS, ROWS), 1)).astype(BF16)
    rank = dot(flag(hit).astype(BF16), earlier)
    position = ((row - (row & (STEPS - 1))) + (target & (STEPS - 1)) + 1).astype(F32)
    table = table_ref[...]
    for c in range(CAP):
        place = jnp.sum(
            jnp.where(hit & (rank == float(c)), position, 0.0), axis=1, keepdims=True
        )
        wanted = flag(row.astype(F32) + 1.0 == place).astype(BF16)
        picked = dot(wanted, table)
        for j in range(G // LANES):
            wide_ref[pl.ds(c * (G // LANES) + j, N_TM, stride=16), :] = picked[
                :, j * LANES : (j + 1) * LANES
            ]
    out_ref[...] = wide_ref[...].astype(BF16)


def half_rows(core):
    k = iota((HALF, S + G), 0)
    eighth = k >> 3
    plane = (eighth * 171) >> 9
    within = eighth - plane * 3
    feature = (plane * N_LINE + (k & 7)) * 6 + core * 3 + within
    return flag(iota((HALF, S + G), 1) == feature).astype(BF16)


def three(x):
    high = x.astype(BF16).astype(F32)
    rest = x - high
    middle = rest.astype(BF16).astype(F32)
    return high, middle, rest - middle


def two(x):
    high = x.astype(BF16).astype(F32)
    return high, x - high


def stack_rows(rows, count):
    width = rows[0].shape[1]
    at = iota((count, width), 0)
    total = jnp.zeros((count, width), F32)
    for n, r in enumerate(rows):
        total = jnp.where(at == n, jnp.broadcast_to(r, (count, width)), total)
    return total


def ahead_kernel(
    place_ref,
    offs_ref,
    table_ref,
    state_ref,
    w_in_ref,
    b_in_ref,
    base_ref,
    near_ref,
    at_ref,
):
    me = place_ref[0]
    row = iota((ROWS, ROWS), 1)
    col = iota((ROWS, ROWS), 0)
    lane = iota((1, ROWS), 1)
    target = me * STEPS + (lane & (STEPS - 1)) + offs_ref[...]
    owner_lane = (target >> 2).astype(F32)
    position_lane = ((lane - (lane & (STEPS - 1))) + (target & (STEPS - 1))).astype(F32)

    def to_column(x):
        return jnp.sum(
            jnp.where(row == col, jnp.broadcast_to(x, (ROWS, ROWS)), 0.0),
            axis=1,
            keepdims=True,
        )

    owner = to_column(owner_lane)
    position = to_column(position_lane)
    slot = jnp.sum(flag((owner == owner_lane) & (row < col)), axis=1, keepdims=True)
    remote = owner != me.astype(F32)
    near_at = jnp.where(remote, -1.0, position)
    far_at = jnp.where(remote, owner * 16.0 + slot * 4.0, -100.0).astype(I32)
    near = flag(row.astype(F32) == near_at).astype(BF16)
    near_ref[...] = dot(near, table_ref[...]).astype(BF16)
    at_ref[...] = jnp.broadcast_to(far_at, (ROWS, LANES))
    state = state_ref[...]

    def step(n, carry):
        at = pl.ds(pl.multiple_of(n * CHUNK, CHUNK), CHUNK)
        base_ref[:, at] = dot(state, w_in_ref[:S, at]) + b_in_ref[:, at]
        return carry

    lax.fori_loop(0, H // CHUNK, step, 0)


def main_kernel(
    scale,
    place_ref,
    b_out_ref,
    fetched_ref,
    base_ref,
    near_ref,
    at_ref,
    table_ref,
    state_ref,
    w_in_ref,
    w_out_ref,
    td_ref,
    send_ref,
    keep_ref,
    slope_ref,
    hidden_ref,
    inputs_ref,
    goal_w_ref,
    sem,
):
    load = pltpu.make_async_copy(w_in_ref.at[pl.ds(S, G), :], goal_w_ref, sem)
    load.start()
    core = place_ref[1]
    far_at = at_ref[:, 0:1]
    spot = iota((ROWS, N_TM * 16), 1)
    inputs_ref[:, :S] = state_ref[...]
    fetched = fetched_ref[...]
    gap = jnp.zeros((ROWS, LANES), F32)
    for j in range(G // LANES):
        at = slice(j * LANES, (j + 1) * LANES)
        goal = dot(flag(spot == far_at + j).astype(BF16), fetched) + near_ref[:, at].astype(F32)
        diff = table_ref[:, at].astype(F32) - goal
        gap = gap + diff * diff
        inputs_ref[:, S + j * LANES : S + (j + 1) * LANES] = goal.astype(BF16)
    reward = -(jnp.sum(gap, axis=1, keepdims=True) * (1.0 / G))
    inputs = inputs_ref[...]
    load.wait()

    def forward(n, total):
        at = pl.ds(pl.multiple_of(n * CHUNK, CHUNK), CHUNK)
        pre = base_ref[:, at] + dot(inputs[:, S:], goal_w_ref[:, at])
        sig = 1.0 / (1.0 + jnp.exp(-pre))
        head = w_out_ref[:, at]
        hidden = (pre * sig).astype(BF16)
        hidden_ref[:, at] = hidden
        slope_ref[:, at] = head * (sig * (1.0 + pre * (1.0 - sig)))
        term = hidden.astype(F32) * head
        return total + term[:, :LANES] + term[:, LANES:]

    total = lax.fori_loop(0, H // CHUNK, forward, jnp.zeros((ROWS, LANES), F32))
    value = jnp.sum(total, axis=1, keepdims=True) + b_out_ref[0]
    error = value - reward
    grad_value = error * scale

    each = (STEPS * iota((ROWS, ROWS // STEPS), 1)) - iota((ROWS, ROWS // STEPS), 0)
    for s in range(STEPS):
        td_ref[s : s + 1, :] = jnp.sum(
            jnp.where(each + s == 0, error, 0.0), axis=0, keepdims=True
        )

    kept = dot(half_rows(core), inputs, (((1,), (1,)), ((), ())))
    keep_ref[...] = kept.astype(BF16)
    sent = dot(half_rows(1 - core), inputs, (((1,), (1,)), ((), ()))).astype(BF16)
    for b in range(H // ROWS):
        send_ref[ROWS : ROWS + 48, b * ROWS : (b + 1) * ROWS] = sent[b * 48 : (b + 1) * 48, :]

    total_value = jnp.sum(grad_value, axis=0, keepdims=True)

    def backward(n, carry):
        at = pl.ds(pl.multiple_of(n * CHUNK, CHUNK), CHUNK)
        grad_pre = grad_value * slope_ref[:, at]
        send_ref[:ROWS, at] = grad_pre.astype(BF16)
        first = jnp.sum(grad_pre, axis=0, keepdims=True)
        second = jnp.sum(grad_value * hidden_ref[:, at].astype(F32), axis=0, keepdims=True)
        third = jnp.broadcast_to(total_value, (1, CHUNK))
        rows = stack_rows(three(first) + three(second) + three(third), 16)
        send_ref[ROWS + 48 : ROWS + 64, at] = rows.astype(BF16)
        return carry

    lax.fori_loop(0, H // CHUNK, backward, 0)


PACK = 464
BLOCK = 88


def product_kernel(own_ref, other_ref, keep_ref, out_ref, left_ref):
    for b in range(H // ROWS):
        left_ref[b * 48 : (b + 1) * 48, :] = other_ref[
            ROWS : ROWS + 48, b * ROWS : (b + 1) * ROWS
        ]
    keep = keep_ref[...]
    left = left_ref[...]
    for n in range(H // CHUNK):
        at = slice(n * CHUNK, (n + 1) * CHUNK)
        part = dot(keep, own_ref[:ROWS, at]) + dot(left, other_ref[:ROWS, at])
        for p in range(N_PLANE):
            for i in range(3):
                tile = part[p * SLAB + 8 * i : p * SLAB + 8 * i + 8]
                pair = jnp.concatenate([tile[:, :LANES], tile[:, LANES:]], axis=0)
                start = p * PACK + (16 * i + 2 * n) * 8
                out_ref[start : start + 16, :] = pair.astype(BF16)
    mine = own_ref[ROWS + 48 : ROWS + 64, :].astype(F32)
    theirs = other_ref[ROWS + 48 : ROWS + 64, :].astype(F32)
    rows = []
    for q in range(3):
        a = mine[3 * q : 3 * q + 1] + mine[3 * q + 1 : 3 * q + 2] + mine[3 * q + 2 : 3 * q + 3]
        b = theirs[3 * q : 3 * q + 1] + theirs[3 * q + 1 : 3 * q + 2] + theirs[3 * q + 2 : 3 * q + 3]
        rows.append(two(a + b))
    blocks = []
    for q in range(2):
        for r in rows[q]:
            pieces = [r[:, b * LANES : (b + 1) * LANES] for b in range(H // LANES)]
            blocks.append(jnp.concatenate(pieces, axis=0))
    blocks.append(stack_rows([r[:, :LANES] for r in rows[2]], 16))
    small = jnp.concatenate(blocks, axis=0).astype(BF16)
    for p in range(N_PLANE):
        out_ref[p * PACK + HALF : (p + 1) * PACK, :] = small


def plane_kernel(got_ref, out_ref, sum_ref):
    for b in range(PACK // 16):
        total = got_ref[b * 16 : b * 16 + 16, :].astype(F32)
        for p in range(1, N_PLANE):
            total = total + got_ref[p * PACK + b * 16 : p * PACK + b * 16 + 16, :].astype(F32)
        sum_ref[b * 16 : b * 16 + 16, :] = total
    for n in range(48):
        out_ref[pl.ds(n, N_LINE, stride=BLOCK), :] = sum_ref[8 * n : 8 * n + 8, :]
    small = jnp.concatenate(
        [
            sum_ref[384:400, :] + sum_ref[400:416, :],
            sum_ref[416:432, :] + sum_ref[432:448, :],
            jnp.broadcast_to(sum_ref[448:449, :] + sum_ref[449:450, :], (8, LANES)),
        ],
        axis=0,
    )
    for z in range(N_LINE):
        out_ref[z * BLOCK + 48 : (z + 1) * BLOCK, :] = small


def line_kernel(got_ref, w_ref, b_in_ref, w_out_ref, b_out_ref, sum_ref):
    total = got_ref[0:BLOCK, :]
    for z in range(1, N_LINE):
        total = total + got_ref[z * BLOCK : (z + 1) * BLOCK, :]
    sum_ref[...] = total
    for i in range(3):
        for b in range(H // LANES):
            w_ref[i : i + 1, b * LANES : (b + 1) * LANES] = sum_ref[i * 16 + b : i * 16 + b + 1, :]
    b_in_ref[...] = sum_ref[48:64, :]
    w_out_ref[...] = sum_ref[64:80, :]
    b_out_ref[...] = sum_ref[80:81, :]


def call(kernel, shapes, operands, scratch, flops, grant, in_smem=0, in_hbm=()):
    specs = [pl.BlockSpec(memory_space=pltpu.SMEM)] * in_smem
    specs += [pl.BlockSpec(memory_space=pltpu.VMEM)] * (len(operands) - in_smem)
    for n in in_hbm:
        specs[n] = pl.BlockSpec(memory_space=pltpu.HBM)
    outs = [jax.ShapeDtypeStruct(shape, kind) for shape, kind in shapes]
    return pl.pallas_call(
        kernel,
        out_shape=outs,
        in_specs=specs,
        out_specs=[pl.BlockSpec(memory_space=pltpu.VMEM)] * len(outs),
        scratch_shapes=scratch,
        compiler_params=pltpu.CompilerParams(vmem_limit_bytes=grant << 20),
        cost_estimate=pl.CostEstimate(flops=flops, bytes_accessed=1 << 20, transcendentals=0),
    )(*operands)


def body(state_feats, achieved, offsets, w_in, b_in, w_out, b_out):
    place = jnp.stack([lax.axis_index(TM), lax.axis_index("dp")]).astype(I32)
    table = achieved.reshape(ROWS, G)
    state = state_feats.reshape(ROWS, S)
    many, offs = call(
        spread_kernel,
        [((N_TM, 1, ROWS), I32), ((1, ROWS), I32)],
        (offsets.T,),
        [],
        10**6,
        4,
    )
    known = lax.all_to_all(many, TM, split_axis=0, concat_axis=0, tiled=True)
    (picked,) = call(
        pick_kernel,
        [((N_TM * 16, LANES), BF16)],
        (place, known, table),
        [pltpu.VMEM((N_TM * 16, LANES), F32)],
        10**8,
        6,
        1,
    )
    base, near, at = call(
        ahead_kernel,
        [((ROWS, H), F32), ((ROWS, G), BF16), ((ROWS, LANES), I32)],
        (place, offs, table, state, w_in, b_in.reshape(1, H)),
        [],
        10**9,
        12,
        1,
    )
    fetched = lax.all_to_all(
        picked.reshape(N_TM, 16, LANES), TM, split_axis=0, concat_axis=0, tiled=True
    ).reshape(N_TM * 16, LANES)
    scale = 1.0 / math.sqrt(ROWS * N_TM * 2)
    td, send, keep = call(
        functools.partial(main_kernel, scale),
        [((STEPS, ROWS // STEPS), F32), ((ROWS + 64, H), BF16), ((HALF, ROWS), BF16)],
        (place, b_out, fetched, base, near, at, table, state, w_in, w_out.reshape(1, H)),
        [pltpu.VMEM((ROWS, H), F32), pltpu.VMEM((ROWS, H), BF16), pltpu.VMEM((ROWS, S + G), BF16), pltpu.VMEM((G, H), BF16), pltpu.SemaphoreType.DMA],
        2 * 10**9,
        48,
        2,
        (8,),
    )
    other = lax.ppermute(send, "dp", [(0, 1), (1, 0)])
    (packs,) = call(
        product_kernel,
        [((N_PLANE * PACK, LANES), BF16)],
        (send, other, keep),
        [pltpu.VMEM((HALF, ROWS), BF16)],
        10**9,
        12,
    )
    got = lax.all_to_all(
        packs.reshape(N_PLANE, PACK, LANES), PLANE, split_axis=0, concat_axis=0, tiled=True
    ).reshape(N_PLANE * PACK, LANES)
    (lines,) = call(
        plane_kernel,
        [((N_LINE * BLOCK, LANES), F32)],
        (got,),
        [pltpu.VMEM((PACK, LANES), F32)],
        10**7,
        6,
    )
    got = lax.all_to_all(
        lines.reshape(N_LINE, BLOCK, LANES), LINE, split_axis=0, concat_axis=0, tiled=True
    ).reshape(N_LINE * BLOCK, LANES)
    grad_w_in, grad_b_in, grad_w_out, grad_b_out = call(
        line_kernel,
        [((3, H), F32), ((16, LANES), F32), ((16, LANES), F32), ((1, LANES), F32)],
        (got,),
        [pltpu.VMEM((BLOCK, LANES), F32)],
        10**6,
        4,
    )
    return td.T, grad_w_in, grad_b_in.reshape(H), grad_w_out.reshape(H), grad_b_out[0, :1]


def solution(mesh):
    split = Mesh(mesh.devices.reshape(4, 4, 8, mesh.shape["dp"]), TM_DP)
    placed = (P("dp", TM, None), P("dp", TM, None), P("dp", TM), P(), P(), P(), P())
    return jax.shard_map(
        body,
        mesh=split,
        in_specs=placed,
        out_specs=(P("dp", TM), P(TM_DP, None), P(), P(), P()),
        check_vma=False,
    )
```

```python
import functools
import math

import jax
import jax.numpy as jnp
from jax import lax
from jax.experimental import pallas as pl
from jax.experimental.pallas import tpu as pltpu
from jax.sharding import Mesh
from jax.sharding import PartitionSpec as P

CAP = 4
TM = ("tm_0", "tm_1", "tm_2")
TM_DP = ("tm_0", "tm_1", "tm_2", "dp")
PLANE = ("tm_0", "tm_1")
LINE = "tm_2"
N_TM = 128
N_PLANE = 16
N_LINE = 8
ROWS = 256
STEPS = 4
S = 256
G = 512
H = 2048
LANES = 128
HALF = (S + G) // 2
SLAB = HALF // N_PLANE
CHUNK = 256
F32 = jnp.float32
BF16 = jnp.bfloat16
I32 = jnp.int32


def iota(shape, dim):
    return lax.broadcasted_iota(I32, shape, dim)


def dot(a, b, dims=(((1,), (0,)), ((), ()))):
    return lax.dot_general(a, b, dims, preferred_element_type=F32)


def flag(mask):
    return jnp.where(mask, 1.0, 0.0)


def spread_kernel(offs_ref, many_ref, row_ref):
    offs = offs_ref[...]
    parts = jnp.concatenate([offs >> 4, offs & 15], axis=0).astype(F32).astype(BF16)
    episode = flag((iota((ROWS // STEPS, ROWS), 1) >> 2) == iota((ROWS // STEPS, ROWS), 0))
    wide = dot(parts, episode.astype(BF16))
    step = iota((2 * STEPS, ROWS), 1) & (STEPS - 1)
    which = iota((2 * STEPS, ROWS), 0)
    mine = (which & (STEPS - 1)) == step
    weight = jnp.where(which < STEPS, 16.0, 1.0)
    row = jnp.sum(jnp.where(mine, wide * weight, 0.0), axis=0, keepdims=True).astype(I32)
    row_ref[...] = row
    many_ref[...] = jnp.broadcast_to(row[None], (N_TM, 1, ROWS))


def pick_kernel(place_ref, offs_ref, table_ref, out_ref, wide_ref):
    me = place_ref[0]
    offs = offs_ref[...].reshape(N_TM, ROWS)
    peer = iota((N_TM, ROWS), 0)
    row = iota((N_TM, ROWS), 1)
    target = peer * STEPS + (row & (STEPS - 1)) + offs
    hit = ((target >> 2) == me) & (peer != me)
    earlier = flag(iota((ROWS, ROWS), 0) < iota((ROWS, ROWS), 1)).astype(BF16)
    rank = dot(flag(hit).astype(BF16), earlier)
    position = ((row - (row & (STEPS - 1))) + (target & (STEPS - 1)) + 1).astype(F32)
    table = table_ref[...]
    for c in range(CAP):
        place = jnp.sum(
            jnp.where(hit & (rank == float(c)), position, 0.0), axis=1, keepdims=True
        )
        wanted = flag(row.astype(F32) + 1.0 == place).astype(BF16)
        picked = dot(wanted, table)
        for j in range(G // LANES):
            wide_ref[pl.ds(c * (G // LANES) + j, N_TM, stride=16), :] = picked[
                :, j * LANES : (j + 1) * LANES
            ]
    out_ref[...] = wide_ref[...].astype(BF16)


def half_rows(core):
    k = iota((HALF, S + G), 0)
    eighth = k >> 3
    plane = (eighth * 171) >> 9
    within = eighth - plane * 3
    feature = (plane * N_LINE + (k & 7)) * 6 + core * 3 + within
    return flag(iota((HALF, S + G), 1) == feature).astype(BF16)


def three(x):
    high = x.astype(BF16).astype(F32)
    rest = x - high
    middle = rest.astype(BF16).astype(F32)
    return high, middle, rest - middle


def two(x):
    high = x.astype(BF16).astype(F32)
    return high, x - high


def stack_rows(rows, count):
    width = rows[0].shape[1]
    at = iota((count, width), 0)
    total = jnp.zeros((count, width), F32)
    for n, r in enumerate(rows):
        total = jnp.where(at == n, jnp.broadcast_to(r, (count, width)), total)
    return total


def ahead_kernel(
    place_ref,
    offs_ref,
    table_ref,
    state_ref,
    w_in_ref,
    b_in_ref,
    base_ref,
    near_ref,
    at_ref,
):
    me = place_ref[0]
    row = iota((ROWS, ROWS), 1)
    col = iota((ROWS, ROWS), 0)
    lane = iota((1, ROWS), 1)
    target = me * STEPS + (lane & (STEPS - 1)) + offs_ref[...]
    owner_lane = (target >> 2).astype(F32)
    position_lane = ((lane - (lane & (STEPS - 1))) + (target & (STEPS - 1))).astype(F32)

    def to_column(x):
        return jnp.sum(
            jnp.where(row == col, jnp.broadcast_to(x, (ROWS, ROWS)), 0.0),
            axis=1,
            keepdims=True,
        )

    owner = to_column(owner_lane)
    position = to_column(position_lane)
    slot = jnp.sum(flag((owner == owner_lane) & (row < col)), axis=1, keepdims=True)
    remote = owner != me.astype(F32)
    near_at = jnp.where(remote, -1.0, position)
    far_at = jnp.where(remote, owner * float(CAP) + slot, -1.0).astype(I32)
    near = flag(row.astype(F32) == near_at).astype(BF16)
    near_ref[...] = dot(near, table_ref[...]).astype(BF16)
    at_ref[...] = jnp.broadcast_to(far_at, (ROWS, LANES))
    state = state_ref[...]

    def step(n, carry):
        at = pl.ds(pl.multiple_of(n * CHUNK, CHUNK), CHUNK)
        base_ref[:, at] = dot(state, w_in_ref[:S, at]) + b_in_ref[:, at]
        return carry

    lax.fori_loop(0, H // CHUNK, step, 0)


def main_kernel(
    scale,
    place_ref,
    b_out_ref,
    fetched_ref,
    base_ref,
    near_ref,
    at_ref,
    table_ref,
    state_ref,
    w_in_ref,
    w_out_ref,
    td_ref,
    send_ref,
    keep_ref,
    slope_ref,
    hidden_ref,
    inputs_ref,
    goal_w_ref,
    wide_ref,
    sem,
):
    load = pltpu.make_async_copy(w_in_ref.at[pl.ds(S, G), :], goal_w_ref, sem)
    load.start()
    core = place_ref[1]
    far_at = at_ref[:, 0:1]
    far = flag(iota((ROWS, N_TM * CAP), 1) == far_at).astype(BF16)
    inputs_ref[:, :S] = state_ref[...]
    wide_ref[...] = fetched_ref[...].astype(F32)
    gap = jnp.zeros((ROWS, LANES), F32)
    for j in range(G // LANES):
        at = slice(j * LANES, (j + 1) * LANES)
        fetched = wide_ref[pl.ds(j, N_TM * CAP, stride=G // LANES), :].astype(BF16)
        goal = dot(far, fetched) + near_ref[:, at].astype(F32)
        diff = table_ref[:, at].astype(F32) - goal
        gap = gap + diff * diff
        inputs_ref[:, S + j * LANES : S + (j + 1) * LANES] = goal.astype(BF16)
    reward = -(jnp.sum(gap, axis=1, keepdims=True) * (1.0 / G))
    inputs = inputs_ref[...]
    load.wait()

    def forward(n, total):
        at = pl.ds(pl.multiple_of(n * CHUNK, CHUNK), CHUNK)
        pre = base_ref[:, at] + dot(inputs[:, S:], goal_w_ref[:, at])
        sig = 1.0 / (1.0 + jnp.exp(-pre))
        head = w_out_ref[:, at]
        hidden = (pre * sig).astype(BF16)
        hidden_ref[:, at] = hidden
        slope_ref[:, at] = head * (sig * (1.0 + pre * (1.0 - sig)))
        term = hidden.astype(F32) * head
        return total + term[:, :LANES] + term[:, LANES:]

    total = lax.fori_loop(0, H // CHUNK, forward, jnp.zeros((ROWS, LANES), F32))
    value = jnp.sum(total, axis=1, keepdims=True) + b_out_ref[0]
    error = value - reward
    grad_value = error * scale

    each = (STEPS * iota((ROWS, ROWS // STEPS), 1)) - iota((ROWS, ROWS // STEPS), 0)
    for s in range(STEPS):
        td_ref[s : s + 1, :] = jnp.sum(
            jnp.where(each + s == 0, error, 0.0), axis=0, keepdims=True
        )

    kept = dot(half_rows(core), inputs, (((1,), (1,)), ((), ())))
    keep_ref[...] = kept.astype(BF16)
    sent = dot(half_rows(1 - core), inputs, (((1,), (1,)), ((), ()))).astype(BF16)
    for b in range(H // ROWS):
        send_ref[ROWS : ROWS + 48, b * ROWS : (b + 1) * ROWS] = sent[b * 48 : (b + 1) * 48, :]

    total_value = jnp.sum(grad_value, axis=0, keepdims=True)

    def backward(n, carry):
        at = pl.ds(pl.multiple_of(n * CHUNK, CHUNK), CHUNK)
        grad_pre = grad_value * slope_ref[:, at]
        send_ref[:ROWS, at] = grad_pre.astype(BF16)
        first = jnp.sum(grad_pre, axis=0, keepdims=True)
        second = jnp.sum(grad_value * hidden_ref[:, at].astype(F32), axis=0, keepdims=True)
        third = jnp.broadcast_to(total_value, (1, CHUNK))
        rows = stack_rows(three(first) + three(second) + three(third), 16)
        send_ref[ROWS + 48 : ROWS + 64, at] = rows.astype(BF16)
        return carry

    lax.fori_loop(0, H // CHUNK, backward, 0)


PACK = 464
BLOCK = 128


def product_kernel(own_ref, other_ref, keep_ref, out_ref, left_ref):
    for b in range(H // ROWS):
        left_ref[b * 48 : (b + 1) * 48, :] = other_ref[
            ROWS : ROWS + 48, b * ROWS : (b + 1) * ROWS
        ]
    keep = keep_ref[...]
    left = left_ref[...]
    for n in range(H // CHUNK):
        at = slice(n * CHUNK, (n + 1) * CHUNK)
        part = dot(keep, own_ref[:ROWS, at]) + dot(left, other_ref[:ROWS, at])
        for p in range(N_PLANE):
            for i in range(3):
                tile = part[p * SLAB + 8 * i : p * SLAB + 8 * i + 8]
                pair = jnp.concatenate([tile[:, :LANES], tile[:, LANES:]], axis=0)
                start = p * PACK + (16 * i + 2 * n) * 8
                out_ref[start : start + 16, :] = pair.astype(BF16)
    mine = own_ref[ROWS + 48 : ROWS + 64, :].astype(F32)
    theirs = other_ref[ROWS + 48 : ROWS + 64, :].astype(F32)
    rows = []
    for q in range(3):
        a = mine[3 * q : 3 * q + 1] + mine[3 * q + 1 : 3 * q + 2] + mine[3 * q + 2 : 3 * q + 3]
        b = theirs[3 * q : 3 * q + 1] + theirs[3 * q + 1 : 3 * q + 2] + theirs[3 * q + 2 : 3 * q + 3]
        rows.append(two(a + b))
    blocks = []
    for q in range(2):
        for r in rows[q]:
            pieces = [r[:, b * LANES : (b + 1) * LANES] for b in range(H // LANES)]
            blocks.append(jnp.concatenate(pieces, axis=0))
    blocks.append(stack_rows([r[:, :LANES] for r in rows[2]], 16))
    small = jnp.concatenate(blocks, axis=0).astype(BF16)
    for p in range(N_PLANE):
        out_ref[p * PACK + HALF : (p + 1) * PACK, :] = small


def plane_kernel(got_ref, out_ref, sum_ref, wide_ref):
    for b in range(PACK // 16):
        total = got_ref[b * 16 : b * 16 + 16, :].astype(F32)
        for p in range(1, N_PLANE):
            total = total + got_ref[p * PACK + b * 16 : p * PACK + b * 16 + 16, :].astype(F32)
        sum_ref[b * 16 : b * 16 + 16, :] = total
    for n in range(48):
        wide_ref[pl.ds(n, N_LINE, stride=48), :] = sum_ref[8 * n : 8 * n + 8, :]
    last = sum_ref[448:449, :] + sum_ref[449:450, :]
    small = jnp.concatenate(
        two(sum_ref[384:400, :] + sum_ref[400:416, :])
        + two(sum_ref[416:432, :] + sum_ref[432:448, :])
        + (stack_rows(two(last), 16),),
        axis=0,
    ).astype(BF16)
    for z in range(N_LINE):
        out_ref[z * BLOCK : z * BLOCK + 48, :] = wide_ref[z * 48 : z * 48 + 48, :].astype(BF16)
        out_ref[z * BLOCK + 48 : (z + 1) * BLOCK, :] = small


def line_kernel(got_ref, w_ref, b_in_ref, w_out_ref, b_out_ref, sum_ref):
    for b in range(BLOCK // 16):
        total = got_ref[b * 16 : b * 16 + 16, :].astype(F32)
        for z in range(1, N_LINE):
            total = total + got_ref[z * BLOCK + b * 16 : z * BLOCK + b * 16 + 16, :].astype(F32)
        sum_ref[b * 16 : b * 16 + 16, :] = total
    for i in range(3):
        for b in range(H // LANES):
            w_ref[i : i + 1, b * LANES : (b + 1) * LANES] = sum_ref[i * 16 + b : i * 16 + b + 1, :]
    b_in_ref[...] = sum_ref[48:64, :] + sum_ref[64:80, :]
    w_out_ref[...] = sum_ref[80:96, :] + sum_ref[96:112, :]
    b_out_ref[...] = sum_ref[112:113, :] + sum_ref[113:114, :]


def call(kernel, shapes, operands, scratch, flops, grant, in_smem=0, in_hbm=()):
    specs = [pl.BlockSpec(memory_space=pltpu.SMEM)] * in_smem
    specs += [pl.BlockSpec(memory_space=pltpu.VMEM)] * (len(operands) - in_smem)
    for n in in_hbm:
        specs[n] = pl.BlockSpec(memory_space=pltpu.HBM)
    outs = [jax.ShapeDtypeStruct(shape, kind) for shape, kind in shapes]
    return pl.pallas_call(
        kernel,
        out_shape=outs,
        in_specs=specs,
        out_specs=[pl.BlockSpec(memory_space=pltpu.VMEM)] * len(outs),
        scratch_shapes=scratch,
        compiler_params=pltpu.CompilerParams(vmem_limit_bytes=grant << 20),
        cost_estimate=pl.CostEstimate(flops=flops, bytes_accessed=1 << 20, transcendentals=0),
    )(*operands)


def body(state_feats, achieved, offsets, w_in, b_in, w_out, b_out):
    place = jnp.stack([lax.axis_index(TM), lax.axis_index("dp")]).astype(I32)
    table = achieved.reshape(ROWS, G)
    state = state_feats.reshape(ROWS, S)
    many, offs = call(
        spread_kernel,
        [((N_TM, 1, ROWS), I32), ((1, ROWS), I32)],
        (offsets.T,),
        [],
        10**6,
        4,
    )
    known = lax.all_to_all(many, TM, split_axis=0, concat_axis=0, tiled=True)
    (picked,) = call(
        pick_kernel,
        [((N_TM * 16, LANES), BF16)],
        (place, known, table),
        [pltpu.VMEM((N_TM * 16, LANES), F32)],
        10**8,
        6,
        1,
    )
    base, near, at = call(
        ahead_kernel,
        [((ROWS, H), F32), ((ROWS, G), BF16), ((ROWS, LANES), I32)],
        (place, offs, table, state, w_in, b_in.reshape(1, H)),
        [],
        10**9,
        12,
        1,
    )
    fetched = lax.all_to_all(
        picked.reshape(N_TM, 16, LANES), TM, split_axis=0, concat_axis=0, tiled=True
    ).reshape(N_TM * 16, LANES)
    scale = 1.0 / math.sqrt(ROWS * N_TM * 2)
    td, send, keep = call(
        functools.partial(main_kernel, scale),
        [((STEPS, ROWS // STEPS), F32), ((ROWS + 64, H), BF16), ((HALF, ROWS), BF16)],
        (place, b_out, fetched, base, near, at, table, state, w_in, w_out.reshape(1, H)),
        [pltpu.VMEM((ROWS, H), F32), pltpu.VMEM((ROWS, H), BF16), pltpu.VMEM((ROWS, S + G), BF16), pltpu.VMEM((G, H), BF16), pltpu.VMEM((N_TM * 16, LANES), F32), pltpu.SemaphoreType.DMA],
        2 * 10**9,
        48,
        2,
        (8,),
    )
    other = lax.ppermute(send, "dp", [(0, 1), (1, 0)])
    (packs,) = call(
        product_kernel,
        [((N_PLANE * PACK, LANES), BF16)],
        (send, other, keep),
        [pltpu.VMEM((HALF, ROWS), BF16)],
        10**9,
        12,
    )
    got = lax.all_to_all(
        packs.reshape(N_PLANE, PACK, LANES), PLANE, split_axis=0, concat_axis=0, tiled=True
    ).reshape(N_PLANE * PACK, LANES)
    (lines,) = call(
        plane_kernel,
        [((N_LINE * BLOCK, LANES), BF16)],
        (got,),
        [pltpu.VMEM((PACK, LANES), F32), pltpu.VMEM((N_LINE * 48, LANES), F32)],
        10**7,
        6,
    )
    got = lax.all_to_all(
        lines.reshape(N_LINE, BLOCK, LANES), LINE, split_axis=0, concat_axis=0, tiled=True
    ).reshape(N_LINE * BLOCK, LANES)
    grad_w_in, grad_b_in, grad_w_out, grad_b_out = call(
        line_kernel,
        [((3, H), F32), ((16, LANES), F32), ((16, LANES), F32), ((1, LANES), F32)],
        (got,),
        [pltpu.VMEM((BLOCK, LANES), F32)],
        10**6,
        4,
    )
    return td.T, grad_w_in, grad_b_in.reshape(H), grad_w_out.reshape(H), grad_b_out[0, :1]


def solution(mesh):
    split = Mesh(mesh.devices.reshape(4, 4, 8, mesh.shape["dp"]), TM_DP)
    placed = (P("dp", TM, None), P("dp", TM, None), P("dp", TM), P(), P(), P(), P())
    return jax.shard_map(
        body,
        mesh=split,
        in_specs=placed,
        out_specs=(P("dp", TM), P(TM_DP, None), P(), P(), P()),
        check_vma=False,
    )
```

```python
import functools
import math

import jax
import jax.numpy as jnp
from jax import lax
from jax.experimental import pallas as pl
from jax.experimental.pallas import tpu as pltpu
from jax.sharding import Mesh
from jax.sharding import PartitionSpec as P

CAP = 4
TM = ("tm_0", "tm_1", "tm_2")
TM_DP = ("tm_0", "tm_1", "tm_2", "dp")
PLANE = ("tm_0", "tm_1")
LINE = "tm_2"
N_TM = 128
N_PLANE = 16
N_LINE = 8
ROWS = 256
STEPS = 4
S = 256
G = 512
H = 2048
LANES = 128
HALF = (S + G) // 2
SLAB = HALF // N_PLANE
CHUNK = 256
F32 = jnp.float32
BF16 = jnp.bfloat16
I32 = jnp.int32


def iota(shape, dim):
    return lax.broadcasted_iota(I32, shape, dim)


def dot(a, b, dims=(((1,), (0,)), ((), ()))):
    return lax.dot_general(a, b, dims, preferred_element_type=F32)


def flag(mask):
    return jnp.where(mask, 1.0, 0.0)


def spread_kernel(offs_ref, many_ref, row_ref):
    offs = offs_ref[...]
    parts = jnp.concatenate([offs >> 4, offs & 15], axis=0).astype(F32).astype(BF16)
    episode = flag((iota((ROWS // STEPS, ROWS), 1) >> 2) == iota((ROWS // STEPS, ROWS), 0))
    wide = dot(parts, episode.astype(BF16))
    step = iota((2 * STEPS, ROWS), 1) & (STEPS - 1)
    which = iota((2 * STEPS, ROWS), 0)
    mine = (which & (STEPS - 1)) == step
    weight = jnp.where(which < STEPS, 16.0, 1.0)
    row = jnp.sum(jnp.where(mine, wide * weight, 0.0), axis=0, keepdims=True).astype(I32)
    row_ref[...] = row
    many_ref[...] = jnp.broadcast_to(row[None], (N_TM, 1, ROWS))


def pick_kernel(place_ref, offs_ref, table_ref, out_ref, wide_ref):
    me = place_ref[0:1, 0:1]
    offs = offs_ref[...].reshape(N_TM, ROWS)
    peer = iota((N_TM, ROWS), 0)
    row = iota((N_TM, ROWS), 1)
    target = peer * STEPS + (row & (STEPS - 1)) + offs
    hit = ((target >> 2) == me) & (peer != me)
    earlier = flag(iota((ROWS, ROWS), 0) < iota((ROWS, ROWS), 1)).astype(BF16)
    rank = dot(flag(hit).astype(BF16), earlier)
    position = ((row - (row & (STEPS - 1))) + (target & (STEPS - 1)) + 1).astype(F32)
    table = table_ref[...]
    for c in range(CAP):
        place = jnp.sum(
            jnp.where(hit & (rank == float(c)), position, 0.0), axis=1, keepdims=True
        )
        wanted = flag(row.astype(F32) + 1.0 == place).astype(BF16)
        picked = dot(wanted, table)
        for j in range(G // LANES):
            wide_ref[pl.ds(c * (G // LANES) + j, N_TM, stride=16), :] = picked[
                :, j * LANES : (j + 1) * LANES
            ]
    out_ref[...] = wide_ref[...].astype(BF16)


def half_rows(core):
    k = iota((HALF, S + G), 0)
    eighth = k >> 3
    plane = (eighth * 171) >> 9
    within = eighth - plane * 3
    feature = (plane * N_LINE + (k & 7)) * 6 + core * 3 + within
    return flag(iota((HALF, S + G), 1) == feature).astype(BF16)


def three(x):
    high = x.astype(BF16).astype(F32)
    rest = x - high
    middle = rest.astype(BF16).astype(F32)
    return high, middle, rest - middle


def two(x):
    high = x.astype(BF16).astype(F32)
    return high, x - high


def stack_rows(rows, count):
    width = rows[0].shape[1]
    at = iota((count, width), 0)
    total = jnp.zeros((count, width), F32)
    for n, r in enumerate(rows):
        total = jnp.where(at == n, jnp.broadcast_to(r, (count, width)), total)
    return total


def ahead_kernel(
    place_ref,
    offs_ref,
    table_ref,
    state_ref,
    w_in_ref,
    b_in_ref,
    base_ref,
    near_ref,
    at_ref,
):
    me = place_ref[0:1, 0:1]
    row = iota((ROWS, ROWS), 1)
    col = iota((ROWS, ROWS), 0)
    lane = iota((1, ROWS), 1)
    target = me * STEPS + (lane & (STEPS - 1)) + offs_ref[...]
    owner_lane = (target >> 2).astype(F32)
    position_lane = ((lane - (lane & (STEPS - 1))) + (target & (STEPS - 1))).astype(F32)

    def to_column(x):
        return jnp.sum(
            jnp.where(row == col, jnp.broadcast_to(x, (ROWS, ROWS)), 0.0),
            axis=1,
            keepdims=True,
        )

    owner = to_column(owner_lane)
    position = to_column(position_lane)
    slot = jnp.sum(flag((owner == owner_lane) & (row < col)), axis=1, keepdims=True)
    remote = owner != me.astype(F32)
    near_at = jnp.where(remote, -1.0, position)
    far_at = jnp.where(remote, owner * float(CAP) + slot, -1.0).astype(I32)
    near = flag(row.astype(F32) == near_at).astype(BF16)
    near_ref[...] = dot(near, table_ref[...]).astype(BF16)
    at_ref[...] = jnp.broadcast_to(far_at, (ROWS, LANES))
    state = state_ref[...]

    def step(n, carry):
        at = pl.ds(pl.multiple_of(n * CHUNK, CHUNK), CHUNK)
        base_ref[:, at] = dot(state, w_in_ref[:S, at]) + b_in_ref[:, at]
        return carry

    lax.fori_loop(0, H // CHUNK, step, 0)


def main_kernel(
    scale,
    place_ref,
    b_out_ref,
    fetched_ref,
    base_ref,
    near_ref,
    at_ref,
    table_ref,
    state_ref,
    w_in_ref,
    w_out_ref,
    td_ref,
    send_ref,
    keep_ref,
    slope_ref,
    hidden_ref,
    inputs_ref,
    goal_w_ref,
    wide_ref,
    total_ref,
    sems,
):
    def load(n):
        at = pl.ds(pl.multiple_of(n * CHUNK, CHUNK), CHUNK)
        return pltpu.make_async_copy(
            w_in_ref.at[pl.ds(S, G), at], goal_w_ref.at[:, at], sems.at[n]
        )

    for n in range(H // CHUNK):
        load(n).start()
    core = place_ref[1:2, 0:1]
    far_at = at_ref[:, 0:1]
    far = flag(iota((ROWS, N_TM * CAP), 1) == far_at).astype(BF16)
    inputs_ref[:, :S] = state_ref[...]
    wide_ref[...] = fetched_ref[...].astype(F32)
    gap = jnp.zeros((ROWS, LANES), F32)
    for j in range(G // LANES):
        at = slice(j * LANES, (j + 1) * LANES)
        fetched = wide_ref[pl.ds(j, N_TM * CAP, stride=G // LANES), :].astype(BF16)
        goal = dot(far, fetched) + near_ref[:, at].astype(F32)
        diff = table_ref[:, at].astype(F32) - goal
        gap = gap + diff * diff
        inputs_ref[:, S + j * LANES : S + (j + 1) * LANES] = goal.astype(BF16)
    reward = -(jnp.sum(gap, axis=1, keepdims=True) * (1.0 / G))
    inputs = inputs_ref[...]
    total_ref[...] = jnp.zeros((ROWS, LANES), F32)

    def forward(n, carry):
        at = pl.ds(pl.multiple_of(n * CHUNK, CHUNK), CHUNK)
        load(n).wait()
        pre = base_ref[:, at] + dot(inputs[:, S:], goal_w_ref[:, at])
        sig = 1.0 / (1.0 + jnp.exp(-pre))
        head = w_out_ref[:, at]
        act = pre * sig
        hidden = act.astype(BF16)
        hidden_ref[:, at] = hidden
        slope_ref[:, at] = head * (sig + act * (1.0 - sig))
        term = hidden.astype(F32) * head
        total_ref[...] += term[:, :LANES] + term[:, LANES:]
        return carry

    lax.fori_loop(0, H // CHUNK, forward, 0)
    value = jnp.sum(total_ref[...], axis=1, keepdims=True) + b_out_ref[:, 0:1]
    error = value - reward
    grad_value = error * scale

    each = (STEPS * iota((ROWS, ROWS // STEPS), 1)) - iota((ROWS, ROWS // STEPS), 0)
    for s in range(STEPS):
        td_ref[s : s + 1, :] = jnp.sum(
            jnp.where(each + s == 0, error, 0.0), axis=0, keepdims=True
        )

    kept = dot(half_rows(core), inputs, (((1,), (1,)), ((), ())))
    keep_ref[...] = kept.astype(BF16)
    sent = dot(half_rows(1 - core), inputs, (((1,), (1,)), ((), ()))).astype(BF16)
    for b in range(H // ROWS):
        send_ref[ROWS : ROWS + 48, b * ROWS : (b + 1) * ROWS] = sent[b * 48 : (b + 1) * 48, :]

    total_value = jnp.sum(grad_value, axis=0, keepdims=True)

    def backward(n, carry):
        at = pl.ds(pl.multiple_of(n * CHUNK, CHUNK), CHUNK)
        grad_pre = grad_value * slope_ref[:, at]
        send_ref[:ROWS, at] = grad_pre.astype(BF16)
        first = jnp.sum(grad_pre, axis=0, keepdims=True)
        second = jnp.sum(grad_value * hidden_ref[:, at].astype(F32), axis=0, keepdims=True)
        third = jnp.broadcast_to(total_value, (1, CHUNK))
        rows = stack_rows(three(first) + three(second) + three(third), 16)
        send_ref[ROWS + 48 : ROWS + 64, at] = rows.astype(BF16)
        return carry

    lax.fori_loop(0, H // CHUNK, backward, 0)


PACK = 464
BLOCK = 128


def product_kernel(own_ref, other_ref, keep_ref, out_ref, left_ref):
    for b in range(H // ROWS):
        left_ref[b * 48 : (b + 1) * 48, :] = other_ref[
            ROWS : ROWS + 48, b * ROWS : (b + 1) * ROWS
        ]
    keep = keep_ref[...]
    left = left_ref[...]
    for n in range(H // CHUNK):
        at = slice(n * CHUNK, (n + 1) * CHUNK)
        part = dot(keep, own_ref[:ROWS, at]) + dot(left, other_ref[:ROWS, at])
        for p in range(N_PLANE):
            for i in range(3):
                tile = part[p * SLAB + 8 * i : p * SLAB + 8 * i + 8]
                pair = jnp.concatenate([tile[:, :LANES], tile[:, LANES:]], axis=0)
                start = p * PACK + (16 * i + 2 * n) * 8
                out_ref[start : start + 16, :] = pair.astype(BF16)
    mine = own_ref[ROWS + 48 : ROWS + 64, :].astype(F32)
    theirs = other_ref[ROWS + 48 : ROWS + 64, :].astype(F32)
    rows = []
    for q in range(3):
        a = mine[3 * q : 3 * q + 1] + mine[3 * q + 1 : 3 * q + 2] + mine[3 * q + 2 : 3 * q + 3]
        b = theirs[3 * q : 3 * q + 1] + theirs[3 * q + 1 : 3 * q + 2] + theirs[3 * q + 2 : 3 * q + 3]
        rows.append(two(a + b))
    blocks = []
    for q in range(2):
        for r in rows[q]:
            pieces = [r[:, b * LANES : (b + 1) * LANES] for b in range(H // LANES)]
            blocks.append(jnp.concatenate(pieces, axis=0))
    blocks.append(stack_rows([r[:, :LANES] for r in rows[2]], 16))
    small = jnp.concatenate(blocks, axis=0).astype(BF16)
    for p in range(N_PLANE):
        out_ref[p * PACK + HALF : (p + 1) * PACK, :] = small


def plane_kernel(got_ref, out_ref, sum_ref, wide_ref):
    for b in range(PACK // 16):
        total = got_ref[b * 16 : b * 16 + 16, :].astype(F32)
        for p in range(1, N_PLANE):
            total = total + got_ref[p * PACK + b * 16 : p * PACK + b * 16 + 16, :].astype(F32)
        sum_ref[b * 16 : b * 16 + 16, :] = total
    for n in range(48):
        wide_ref[pl.ds(n, N_LINE, stride=48), :] = sum_ref[8 * n : 8 * n + 8, :]
    last = sum_ref[448:449, :] + sum_ref[449:450, :]
    small = jnp.concatenate(
        two(sum_ref[384:400, :] + sum_ref[400:416, :])
        + two(sum_ref[416:432, :] + sum_ref[432:448, :])
        + (stack_rows(two(last), 16),),
        axis=0,
    ).astype(BF16)
    for z in range(N_LINE):
        out_ref[z * BLOCK : z * BLOCK + 48, :] = wide_ref[z * 48 : z * 48 + 48, :].astype(BF16)
        out_ref[z * BLOCK + 48 : (z + 1) * BLOCK, :] = small


def line_kernel(got_ref, w_ref, b_in_ref, w_out_ref, b_out_ref, sum_ref):
    for b in range(BLOCK // 16):
        total = got_ref[b * 16 : b * 16 + 16, :].astype(F32)
        for z in range(1, N_LINE):
            total = total + got_ref[z * BLOCK + b * 16 : z * BLOCK + b * 16 + 16, :].astype(F32)
        sum_ref[b * 16 : b * 16 + 16, :] = total
    for i in range(3):
        for b in range(H // LANES):
            w_ref[i : i + 1, b * LANES : (b + 1) * LANES] = sum_ref[i * 16 + b : i * 16 + b + 1, :]
    b_in_ref[...] = sum_ref[48:64, :] + sum_ref[64:80, :]
    w_out_ref[...] = sum_ref[80:96, :] + sum_ref[96:112, :]
    b_out_ref[...] = sum_ref[112:113, :] + sum_ref[113:114, :]


def call(kernel, shapes, operands, scratch, flops, grant, in_hbm=()):
    specs = [pl.BlockSpec(memory_space=pltpu.VMEM)] * len(operands)
    for n in in_hbm:
        specs[n] = pl.BlockSpec(memory_space=pltpu.HBM)
    outs = [jax.ShapeDtypeStruct(shape, kind) for shape, kind in shapes]
    return pl.pallas_call(
        kernel,
        out_shape=outs,
        in_specs=specs,
        out_specs=[pl.BlockSpec(memory_space=pltpu.VMEM)] * len(outs),
        scratch_shapes=scratch,
        compiler_params=pltpu.CompilerParams(vmem_limit_bytes=grant << 20),
        cost_estimate=pl.CostEstimate(flops=flops, bytes_accessed=1 << 20, transcendentals=0),
    )(*operands)


def body(state_feats, achieved, offsets, w_in, b_in, w_out, b_out):
    place = jnp.stack([lax.axis_index(TM), lax.axis_index("dp")]).astype(I32)
    place = jnp.broadcast_to(place[:, None], (2, LANES))
    table = achieved.reshape(ROWS, G)
    state = state_feats.reshape(ROWS, S)
    many, offs = call(
        spread_kernel,
        [((N_TM, 1, ROWS), I32), ((1, ROWS), I32)],
        (offsets.T,),
        [],
        10**6,
        4,
    )
    known = lax.all_to_all(many, TM, split_axis=0, concat_axis=0, tiled=True)
    (picked,) = call(
        pick_kernel,
        [((N_TM * 16, LANES), BF16)],
        (place, known, table),
        [pltpu.VMEM((N_TM * 16, LANES), F32)],
        10**8,
        6,
    )
    base, near, at = call(
        ahead_kernel,
        [((ROWS, H), F32), ((ROWS, G), BF16), ((ROWS, LANES), I32)],
        (place, offs, table, state, w_in, b_in.reshape(1, H)),
        [],
        10**9,
        12,
    )
    fetched = lax.all_to_all(
        picked.reshape(N_TM, 16, LANES), TM, split_axis=0, concat_axis=0, tiled=True
    ).reshape(N_TM * 16, LANES)
    head_bias = jnp.broadcast_to(b_out[None], (1, LANES))
    scale = 1.0 / math.sqrt(ROWS * N_TM * 2)
    td, send, keep = call(
        functools.partial(main_kernel, scale),
        [((STEPS, ROWS // STEPS), F32), ((ROWS + 64, H), BF16), ((HALF, ROWS), BF16)],
        (place, head_bias, fetched, base, near, at, table, state, w_in, w_out.reshape(1, H)),
        [pltpu.VMEM((ROWS, H), F32), pltpu.VMEM((ROWS, H), BF16), pltpu.VMEM((ROWS, S + G), BF16), pltpu.VMEM((G, H), BF16), pltpu.VMEM((N_TM * 16, LANES), F32), pltpu.VMEM((ROWS, LANES), F32), pltpu.SemaphoreType.DMA((H // CHUNK,))],
        2 * 10**9,
        48,
        (8,),
    )
    other = lax.ppermute(send, "dp", [(0, 1), (1, 0)])
    (packs,) = call(
        product_kernel,
        [((N_PLANE * PACK, LANES), BF16)],
        (send, other, keep),
        [pltpu.VMEM((HALF, ROWS), BF16)],
        10**9,
        12,
    )
    got = lax.all_to_all(
        packs.reshape(N_PLANE, PACK, LANES), PLANE, split_axis=0, concat_axis=0, tiled=True
    ).reshape(N_PLANE * PACK, LANES)
    (lines,) = call(
        plane_kernel,
        [((N_LINE * BLOCK, LANES), BF16)],
        (got,),
        [pltpu.VMEM((PACK, LANES), F32), pltpu.VMEM((N_LINE * 48, LANES), F32)],
        10**7,
        6,
    )
    got = lax.all_to_all(
        lines.reshape(N_LINE, BLOCK, LANES), LINE, split_axis=0, concat_axis=0, tiled=True
    ).reshape(N_LINE * BLOCK, LANES)
    grad_w_in, grad_b_in, grad_w_out, grad_b_out = call(
        line_kernel,
        [((3, H), F32), ((16, LANES), F32), ((16, LANES), F32), ((1, LANES), F32)],
        (got,),
        [pltpu.VMEM((BLOCK, LANES), F32)],
        10**6,
        4,
    )
    return td.T, grad_w_in, grad_b_in.reshape(H), grad_w_out.reshape(H), grad_b_out[0, :1]


def solution(mesh):
    split = Mesh(mesh.devices.reshape(4, 4, 8, mesh.shape["dp"]), TM_DP)
    placed = (P("dp", TM, None), P("dp", TM, None), P("dp", TM), P(), P(), P(), P())
    return jax.shard_map(
        body,
        mesh=split,
        in_specs=placed,
        out_specs=(P("dp", TM), P(TM_DP, None), P(), P(), P()),
        check_vma=False,
    )
```

```python
import functools
import math

import jax
import jax.numpy as jnp
from jax import lax
from jax.experimental import pallas as pl
from jax.experimental.pallas import tpu as pltpu
from jax.sharding import Mesh
from jax.sharding import PartitionSpec as P

CAP = 4
TM = ("tm_0", "tm_1", "tm_2")
TM_DP = ("tm_0", "tm_1", "tm_2", "dp")
PLANE = ("tm_0", "tm_1")
LINE = "tm_2"
N_TM = 128
N_PLANE = 16
N_LINE = 8
ROWS = 256
STEPS = 4
S = 256
G = 512
H = 2048
LANES = 128
HALF = (S + G) // 2
SLAB = HALF // N_PLANE
CHUNK = 256
F32 = jnp.float32
BF16 = jnp.bfloat16
I32 = jnp.int32


def iota(shape, dim):
    return lax.broadcasted_iota(I32, shape, dim)


def dot(a, b, dims=(((1,), (0,)), ((), ()))):
    return lax.dot_general(a, b, dims, preferred_element_type=F32)


def flag(mask):
    return jnp.where(mask, 1.0, 0.0)


def spread_kernel(offs_ref, many_ref, row_ref):
    offs = offs_ref[...]
    parts = jnp.concatenate([offs >> 4, offs & 15], axis=0).astype(F32).astype(BF16)
    episode = flag((iota((ROWS // STEPS, ROWS), 1) >> 2) == iota((ROWS // STEPS, ROWS), 0))
    wide = dot(parts, episode.astype(BF16))
    step = iota((2 * STEPS, ROWS), 1) & (STEPS - 1)
    which = iota((2 * STEPS, ROWS), 0)
    mine = (which & (STEPS - 1)) == step
    weight = jnp.where(which < STEPS, 16.0, 1.0)
    row = jnp.sum(jnp.where(mine, wide * weight, 0.0), axis=0, keepdims=True).astype(I32)
    row_ref[...] = row
    many_ref[...] = jnp.broadcast_to(row[None], (N_TM, 1, ROWS))


def pick_kernel(place_ref, offs_ref, table_ref, out_ref, wide_ref, ready_ref, sems):
    me = place_ref[0:1, 0:1]
    offs = offs_ref[...].reshape(N_TM, ROWS)
    peer = iota((N_TM, ROWS), 0)
    row = iota((N_TM, ROWS), 1)
    target = peer * STEPS + (row & (STEPS - 1)) + offs
    hit = ((target >> 2) == me) & (peer != me)
    earlier = flag(iota((ROWS, ROWS), 0) < iota((ROWS, ROWS), 1)).astype(BF16)
    rank = dot(flag(hit).astype(BF16), earlier)
    position = ((row - (row & (STEPS - 1))) + (target & (STEPS - 1)) + 1).astype(F32)
    wanted = []
    for c in range(CAP):
        place = jnp.sum(
            jnp.where(hit & (rank == float(c)), position, 0.0), axis=1, keepdims=True
        )
        wanted.append(flag(row.astype(F32) + 1.0 == place).astype(BF16))
    half = N_TM // 2
    copies = []
    for h in range(2):
        part = jnp.concatenate([w[h * half : (h + 1) * half] for w in wanted], axis=0)
        picked = dot(part, table_ref[...])
        for c in range(CAP):
            for j in range(G // LANES):
                at = pl.ds(h * half * 16 + c * (G // LANES) + j, half, stride=16)
                wide_ref[at, :] = picked[
                    c * half : (c + 1) * half, j * LANES : (j + 1) * LANES
                ]
        rows = slice(h * half * 16, (h + 1) * half * 16)
        ready_ref[rows, :] = wide_ref[rows, :].astype(BF16)
        there = pl.ds(h * half * 16, half * 16)
        copies.append(
            pltpu.make_async_copy(ready_ref.at[there, :], out_ref.at[there, :], sems.at[h])
        )
        copies[-1].start()
    for copy in copies:
        copy.wait()


def half_rows(core):
    k = iota((HALF, S + G), 0)
    eighth = k >> 3
    plane = (eighth * 171) >> 9
    within = eighth - plane * 3
    feature = (plane * N_LINE + (k & 7)) * 6 + core * 3 + within
    return flag(iota((HALF, S + G), 1) == feature).astype(BF16)


def three(x):
    high = x.astype(BF16).astype(F32)
    rest = x - high
    middle = rest.astype(BF16).astype(F32)
    return high, middle, rest - middle


def two(x):
    high = x.astype(BF16).astype(F32)
    return high, x - high


def stack_rows(rows, count):
    width = rows[0].shape[1]
    at = iota((count, width), 0)
    total = jnp.zeros((count, width), F32)
    for n, r in enumerate(rows):
        total = jnp.where(at == n, jnp.broadcast_to(r, (count, width)), total)
    return total


def ahead_kernel(
    place_ref,
    offs_ref,
    table_ref,
    w_in_ref,
    goal_w_ref,
    near_ref,
    at_ref,
):
    me = place_ref[0:1, 0:1]
    row = iota((ROWS, ROWS), 1)
    col = iota((ROWS, ROWS), 0)
    lane = iota((1, ROWS), 1)
    target = me * STEPS + (lane & (STEPS - 1)) + offs_ref[...]
    owner_lane = (target >> 2).astype(F32)
    position_lane = ((lane - (lane & (STEPS - 1))) + (target & (STEPS - 1))).astype(F32)

    def to_column(x):
        return jnp.sum(
            jnp.where(row == col, jnp.broadcast_to(x, (ROWS, ROWS)), 0.0),
            axis=1,
            keepdims=True,
        )

    owner = to_column(owner_lane)
    position = to_column(position_lane)
    slot = jnp.sum(flag((owner == owner_lane) & (row < col)), axis=1, keepdims=True)
    remote = owner != me.astype(F32)
    near_at = jnp.where(remote, -1.0, position)
    far_at = jnp.where(remote, owner * float(CAP) + slot, -1.0).astype(I32)
    near = flag(row.astype(F32) == near_at).astype(BF16)
    near_ref[...] = dot(near, table_ref[...]).astype(BF16)
    at_ref[...] = jnp.broadcast_to(far_at, (ROWS, LANES))
    goal_w_ref[...] = w_in_ref[S:, :]


def main_kernel(
    scale,
    place_ref,
    b_out_ref,
    fetched_ref,
    goal_w_ref,
    near_ref,
    at_ref,
    table_ref,
    state_ref,
    w_in_ref,
    b_in_ref,
    w_out_ref,
    td_ref,
    send_ref,
    keep_ref,
    slope_ref,
    hidden_ref,
    inputs_ref,
    state_w_ref,
    wide_ref,
    total_ref,
    td_rows_ref,
    sems,
    td_sem,
):
    def load(n):
        at = pl.ds(pl.multiple_of(n * CHUNK, CHUNK), CHUNK)
        return pltpu.make_async_copy(
            w_in_ref.at[pl.ds(0, S), at], state_w_ref.at[:, at], sems.at[n]
        )

    def begin(n, carry):
        load(n).start()
        return carry

    lax.fori_loop(0, H // CHUNK, begin, 0)
    core = place_ref[1:2, 0:1]
    far_at = at_ref[:, 0:1]
    far = flag(iota((ROWS, N_TM * CAP), 1) == far_at).astype(BF16)
    inputs_ref[:, :S] = state_ref[...]
    wide_ref[...] = fetched_ref[...].astype(F32)
    gap = jnp.zeros((ROWS, LANES), F32)
    for j in range(G // LANES):
        at = slice(j * LANES, (j + 1) * LANES)
        fetched = wide_ref[pl.ds(j, N_TM * CAP, stride=G // LANES), :].astype(BF16)
        goal = dot(far, fetched) + near_ref[:, at].astype(F32)
        diff = table_ref[:, at].astype(F32) - goal
        gap = gap + diff * diff
        inputs_ref[:, S + j * LANES : S + (j + 1) * LANES] = goal.astype(BF16)
    reward = -(jnp.sum(gap, axis=1, keepdims=True) * (1.0 / G))
    inputs = inputs_ref[...]
    total_ref[...] = jnp.zeros((ROWS, LANES), F32)

    def forward(n, carry):
        at = pl.ds(pl.multiple_of(n * CHUNK, CHUNK), CHUNK)
        load(n).wait()
        pre = dot(inputs[:, :S], state_w_ref[:, at]) + dot(inputs[:, S:], goal_w_ref[:, at])
        pre = pre + b_in_ref[:, at]
        sig = 1.0 / (1.0 + jnp.exp(-pre))
        head = w_out_ref[:, at]
        act = pre * sig
        hidden = act.astype(BF16)
        hidden_ref[:, at] = hidden
        slope_ref[:, at] = head * (sig + act * (1.0 - sig))
        term = hidden.astype(F32) * head
        total_ref[...] += term[:, :LANES] + term[:, LANES:]
        return carry

    lax.fori_loop(0, H // CHUNK, forward, 0)
    value = jnp.sum(total_ref[...], axis=1, keepdims=True) + b_out_ref[:, 0:1]
    error = value - reward
    grad_value = error * scale

    each = (STEPS * iota((ROWS, ROWS // STEPS), 1)) - iota((ROWS, ROWS // STEPS), 0)
    for s in range(STEPS):
        td_rows_ref[s : s + 1, :] = jnp.sum(
            jnp.where(each + s == 0, error, 0.0), axis=0, keepdims=True
        )

    td_copy = pltpu.make_async_copy(td_rows_ref, td_ref, td_sem)
    td_copy.start()

    kept = dot(half_rows(core), inputs, (((1,), (1,)), ((), ())))
    keep_ref[...] = kept.astype(BF16)
    sent = dot(half_rows(1 - core), inputs, (((1,), (1,)), ((), ()))).astype(BF16)
    for b in range(H // ROWS):
        send_ref[ROWS : ROWS + 48, b * ROWS : (b + 1) * ROWS] = sent[b * 48 : (b + 1) * 48, :]

    total_value = jnp.sum(grad_value, axis=0, keepdims=True)

    def backward(n, carry):
        at = pl.ds(pl.multiple_of(n * CHUNK, CHUNK), CHUNK)
        grad_pre = grad_value * slope_ref[:, at]
        send_ref[:ROWS, at] = grad_pre.astype(BF16)
        first = jnp.sum(grad_pre, axis=0, keepdims=True)
        second = jnp.sum(grad_value * hidden_ref[:, at].astype(F32), axis=0, keepdims=True)
        third = jnp.broadcast_to(total_value, (1, CHUNK))
        rows = stack_rows(three(first) + three(second) + three(third), 16)
        send_ref[ROWS + 48 : ROWS + 64, at] = rows.astype(BF16)
        return carry

    lax.fori_loop(0, H // CHUNK, backward, 0)
    td_copy.wait()


PACK = 432
BLOCK = 128


def product_kernel(own_ref, other_ref, keep_ref, out_ref, left_ref):
    for b in range(H // ROWS):
        left_ref[b * 48 : (b + 1) * 48, :] = other_ref[
            ROWS : ROWS + 48, b * ROWS : (b + 1) * ROWS
        ]
    keep = keep_ref[...]
    left = left_ref[...]
    for n in range(H // CHUNK):
        at = slice(n * CHUNK, (n + 1) * CHUNK)
        part = dot(keep, own_ref[:ROWS, at]) + dot(left, other_ref[:ROWS, at])
        for p in range(N_PLANE):
            for i in range(3):
                tile = part[p * SLAB + 8 * i : p * SLAB + 8 * i + 8]
                pair = jnp.concatenate([tile[:, :LANES], tile[:, LANES:]], axis=0)
                start = p * PACK + (16 * i + 2 * n) * 8
                out_ref[start : start + 16, :] = pair.astype(BF16)
    mine = own_ref[ROWS + 48 : ROWS + 64, :].astype(F32)
    theirs = other_ref[ROWS + 48 : ROWS + 64, :].astype(F32)
    rows = []
    for q in range(3):
        a = mine[3 * q : 3 * q + 1] + mine[3 * q + 1 : 3 * q + 2] + mine[3 * q + 2 : 3 * q + 3]
        b = theirs[3 * q : 3 * q + 1] + theirs[3 * q + 1 : 3 * q + 2] + theirs[3 * q + 2 : 3 * q + 3]
        rows.append(a + b)
    blocks = []
    for r in rows[:2]:
        pieces = [r[:, b * LANES : (b + 1) * LANES] for b in range(H // LANES)]
        blocks.append(jnp.concatenate(pieces, axis=0))
    blocks.append(stack_rows(two(rows[2][:, :LANES]), 16))
    small = jnp.concatenate(blocks, axis=0).astype(BF16)
    for p in range(N_PLANE):
        out_ref[p * PACK + HALF : (p + 1) * PACK, :] = small


def plane_kernel(got_ref, out_ref, sum_ref, wide_ref):
    for b in range(PACK // 16):
        total = got_ref[b * 16 : b * 16 + 16, :].astype(F32)
        for p in range(1, N_PLANE):
            total = total + got_ref[p * PACK + b * 16 : p * PACK + b * 16 + 16, :].astype(F32)
        sum_ref[b * 16 : b * 16 + 16, :] = total
    for n in range(48):
        wide_ref[pl.ds(n, N_LINE, stride=48), :] = sum_ref[8 * n : 8 * n + 8, :]
    last = sum_ref[416:417, :] + sum_ref[417:418, :]
    small = jnp.concatenate(
        two(sum_ref[384:400, :]) + two(sum_ref[400:416, :]) + (stack_rows(two(last), 16),),
        axis=0,
    ).astype(BF16)
    for z in range(N_LINE):
        out_ref[z * BLOCK : z * BLOCK + 48, :] = wide_ref[z * 48 : z * 48 + 48, :].astype(BF16)
        out_ref[z * BLOCK + 48 : (z + 1) * BLOCK, :] = small


def line_kernel(got_ref, w_ref, b_in_ref, w_out_ref, b_out_ref, sum_ref):
    for b in range(BLOCK // 16):
        total = got_ref[b * 16 : b * 16 + 16, :].astype(F32)
        for z in range(1, N_LINE):
            total = total + got_ref[z * BLOCK + b * 16 : z * BLOCK + b * 16 + 16, :].astype(F32)
        sum_ref[b * 16 : b * 16 + 16, :] = total
    for i in range(3):
        for b in range(H // LANES):
            w_ref[i : i + 1, b * LANES : (b + 1) * LANES] = sum_ref[i * 16 + b : i * 16 + b + 1, :]
    b_in_ref[...] = sum_ref[48:64, :] + sum_ref[64:80, :]
    w_out_ref[...] = sum_ref[80:96, :] + sum_ref[96:112, :]
    b_out_ref[...] = sum_ref[112:113, :] + sum_ref[113:114, :]


def call(kernel, shapes, operands, scratch, flops, grant, in_hbm=(), out_hbm=()):
    specs = [pl.BlockSpec(memory_space=pltpu.VMEM)] * len(operands)
    for n in in_hbm:
        specs[n] = pl.BlockSpec(memory_space=pltpu.HBM)
    back = [pl.BlockSpec(memory_space=pltpu.VMEM)] * len(shapes)
    for n in out_hbm:
        back[n] = pl.BlockSpec(memory_space=pltpu.HBM)
    outs = [jax.ShapeDtypeStruct(shape, kind) for shape, kind in shapes]
    return pl.pallas_call(
        kernel,
        out_shape=outs,
        in_specs=specs,
        out_specs=back,
        scratch_shapes=scratch,
        compiler_params=pltpu.CompilerParams(vmem_limit_bytes=grant << 20),
        cost_estimate=pl.CostEstimate(flops=flops, bytes_accessed=1 << 20, transcendentals=0),
    )(*operands)


def body(state_feats, achieved, offsets, w_in, b_in, w_out, b_out):
    place = jnp.stack([lax.axis_index(TM), lax.axis_index("dp")]).astype(I32)
    place = jnp.broadcast_to(place[:, None], (2, LANES))
    table = achieved.reshape(ROWS, G)
    state = state_feats.reshape(ROWS, S)
    many, offs = call(
        spread_kernel,
        [((N_TM, 1, ROWS), I32), ((1, ROWS), I32)],
        (offsets.T,),
        [],
        10**6,
        4,
    )
    known = lax.all_to_all(many, TM, split_axis=0, concat_axis=0, tiled=True)
    (picked,) = call(
        pick_kernel,
        [((N_TM * 16, LANES), BF16)],
        (place, known, table),
        [
            pltpu.VMEM((N_TM * 16, LANES), F32),
            pltpu.VMEM((N_TM * 16, LANES), BF16),
            pltpu.SemaphoreType.DMA((2,)),
        ],
        10**8,
        8,
        (),
        (0,),
    )
    goal_w, near, at = call(
        ahead_kernel,
        [((G, H), BF16), ((ROWS, G), BF16), ((ROWS, LANES), I32)],
        (place, offs, table, w_in),
        [],
        10**9,
        12,
    )
    fetched = lax.all_to_all(
        picked.reshape(N_TM, 16, LANES), TM, split_axis=0, concat_axis=0, tiled=True
    ).reshape(N_TM * 16, LANES)
    head_bias = jnp.broadcast_to(b_out[None], (1, LANES))
    scale = 1.0 / math.sqrt(ROWS * N_TM * 2)
    td, send, keep = call(
        functools.partial(main_kernel, scale),
        [((STEPS, ROWS // STEPS), F32), ((ROWS + 64, H), BF16), ((HALF, ROWS), BF16)],
        (
            place,
            head_bias,
            fetched,
            goal_w,
            near,
            at,
            table,
            state,
            w_in,
            b_in.reshape(1, H),
            w_out.reshape(1, H),
        ),
        [
            pltpu.VMEM((ROWS, H), F32),
            pltpu.VMEM((ROWS, H), BF16),
            pltpu.VMEM((ROWS, S + G), BF16),
            pltpu.VMEM((S, H), BF16),
            pltpu.VMEM((N_TM * 16, LANES), F32),
            pltpu.VMEM((ROWS, LANES), F32),
            pltpu.VMEM((STEPS, ROWS // STEPS), F32),
            pltpu.SemaphoreType.DMA((H // CHUNK,)),
            pltpu.SemaphoreType.DMA,
        ],
        2 * 10**9,
        48,
        (8,),
        (0,),
    )
    other = lax.ppermute(send, "dp", [(0, 1), (1, 0)])
    (packs,) = call(
        product_kernel,
        [((N_PLANE * PACK, LANES), BF16)],
        (send, other, keep),
        [pltpu.VMEM((HALF, ROWS), BF16)],
        10**9,
        12,
    )
    got = lax.all_to_all(
        packs.reshape(N_PLANE, PACK, LANES), PLANE, split_axis=0, concat_axis=0, tiled=True
    ).reshape(N_PLANE * PACK, LANES)
    (lines,) = call(
        plane_kernel,
        [((N_LINE * BLOCK, LANES), BF16)],
        (got,),
        [pltpu.VMEM((PACK, LANES), F32), pltpu.VMEM((N_LINE * 48, LANES), F32)],
        10**7,
        6,
    )
    got = lax.all_to_all(
        lines.reshape(N_LINE, BLOCK, LANES), LINE, split_axis=0, concat_axis=0, tiled=True
    ).reshape(N_LINE * BLOCK, LANES)
    grad_w_in, grad_b_in, grad_w_out, grad_b_out = call(
        line_kernel,
        [((3, H), F32), ((16, LANES), F32), ((16, LANES), F32), ((1, LANES), F32)],
        (got,),
        [pltpu.VMEM((BLOCK, LANES), F32)],
        10**6,
        4,
    )
    return td.T, grad_w_in, grad_b_in.reshape(H), grad_w_out.reshape(H), grad_b_out[0, :1]


def solution(mesh):
    split = Mesh(mesh.devices.reshape(4, 4, 8, mesh.shape["dp"]), TM_DP)
    placed = (P("dp", TM, None), P("dp", TM, None), P("dp", TM), P(), P(), P(), P())
    return jax.shard_map(
        body,
        mesh=split,
        in_specs=placed,
        out_specs=(P("dp", TM), P(TM_DP, None), P(), P(), P()),
        check_vma=False,
    )
```

```python
import functools
import math

import jax
import jax.numpy as jnp
from jax import lax
from jax.experimental import pallas as pl
from jax.experimental.pallas import tpu as pltpu
from jax.sharding import Mesh
from jax.sharding import PartitionSpec as P

CAP = 4
TM = ("tm_0", "tm_1", "tm_2")
TM_DP = ("tm_0", "tm_1", "tm_2", "dp")
PLANE = ("tm_0", "tm_1")
LINE = "tm_2"
N_TM = 128
N_PLANE = 16
N_LINE = 8
ROWS = 256
STEPS = 4
S = 256
G = 512
H = 2048
LANES = 128
HALF = (S + G) // 2
SLAB = HALF // N_PLANE
CHUNK = 256
F32 = jnp.float32
BF16 = jnp.bfloat16
I32 = jnp.int32


def iota(shape, dim):
    return lax.broadcasted_iota(I32, shape, dim)


def dot(a, b, dims=(((1,), (0,)), ((), ()))):
    return lax.dot_general(a, b, dims, preferred_element_type=F32)


def flag(mask):
    return jnp.where(mask, 1.0, 0.0)


def spread_kernel(offs_ref, many_ref, row_ref):
    offs = offs_ref[...]
    parts = jnp.concatenate([offs >> 4, offs & 15], axis=0).astype(F32).astype(BF16)
    episode = flag((iota((ROWS // STEPS, ROWS), 1) >> 2) == iota((ROWS // STEPS, ROWS), 0))
    wide = dot(parts, episode.astype(BF16))
    step = iota((2 * STEPS, ROWS), 1) & (STEPS - 1)
    which = iota((2 * STEPS, ROWS), 0)
    mine = (which & (STEPS - 1)) == step
    weight = jnp.where(which < STEPS, 16.0, 1.0)
    row = jnp.sum(jnp.where(mine, wide * weight, 0.0), axis=0, keepdims=True).astype(I32)
    row_ref[...] = row
    many_ref[...] = jnp.broadcast_to(row[None], (N_TM, 1, ROWS))


def pick_kernel(place_ref, offs_ref, table_ref, out_ref, wide_ref, ready_ref, sems):
    me = place_ref[0:1, 0:1]
    offs = offs_ref[...].reshape(N_TM, ROWS)
    peer = iota((N_TM, ROWS), 0)
    row = iota((N_TM, ROWS), 1)
    target = peer * STEPS + (row & (STEPS - 1)) + offs
    hit = ((target >> 2) == me) & (peer != me)
    earlier = flag(iota((ROWS, ROWS), 0) < iota((ROWS, ROWS), 1)).astype(BF16)
    rank = dot(flag(hit).astype(BF16), earlier)
    position = ((row - (row & (STEPS - 1))) + (target & (STEPS - 1)) + 1).astype(F32)
    wanted = []
    for c in range(CAP):
        place = jnp.sum(
            jnp.where(hit & (rank == float(c)), position, 0.0), axis=1, keepdims=True
        )
        wanted.append(flag(row.astype(F32) + 1.0 == place).astype(BF16))
    half = N_TM // 2
    copies = []
    for h in range(2):
        part = jnp.concatenate([w[h * half : (h + 1) * half] for w in wanted], axis=0)
        picked = dot(part, table_ref[...])
        for c in range(CAP):
            for j in range(G // LANES):
                at = pl.ds(h * half * 16 + c * (G // LANES) + j, half, stride=16)
                wide_ref[at, :] = picked[
                    c * half : (c + 1) * half, j * LANES : (j + 1) * LANES
                ]
        rows = slice(h * half * 16, (h + 1) * half * 16)
        ready_ref[rows, :] = wide_ref[rows, :].astype(BF16)
        there = pl.ds(h * half * 16, half * 16)
        copies.append(
            pltpu.make_async_copy(ready_ref.at[there, :], out_ref.at[there, :], sems.at[h])
        )
        copies[-1].start()
    for copy in copies:
        copy.wait()


def half_rows(core):
    k = iota((HALF, S + G), 0)
    eighth = k >> 3
    plane = (eighth * 171) >> 9
    within = eighth - plane * 3
    feature = (plane * N_LINE + (k & 7)) * 6 + core * 3 + within
    return flag(iota((HALF, S + G), 1) == feature).astype(BF16)


def three(x):
    high = x.astype(BF16).astype(F32)
    rest = x - high
    middle = rest.astype(BF16).astype(F32)
    return high, middle, rest - middle


def two(x):
    high = x.astype(BF16).astype(F32)
    return high, x - high


def stack_rows(rows, count):
    width = rows[0].shape[1]
    at = iota((count, width), 0)
    total = jnp.zeros((count, width), F32)
    for n, r in enumerate(rows):
        total = jnp.where(at == n, jnp.broadcast_to(r, (count, width)), total)
    return total


def ahead_kernel(
    place_ref,
    offs_ref,
    table_ref,
    w_in_ref,
    goal_w_ref,
    near_ref,
    at_ref,
):
    me = place_ref[0:1, 0:1]
    row = iota((ROWS, ROWS), 1)
    col = iota((ROWS, ROWS), 0)
    lane = iota((1, ROWS), 1)
    target = me * STEPS + (lane & (STEPS - 1)) + offs_ref[...]
    owner_lane = (target >> 2).astype(F32)
    position_lane = ((lane - (lane & (STEPS - 1))) + (target & (STEPS - 1))).astype(F32)

    def to_column(x):
        return jnp.sum(
            jnp.where(row == col, jnp.broadcast_to(x, (ROWS, ROWS)), 0.0),
            axis=1,
            keepdims=True,
        )

    owner = to_column(owner_lane)
    position = to_column(position_lane)
    slot = jnp.sum(flag((owner == owner_lane) & (row < col)), axis=1, keepdims=True)
    remote = owner != me.astype(F32)
    near_at = jnp.where(remote, -1.0, position)
    far_at = jnp.where(remote, owner * float(CAP) + slot, -1.0).astype(I32)
    near = flag(row.astype(F32) == near_at).astype(BF16)
    near_ref[...] = dot(near, table_ref[...]).astype(BF16)
    at_ref[...] = jnp.broadcast_to(far_at, (ROWS, LANES))
    goal_w_ref[...] = w_in_ref[S:, :]


def main_kernel(
    scale,
    place_ref,
    b_out_ref,
    fetched_ref,
    goal_w_ref,
    near_ref,
    at_ref,
    table_ref,
    state_ref,
    w_in_ref,
    b_in_ref,
    w_out_ref,
    td_ref,
    send_ref,
    keep_ref,
    slope_ref,
    hidden_ref,
    inputs_ref,
    state_w_ref,
    wide_ref,
    total_ref,
    td_rows_ref,
    sems,
    td_sem,
):
    def load(n):
        at = pl.ds(pl.multiple_of(n * CHUNK, CHUNK), CHUNK)
        return pltpu.make_async_copy(
            w_in_ref.at[pl.ds(0, S), at], state_w_ref.at[:, at], sems.at[n]
        )

    def begin(n, carry):
        load(n).start()
        return carry

    lax.fori_loop(0, H // CHUNK, begin, 0)
    core = place_ref[1:2, 0:1]
    far_at = at_ref[:, 0:1]
    far = flag(iota((ROWS, N_TM * CAP), 1) == far_at).astype(BF16)
    inputs_ref[:, :S] = state_ref[...]
    wide_ref[...] = fetched_ref[...].astype(F32)
    gap = jnp.zeros((ROWS, LANES), F32)
    for j in range(G // LANES):
        at = slice(j * LANES, (j + 1) * LANES)
        fetched = wide_ref[pl.ds(j, N_TM * CAP, stride=G // LANES), :].astype(BF16)
        goal = dot(far, fetched) + near_ref[:, at].astype(F32)
        diff = table_ref[:, at].astype(F32) - goal
        gap = gap + diff * diff
        inputs_ref[:, S + j * LANES : S + (j + 1) * LANES] = goal.astype(BF16)
    reward = -(jnp.sum(gap, axis=1, keepdims=True) * (1.0 / G))
    inputs = inputs_ref[...]

    kept = dot(half_rows(core), inputs, (((1,), (1,)), ((), ())))
    keep_ref[...] = kept.astype(BF16)
    sent = dot(half_rows(1 - core), inputs, (((1,), (1,)), ((), ()))).astype(BF16)
    for b in range(H // ROWS):
        send_ref[ROWS : ROWS + 48, b * ROWS : (b + 1) * ROWS] = sent[b * 48 : (b + 1) * 48, :]

    total_ref[...] = jnp.zeros((ROWS, LANES), F32)

    def forward(n, carry):
        at = pl.ds(pl.multiple_of(n * CHUNK, CHUNK), CHUNK)
        load(n).wait()
        pre = dot(inputs[:, :S], state_w_ref[:, at]) + dot(inputs[:, S:], goal_w_ref[:, at])
        pre = pre + b_in_ref[:, at]
        sig = 1.0 / (1.0 + jnp.exp(-pre))
        head = w_out_ref[:, at]
        act = pre * sig
        hidden = act.astype(BF16)
        hidden_ref[:, at] = hidden
        slope_ref[:, at] = head * (sig + act * (1.0 - sig))
        term = hidden.astype(F32) * head
        total_ref[...] += term[:, :LANES] + term[:, LANES:]
        return carry

    lax.fori_loop(0, H // CHUNK, forward, 0)
    value = jnp.sum(total_ref[...], axis=1, keepdims=True) + b_out_ref[:, 0:1]
    error = value - reward
    grad_value = error * scale

    each = (STEPS * iota((ROWS, ROWS // STEPS), 1)) - iota((ROWS, ROWS // STEPS), 0)
    for s in range(STEPS):
        td_rows_ref[s : s + 1, :] = jnp.sum(
            jnp.where(each + s == 0, error, 0.0), axis=0, keepdims=True
        )

    td_copy = pltpu.make_async_copy(td_rows_ref, td_ref, td_sem)
    td_copy.start()

    total_value = jnp.sum(grad_value, axis=0, keepdims=True)

    def backward(n, carry):
        at = pl.ds(pl.multiple_of(n * CHUNK, CHUNK), CHUNK)
        grad_pre = grad_value * slope_ref[:, at]
        send_ref[:ROWS, at] = grad_pre.astype(BF16)
        first = jnp.sum(grad_pre, axis=0, keepdims=True)
        second = jnp.sum(grad_value * hidden_ref[:, at].astype(F32), axis=0, keepdims=True)
        third = jnp.broadcast_to(total_value, (1, CHUNK))
        rows = stack_rows(three(first) + three(second) + three(third), 16)
        send_ref[ROWS + 48 : ROWS + 64, at] = rows.astype(BF16)
        return carry

    lax.fori_loop(0, H // CHUNK, backward, 0)
    td_copy.wait()


PACK = 432
BLOCK = 96


def product_kernel(own_ref, other_ref, keep_ref, out_ref, left_ref):
    for b in range(H // ROWS):
        left_ref[b * 48 : (b + 1) * 48, :] = other_ref[
            ROWS : ROWS + 48, b * ROWS : (b + 1) * ROWS
        ]
    keep = keep_ref[...]
    left = left_ref[...]
    for n in range(H // CHUNK):
        at = slice(n * CHUNK, (n + 1) * CHUNK)
        part = dot(keep, own_ref[:ROWS, at]) + dot(left, other_ref[:ROWS, at])
        for p in range(N_PLANE):
            for i in range(3):
                tile = part[p * SLAB + 8 * i : p * SLAB + 8 * i + 8]
                pair = jnp.concatenate([tile[:, :LANES], tile[:, LANES:]], axis=0)
                start = p * PACK + (16 * i + 2 * n) * 8
                out_ref[start : start + 16, :] = pair.astype(BF16)
    mine = own_ref[ROWS + 48 : ROWS + 64, :].astype(F32)
    theirs = other_ref[ROWS + 48 : ROWS + 64, :].astype(F32)
    rows = []
    for q in range(3):
        a = mine[3 * q : 3 * q + 1] + mine[3 * q + 1 : 3 * q + 2] + mine[3 * q + 2 : 3 * q + 3]
        b = theirs[3 * q : 3 * q + 1] + theirs[3 * q + 1 : 3 * q + 2] + theirs[3 * q + 2 : 3 * q + 3]
        rows.append(a + b)
    blocks = []
    for r in rows[:2]:
        pieces = [r[:, b * LANES : (b + 1) * LANES] for b in range(H // LANES)]
        blocks.append(jnp.concatenate(pieces, axis=0))
    blocks.append(stack_rows(two(rows[2][:, :LANES]), 16))
    small = jnp.concatenate(blocks, axis=0).astype(BF16)
    for p in range(N_PLANE):
        out_ref[p * PACK + HALF : (p + 1) * PACK, :] = small


def plane_kernel(got_ref, out_ref, sum_ref, wide_ref):
    for b in range(PACK // 16):
        total = got_ref[b * 16 : b * 16 + 16, :].astype(F32)
        for p in range(1, N_PLANE):
            total = total + got_ref[p * PACK + b * 16 : p * PACK + b * 16 + 16, :].astype(F32)
        sum_ref[b * 16 : b * 16 + 16, :] = total
    for n in range(48):
        wide_ref[pl.ds(n, N_LINE, stride=48), :] = sum_ref[8 * n : 8 * n + 8, :]
    last = sum_ref[416:417, :] + sum_ref[417:418, :]
    small = jnp.concatenate(
        (sum_ref[384:416, :], stack_rows(two(last), 16)),
        axis=0,
    ).astype(BF16)
    for z in range(N_LINE):
        out_ref[z * BLOCK : z * BLOCK + 48, :] = wide_ref[z * 48 : z * 48 + 48, :].astype(BF16)
        out_ref[z * BLOCK + 48 : (z + 1) * BLOCK, :] = small


def line_kernel(got_ref, w_ref, b_in_ref, w_out_ref, b_out_ref, sum_ref):
    for b in range(BLOCK // 16):
        total = got_ref[b * 16 : b * 16 + 16, :].astype(F32)
        for z in range(1, N_LINE):
            total = total + got_ref[z * BLOCK + b * 16 : z * BLOCK + b * 16 + 16, :].astype(F32)
        sum_ref[b * 16 : b * 16 + 16, :] = total
    for i in range(3):
        for b in range(H // LANES):
            w_ref[i : i + 1, b * LANES : (b + 1) * LANES] = sum_ref[i * 16 + b : i * 16 + b + 1, :]
    b_in_ref[...] = sum_ref[48:64, :]
    w_out_ref[...] = sum_ref[64:80, :]
    b_out_ref[...] = sum_ref[80:81, :] + sum_ref[81:82, :]


def call(kernel, shapes, operands, scratch, flops, grant, in_hbm=(), out_hbm=()):
    specs = [pl.BlockSpec(memory_space=pltpu.VMEM)] * len(operands)
    for n in in_hbm:
        specs[n] = pl.BlockSpec(memory_space=pltpu.HBM)
    back = [pl.BlockSpec(memory_space=pltpu.VMEM)] * len(shapes)
    for n in out_hbm:
        back[n] = pl.BlockSpec(memory_space=pltpu.HBM)
    outs = [jax.ShapeDtypeStruct(shape, kind) for shape, kind in shapes]
    return pl.pallas_call(
        kernel,
        out_shape=outs,
        in_specs=specs,
        out_specs=back,
        scratch_shapes=scratch,
        compiler_params=pltpu.CompilerParams(vmem_limit_bytes=grant << 20),
        cost_estimate=pl.CostEstimate(flops=flops, bytes_accessed=1 << 20, transcendentals=0),
    )(*operands)


def body(state_feats, achieved, offsets, w_in, b_in, w_out, b_out):
    place = jnp.stack([lax.axis_index(TM), lax.axis_index("dp")]).astype(I32)
    place = jnp.broadcast_to(place[:, None], (2, LANES))
    table = achieved.reshape(ROWS, G)
    state = state_feats.reshape(ROWS, S)
    many, offs = call(
        spread_kernel,
        [((N_TM, 1, ROWS), I32), ((1, ROWS), I32)],
        (offsets.T,),
        [],
        10**6,
        4,
    )
    known = lax.all_to_all(many, TM, split_axis=0, concat_axis=0, tiled=True)
    (picked,) = call(
        pick_kernel,
        [((N_TM * 16, LANES), BF16)],
        (place, known, table),
        [
            pltpu.VMEM((N_TM * 16, LANES), F32),
            pltpu.VMEM((N_TM * 16, LANES), BF16),
            pltpu.SemaphoreType.DMA((2,)),
        ],
        10**8,
        8,
        (),
        (0,),
    )
    goal_w, near, at = call(
        ahead_kernel,
        [((G, H), BF16), ((ROWS, G), BF16), ((ROWS, LANES), I32)],
        (place, offs, table, w_in),
        [],
        10**9,
        12,
    )
    fetched = lax.all_to_all(
        picked.reshape(N_TM, 16, LANES), TM, split_axis=0, concat_axis=0, tiled=True
    ).reshape(N_TM * 16, LANES)
    head_bias = jnp.broadcast_to(b_out[None], (1, LANES))
    scale = 1.0 / math.sqrt(ROWS * N_TM * 2)
    td, send, keep = call(
        functools.partial(main_kernel, scale),
        [((STEPS, ROWS // STEPS), F32), ((ROWS + 64, H), BF16), ((HALF, ROWS), BF16)],
        (
            place,
            head_bias,
            fetched,
            goal_w,
            near,
            at,
            table,
            state,
            w_in,
            b_in.reshape(1, H),
            w_out.reshape(1, H),
        ),
        [
            pltpu.VMEM((ROWS, H), F32),
            pltpu.VMEM((ROWS, H), BF16),
            pltpu.VMEM((ROWS, S + G), BF16),
            pltpu.VMEM((S, H), BF16),
            pltpu.VMEM((N_TM * 16, LANES), F32),
            pltpu.VMEM((ROWS, LANES), F32),
            pltpu.VMEM((STEPS, ROWS // STEPS), F32),
            pltpu.SemaphoreType.DMA((H // CHUNK,)),
            pltpu.SemaphoreType.DMA,
        ],
        2 * 10**9,
        48,
        (8,),
        (0,),
    )
    other = lax.ppermute(send, "dp", [(0, 1), (1, 0)])
    (packs,) = call(
        product_kernel,
        [((N_PLANE * PACK, LANES), BF16)],
        (send, other, keep),
        [pltpu.VMEM((HALF, ROWS), BF16)],
        10**9,
        12,
    )
    got = lax.all_to_all(
        packs.reshape(N_PLANE, PACK, LANES), PLANE, split_axis=0, concat_axis=0, tiled=True
    ).reshape(N_PLANE * PACK, LANES)
    (lines,) = call(
        plane_kernel,
        [((N_LINE * BLOCK, LANES), BF16)],
        (got,),
        [pltpu.VMEM((PACK, LANES), F32), pltpu.VMEM((N_LINE * 48, LANES), F32)],
        10**7,
        6,
    )
    got = lax.all_to_all(
        lines.reshape(N_LINE, BLOCK, LANES), LINE, split_axis=0, concat_axis=0, tiled=True
    ).reshape(N_LINE * BLOCK, LANES)
    grad_w_in, grad_b_in, grad_w_out, grad_b_out = call(
        line_kernel,
        [((3, H), F32), ((16, LANES), F32), ((16, LANES), F32), ((1, LANES), F32)],
        (got,),
        [pltpu.VMEM((BLOCK, LANES), F32)],
        10**6,
        4,
    )
    return td.T, grad_w_in, grad_b_in.reshape(H), grad_w_out.reshape(H), grad_b_out[0, :1]


def solution(mesh):
    split = Mesh(mesh.devices.reshape(4, 4, 8, mesh.shape["dp"]), TM_DP)
    placed = (P("dp", TM, None), P("dp", TM, None), P("dp", TM), P(), P(), P(), P())
    return jax.shard_map(
        body,
        mesh=split,
        in_specs=placed,
        out_specs=(P("dp", TM), P(TM_DP, None), P(), P(), P()),
        check_vma=False,
    )
```

```python
import functools
import math

import jax
import jax.numpy as jnp
from jax import lax
from jax.experimental import pallas as pl
from jax.experimental.pallas import tpu as pltpu
from jax.sharding import Mesh
from jax.sharding import PartitionSpec as P

CAP = 4
TM = ("tm_0", "tm_1", "tm_2")
TM_DP = ("tm_0", "tm_1", "tm_2", "dp")
PLANE = ("tm_0", "tm_1")
LINE = "tm_2"
N_TM = 128
N_PLANE = 16
N_LINE = 8
ROWS = 256
STEPS = 4
S = 256
G = 512
H = 2048
LANES = 128
HALF = (S + G) // 2
SLAB = HALF // N_PLANE
CHUNK = 256
F32 = jnp.float32
BF16 = jnp.bfloat16
I32 = jnp.int32


def iota(shape, dim):
    return lax.broadcasted_iota(I32, shape, dim)


def dot(a, b, dims=(((1,), (0,)), ((), ()))):
    return lax.dot_general(a, b, dims, preferred_element_type=F32)


def flag(mask):
    return jnp.where(mask, 1.0, 0.0)


def spread_kernel(offs_ref, many_ref, row_ref):
    offs = offs_ref[...]
    parts = jnp.concatenate([offs >> 4, offs & 15], axis=0).astype(F32).astype(BF16)
    episode = flag((iota((ROWS // STEPS, ROWS), 1) >> 2) == iota((ROWS // STEPS, ROWS), 0))
    wide = dot(parts, episode.astype(BF16))
    step = iota((2 * STEPS, ROWS), 1) & (STEPS - 1)
    which = iota((2 * STEPS, ROWS), 0)
    mine = (which & (STEPS - 1)) == step
    weight = jnp.where(which < STEPS, 16.0, 1.0)
    row = jnp.sum(jnp.where(mine, wide * weight, 0.0), axis=0, keepdims=True).astype(I32)
    row_ref[...] = row
    many_ref[...] = jnp.broadcast_to(row[None], (N_TM, 1, ROWS))


def pick_kernel(place_ref, offs_ref, table_ref, out_ref, wide_ref, ready_ref, sems):
    me = place_ref[0:1, 0:1]
    offs = offs_ref[...].reshape(N_TM, ROWS)
    peer = iota((N_TM, ROWS), 0)
    row = iota((N_TM, ROWS), 1)
    target = peer * STEPS + (row & (STEPS - 1)) + offs
    hit = ((target >> 2) == me) & (peer != me)
    earlier = flag(iota((ROWS, ROWS), 0) < iota((ROWS, ROWS), 1)).astype(BF16)
    rank = dot(flag(hit).astype(BF16), earlier)
    position = ((row - (row & (STEPS - 1))) + (target & (STEPS - 1)) + 1).astype(F32)
    wanted = []
    for c in range(CAP):
        place = jnp.sum(
            jnp.where(hit & (rank == float(c)), position, 0.0), axis=1, keepdims=True
        )
        wanted.append(flag(row.astype(F32) + 1.0 == place).astype(BF16))
    half = N_TM // 2
    copies = []
    for h in range(2):
        part = jnp.concatenate([w[h * half : (h + 1) * half] for w in wanted], axis=0)
        picked = dot(part, table_ref[...])
        for c in range(CAP):
            for j in range(G // LANES):
                at = pl.ds(h * half * 16 + c * (G // LANES) + j, half, stride=16)
                wide_ref[at, :] = picked[
                    c * half : (c + 1) * half, j * LANES : (j + 1) * LANES
                ]
        rows = slice(h * half * 16, (h + 1) * half * 16)
        ready_ref[rows, :] = wide_ref[rows, :].astype(BF16)
        there = pl.ds(h * half * 16, half * 16)
        copies.append(
            pltpu.make_async_copy(ready_ref.at[there, :], out_ref.at[there, :], sems.at[h])
        )
        copies[-1].start()
    for copy in copies:
        copy.wait()


def half_rows(core):
    k = iota((HALF, S + G), 0)
    eighth = k >> 3
    plane = (eighth * 171) >> 9
    within = eighth - plane * 3
    feature = (plane * N_LINE + (k & 7)) * 6 + core * 3 + within
    return flag(iota((HALF, S + G), 1) == feature).astype(BF16)


def three(x):
    high = x.astype(BF16).astype(F32)
    rest = x - high
    middle = rest.astype(BF16).astype(F32)
    return high, middle, rest - middle


def two(x):
    high = x.astype(BF16).astype(F32)
    return high, x - high


def stack_rows(rows, count):
    width = rows[0].shape[1]
    at = iota((count, width), 0)
    total = jnp.zeros((count, width), F32)
    for n, r in enumerate(rows):
        total = jnp.where(at == n, jnp.broadcast_to(r, (count, width)), total)
    return total


def ahead_kernel(
    place_ref,
    offs_ref,
    table_ref,
    w_in_ref,
    goal_w_ref,
    near_ref,
    at_ref,
):
    me = place_ref[0:1, 0:1]
    row = iota((ROWS, ROWS), 1)
    col = iota((ROWS, ROWS), 0)
    lane = iota((1, ROWS), 1)
    target = me * STEPS + (lane & (STEPS - 1)) + offs_ref[...]
    owner_lane = (target >> 2).astype(F32)
    position_lane = ((lane - (lane & (STEPS - 1))) + (target & (STEPS - 1))).astype(F32)

    def to_column(x):
        return jnp.sum(
            jnp.where(row == col, jnp.broadcast_to(x, (ROWS, ROWS)), 0.0),
            axis=1,
            keepdims=True,
        )

    owner = to_column(owner_lane)
    position = to_column(position_lane)
    slot = jnp.sum(flag((owner == owner_lane) & (row < col)), axis=1, keepdims=True)
    remote = owner != me.astype(F32)
    near_at = jnp.where(remote, -1.0, position)
    far_at = jnp.where(remote, owner * float(CAP) + slot, -1.0).astype(I32)
    near = flag(row.astype(F32) == near_at).astype(BF16)
    near_ref[...] = dot(near, table_ref[...]).astype(BF16)
    at_ref[...] = jnp.broadcast_to(far_at, (ROWS, LANES))
    goal_w_ref[...] = w_in_ref[S:, :]


def main_kernel(
    scale,
    place_ref,
    b_out_ref,
    fetched_ref,
    goal_w_ref,
    near_ref,
    at_ref,
    table_ref,
    state_ref,
    w_in_ref,
    b_in_ref,
    w_out_ref,
    td_ref,
    send_ref,
    keep_ref,
    slope_ref,
    hidden_ref,
    inputs_ref,
    state_w_ref,
    wide_ref,
    total_ref,
    td_rows_ref,
    sems,
    td_sem,
):
    def load(n):
        at = pl.ds(pl.multiple_of(n * CHUNK, CHUNK), CHUNK)
        return pltpu.make_async_copy(
            w_in_ref.at[pl.ds(0, S), at], state_w_ref.at[:, at], sems.at[n]
        )

    def begin(n, carry):
        load(n).start()
        return carry

    lax.fori_loop(0, H // CHUNK, begin, 0)
    core = place_ref[1:2, 0:1]
    far_at = at_ref[:, 0:1]
    far = flag(iota((ROWS, N_TM * CAP), 1) == far_at).astype(BF16)
    inputs_ref[:, :S] = state_ref[...]
    wide_ref[...] = fetched_ref[...].astype(F32)
    gap = jnp.zeros((ROWS, LANES), F32)
    for j in range(G // LANES):
        at = slice(j * LANES, (j + 1) * LANES)
        fetched = wide_ref[pl.ds(j, N_TM * CAP, stride=G // LANES), :].astype(BF16)
        goal = dot(far, fetched) + near_ref[:, at].astype(F32)
        diff = table_ref[:, at].astype(F32) - goal
        gap = gap + diff * diff
        inputs_ref[:, S + j * LANES : S + (j + 1) * LANES] = goal.astype(BF16)
    reward = -(jnp.sum(gap, axis=1, keepdims=True) * (1.0 / G))
    inputs = inputs_ref[...]

    kept = dot(half_rows(core), inputs, (((1,), (1,)), ((), ())))
    keep_ref[...] = kept.astype(BF16)
    sent = dot(half_rows(1 - core), inputs, (((1,), (1,)), ((), ()))).astype(BF16)
    for b in range(H // ROWS):
        send_ref[ROWS : ROWS + 48, b * ROWS : (b + 1) * ROWS] = sent[b * 48 : (b + 1) * 48, :]

    total_ref[...] = jnp.zeros((ROWS, LANES), F32)

    def forward(n, carry):
        at = pl.ds(pl.multiple_of(n * CHUNK, CHUNK), CHUNK)
        load(n).wait()
        pre = dot(inputs[:, :S], state_w_ref[:, at]) + dot(inputs[:, S:], goal_w_ref[:, at])
        pre = pre + b_in_ref[:, at]
        sig = 1.0 / (1.0 + jnp.exp(-pre))
        head = w_out_ref[:, at]
        act = pre * sig
        hidden = act.astype(BF16)
        hidden_ref[:, at] = hidden
        slope_ref[:, at] = head * (sig + act * (1.0 - sig))
        term = hidden.astype(F32) * head
        total_ref[...] += term[:, :LANES] + term[:, LANES:]
        return carry

    lax.fori_loop(0, H // CHUNK, forward, 0)
    value = jnp.sum(total_ref[...], axis=1, keepdims=True) + b_out_ref[:, 0:1]
    error = value - reward
    grad_value = error * scale

    each = (STEPS * iota((ROWS, ROWS // STEPS), 1)) - iota((ROWS, ROWS // STEPS), 0)
    for s in range(STEPS):
        td_rows_ref[s : s + 1, :] = jnp.sum(
            jnp.where(each + s == 0, error, 0.0), axis=0, keepdims=True
        )

    td_copy = pltpu.make_async_copy(td_rows_ref, td_ref, td_sem)
    td_copy.start()

    total_value = jnp.sum(grad_value, axis=0, keepdims=True)

    def backward(n, carry):
        at = pl.ds(pl.multiple_of(n * CHUNK, CHUNK), CHUNK)
        grad_pre = grad_value * slope_ref[:, at]
        send_ref[:ROWS, at] = grad_pre.astype(BF16)
        first = jnp.sum(grad_pre, axis=0, keepdims=True)
        second = jnp.sum(grad_value * hidden_ref[:, at].astype(F32), axis=0, keepdims=True)
        third = jnp.broadcast_to(total_value, (1, CHUNK))
        rows = stack_rows(three(first) + three(second) + three(third), 16)
        send_ref[ROWS + 48 : ROWS + 64, at] = rows.astype(BF16)
        return carry

    lax.fori_loop(0, H // CHUNK, backward, 0)
    td_copy.wait()


PACK = 424
BLOCK = 88


def product_kernel(own_ref, other_ref, keep_ref, out_ref, left_ref):
    for b in range(H // ROWS):
        left_ref[b * 48 : (b + 1) * 48, :] = other_ref[
            ROWS : ROWS + 48, b * ROWS : (b + 1) * ROWS
        ]
    keep = keep_ref[...]
    left = left_ref[...]
    for n in range(H // CHUNK):
        at = slice(n * CHUNK, (n + 1) * CHUNK)
        part = dot(keep, own_ref[:ROWS, at]) + dot(left, other_ref[:ROWS, at])
        for p in range(N_PLANE):
            for i in range(3):
                tile = part[p * SLAB + 8 * i : p * SLAB + 8 * i + 8]
                pair = jnp.concatenate([tile[:, :LANES], tile[:, LANES:]], axis=0)
                start = p * PACK + (16 * i + 2 * n) * 8
                out_ref[start : start + 16, :] = pair.astype(BF16)
    mine = own_ref[ROWS + 48 : ROWS + 64, :].astype(F32)
    theirs = other_ref[ROWS + 48 : ROWS + 64, :].astype(F32)
    rows = []
    for q in range(3):
        a = mine[3 * q : 3 * q + 1] + mine[3 * q + 1 : 3 * q + 2] + mine[3 * q + 2 : 3 * q + 3]
        b = theirs[3 * q : 3 * q + 1] + theirs[3 * q + 1 : 3 * q + 2] + theirs[3 * q + 2 : 3 * q + 3]
        rows.append(a + b)
    blocks = []
    for r in rows[:2]:
        pieces = [r[:, b * LANES : (b + 1) * LANES] for b in range(H // LANES)]
        blocks.append(jnp.concatenate(pieces, axis=0))
    blocks.append(stack_rows(two(rows[2][:, :LANES]), 8))
    small = jnp.concatenate(blocks, axis=0).astype(BF16)
    for p in range(N_PLANE):
        out_ref[p * PACK + HALF : (p + 1) * PACK, :] = small


def plane_kernel(got_ref, out_ref, sum_ref, wide_ref):
    for b in range(PACK // 8):
        total = got_ref[b * 8 : b * 8 + 8, :].astype(F32)
        for p in range(1, N_PLANE):
            total = total + got_ref[p * PACK + b * 8 : p * PACK + b * 8 + 8, :].astype(F32)
        sum_ref[b * 8 : b * 8 + 8, :] = total
    for n in range(48):
        wide_ref[pl.ds(n, N_LINE, stride=48), :] = sum_ref[8 * n : 8 * n + 8, :]
    last = sum_ref[416:417, :] + sum_ref[417:418, :]
    small = jnp.concatenate(
        (sum_ref[384:416, :], stack_rows(two(last), 8)),
        axis=0,
    ).astype(BF16)
    for z in range(N_LINE):
        out_ref[z * BLOCK : z * BLOCK + 48, :] = wide_ref[z * 48 : z * 48 + 48, :].astype(BF16)
        out_ref[z * BLOCK + 48 : (z + 1) * BLOCK, :] = small


def line_kernel(got_ref, w_ref, b_in_ref, w_out_ref, b_out_ref, sum_ref):
    for b in range(BLOCK // 8):
        total = got_ref[b * 8 : b * 8 + 8, :].astype(F32)
        for z in range(1, N_LINE):
            total = total + got_ref[z * BLOCK + b * 8 : z * BLOCK + b * 8 + 8, :].astype(F32)
        sum_ref[b * 8 : b * 8 + 8, :] = total
    for i in range(3):
        for b in range(H // LANES):
            w_ref[i : i + 1, b * LANES : (b + 1) * LANES] = sum_ref[i * 16 + b : i * 16 + b + 1, :]
    b_in_ref[...] = sum_ref[48:64, :]
    w_out_ref[...] = sum_ref[64:80, :]
    b_out_ref[...] = sum_ref[80:81, :] + sum_ref[81:82, :]


def call(kernel, shapes, operands, scratch, flops, grant, in_hbm=(), out_hbm=()):
    specs = [pl.BlockSpec(memory_space=pltpu.VMEM)] * len(operands)
    for n in in_hbm:
        specs[n] = pl.BlockSpec(memory_space=pltpu.HBM)
    back = [pl.BlockSpec(memory_space=pltpu.VMEM)] * len(shapes)
    for n in out_hbm:
        back[n] = pl.BlockSpec(memory_space=pltpu.HBM)
    outs = [jax.ShapeDtypeStruct(shape, kind) for shape, kind in shapes]
    return pl.pallas_call(
        kernel,
        out_shape=outs,
        in_specs=specs,
        out_specs=back,
        scratch_shapes=scratch,
        compiler_params=pltpu.CompilerParams(vmem_limit_bytes=grant << 20),
        cost_estimate=pl.CostEstimate(flops=flops, bytes_accessed=1 << 20, transcendentals=0),
    )(*operands)


def body(state_feats, achieved, offsets, w_in, b_in, w_out, b_out):
    place = jnp.stack([lax.axis_index(TM), lax.axis_index("dp")]).astype(I32)
    place = jnp.broadcast_to(place[:, None], (2, LANES))
    table = achieved.reshape(ROWS, G)
    state = state_feats.reshape(ROWS, S)
    many, offs = call(
        spread_kernel,
        [((N_TM, 1, ROWS), I32), ((1, ROWS), I32)],
        (offsets.T,),
        [],
        10**6,
        60,
    )
    known = lax.all_to_all(many, TM, split_axis=0, concat_axis=0, tiled=True)
    (picked,) = call(
        pick_kernel,
        [((N_TM * 16, LANES), BF16)],
        (place, known, table),
        [
            pltpu.VMEM((N_TM * 16, LANES), F32),
            pltpu.VMEM((N_TM * 16, LANES), BF16),
            pltpu.SemaphoreType.DMA((2,)),
        ],
        10**8,
        8,
        (),
        (0,),
    )
    goal_w, near, at = call(
        ahead_kernel,
        [((G, H), BF16), ((ROWS, G), BF16), ((ROWS, LANES), I32)],
        (place, offs, table, w_in),
        [],
        10**9,
        12,
    )
    fetched = lax.all_to_all(
        picked.reshape(N_TM, 16, LANES), TM, split_axis=0, concat_axis=0, tiled=True
    ).reshape(N_TM * 16, LANES)
    head_bias = jnp.broadcast_to(b_out[None], (1, LANES))
    scale = 1.0 / math.sqrt(ROWS * N_TM * 2)
    td, send, keep = call(
        functools.partial(main_kernel, scale),
        [((STEPS, ROWS // STEPS), F32), ((ROWS + 64, H), BF16), ((HALF, ROWS), BF16)],
        (
            place,
            head_bias,
            fetched,
            goal_w,
            near,
            at,
            table,
            state,
            w_in,
            b_in.reshape(1, H),
            w_out.reshape(1, H),
        ),
        [
            pltpu.VMEM((ROWS, H), F32),
            pltpu.VMEM((ROWS, H), BF16),
            pltpu.VMEM((ROWS, S + G), BF16),
            pltpu.VMEM((S, H), BF16),
            pltpu.VMEM((N_TM * 16, LANES), F32),
            pltpu.VMEM((ROWS, LANES), F32),
            pltpu.VMEM((STEPS, ROWS // STEPS), F32),
            pltpu.SemaphoreType.DMA((H // CHUNK,)),
            pltpu.SemaphoreType.DMA,
        ],
        2 * 10**9,
        48,
        (8,),
        (0,),
    )
    other = lax.ppermute(send, "dp", [(0, 1), (1, 0)])
    (packs,) = call(
        product_kernel,
        [((N_PLANE * PACK, LANES), BF16)],
        (send, other, keep),
        [pltpu.VMEM((HALF, ROWS), BF16)],
        10**9,
        12,
    )
    got = lax.all_to_all(
        packs.reshape(N_PLANE, PACK, LANES), PLANE, split_axis=0, concat_axis=0, tiled=True
    ).reshape(N_PLANE * PACK, LANES)
    (lines,) = call(
        plane_kernel,
        [((N_LINE * BLOCK, LANES), BF16)],
        (got,),
        [pltpu.VMEM((PACK, LANES), F32), pltpu.VMEM((N_LINE * 48, LANES), F32)],
        10**7,
        6,
    )
    got = lax.all_to_all(
        lines.reshape(N_LINE, BLOCK, LANES), LINE, split_axis=0, concat_axis=0, tiled=True
    ).reshape(N_LINE * BLOCK, LANES)
    grad_w_in, grad_b_in, grad_w_out, grad_b_out = call(
        line_kernel,
        [((3, H), F32), ((16, LANES), F32), ((16, LANES), F32), ((1, LANES), F32)],
        (got,),
        [pltpu.VMEM((BLOCK, LANES), F32)],
        10**6,
        4,
    )
    return td.T, grad_w_in, grad_b_in.reshape(H), grad_w_out.reshape(H), grad_b_out[0, :1]


def solution(mesh):
    split = Mesh(mesh.devices.reshape(4, 4, 8, mesh.shape["dp"]), TM_DP)
    placed = (P("dp", TM, None), P("dp", TM, None), P("dp", TM), P(), P(), P(), P())
    return jax.shard_map(
        body,
        mesh=split,
        in_specs=placed,
        out_specs=(P("dp", TM), P(TM_DP, None), P(), P(), P()),
        check_vma=False,
    )
```

```python
import functools
import math

import jax
import jax.numpy as jnp
from jax import lax
from jax.experimental import pallas as pl
from jax.experimental.pallas import tpu as pltpu
from jax.sharding import Mesh
from jax.sharding import PartitionSpec as P

CAP = 4
TM = ("tm_0", "tm_1", "tm_2")
TM_DP = ("tm_0", "tm_1", "tm_2", "dp")
PLANE = ("tm_0", "tm_1")
LINE = "tm_2"
N_TM = 128
N_PLANE = 16
N_LINE = 8
ROWS = 256
STEPS = 4
S = 256
G = 512
H = 2048
LANES = 128
HALF = (S + G) // 2
SLAB = HALF // N_PLANE
CHUNK = 256
F32 = jnp.float32
BF16 = jnp.bfloat16
I32 = jnp.int32


def iota(shape, dim):
    return lax.broadcasted_iota(I32, shape, dim)


def dot(a, b, dims=(((1,), (0,)), ((), ()))):
    return lax.dot_general(a, b, dims, preferred_element_type=F32)


def flag(mask):
    return jnp.where(mask, 1.0, 0.0)


def spread_kernel(offs_ref, many_ref, row_ref):
    offs = offs_ref[...]
    parts = jnp.concatenate([offs >> 4, offs & 15], axis=0).astype(F32).astype(BF16)
    episode = flag((iota((ROWS // STEPS, ROWS), 1) >> 2) == iota((ROWS // STEPS, ROWS), 0))
    wide = dot(parts, episode.astype(BF16))
    step = iota((2 * STEPS, ROWS), 1) & (STEPS - 1)
    which = iota((2 * STEPS, ROWS), 0)
    mine = (which & (STEPS - 1)) == step
    weight = jnp.where(which < STEPS, 16.0, 1.0)
    row = jnp.sum(jnp.where(mine, wide * weight, 0.0), axis=0, keepdims=True).astype(I32)
    row_ref[...] = row
    many_ref[...] = jnp.broadcast_to(row[None], (N_TM, 1, ROWS))


def pick_kernel(place_ref, offs_ref, table_ref, out_ref, wide_ref, ready_ref, sems):
    me = place_ref[0:1, 0:1]
    offs = offs_ref[...].reshape(N_TM, ROWS)
    peer = iota((N_TM, ROWS), 0)
    row = iota((N_TM, ROWS), 1)
    target = peer * STEPS + (row & (STEPS - 1)) + offs
    hit = ((target >> 2) == me) & (peer != me)
    earlier = flag(iota((ROWS, ROWS), 0) < iota((ROWS, ROWS), 1)).astype(BF16)
    rank = dot(flag(hit).astype(BF16), earlier)
    position = ((row - (row & (STEPS - 1))) + (target & (STEPS - 1)) + 1).astype(F32)
    wanted = []
    for c in range(CAP):
        place = jnp.sum(
            jnp.where(hit & (rank == float(c)), position, 0.0), axis=1, keepdims=True
        )
        wanted.append(flag(row.astype(F32) + 1.0 == place).astype(BF16))
    half = N_TM // 2
    copies = []
    for h in range(2):
        part = jnp.concatenate([w[h * half : (h + 1) * half] for w in wanted], axis=0)
        picked = dot(part, table_ref[...])
        for c in range(CAP):
            for j in range(G // LANES):
                at = pl.ds(h * half * 16 + c * (G // LANES) + j, half, stride=16)
                wide_ref[at, :] = picked[
                    c * half : (c + 1) * half, j * LANES : (j + 1) * LANES
                ]
        rows = slice(h * half * 16, (h + 1) * half * 16)
        ready_ref[rows, :] = wide_ref[rows, :].astype(BF16)
        there = pl.ds(h * half * 16, half * 16)
        copies.append(
            pltpu.make_async_copy(ready_ref.at[there, :], out_ref.at[there, :], sems.at[h])
        )
        copies[-1].start()
    for copy in copies:
        copy.wait()


def half_rows(core):
    k = iota((HALF, S + G), 0)
    eighth = k >> 3
    plane = (eighth * 171) >> 9
    within = eighth - plane * 3
    feature = (plane * N_LINE + (k & 7)) * 6 + core * 3 + within
    return flag(iota((HALF, S + G), 1) == feature).astype(BF16)


def three(x):
    high = x.astype(BF16).astype(F32)
    rest = x - high
    middle = rest.astype(BF16).astype(F32)
    return high, middle, rest - middle


def two(x):
    high = x.astype(BF16).astype(F32)
    return high, x - high


def stack_rows(rows, count):
    width = rows[0].shape[1]
    at = iota((count, width), 0)
    total = jnp.zeros((count, width), F32)
    for n, r in enumerate(rows):
        total = jnp.where(at == n, jnp.broadcast_to(r, (count, width)), total)
    return total


def ahead_kernel(
    place_ref,
    offs_ref,
    table_ref,
    w_in_ref,
    goal_w_ref,
    near_ref,
    at_ref,
):
    me = place_ref[0:1, 0:1]
    row = iota((ROWS, ROWS), 1)
    col = iota((ROWS, ROWS), 0)
    lane = iota((1, ROWS), 1)
    target = me * STEPS + (lane & (STEPS - 1)) + offs_ref[...]
    owner_lane = (target >> 2).astype(F32)
    position_lane = ((lane - (lane & (STEPS - 1))) + (target & (STEPS - 1))).astype(F32)

    def to_column(x):
        return jnp.sum(
            jnp.where(row == col, jnp.broadcast_to(x, (ROWS, ROWS)), 0.0),
            axis=1,
            keepdims=True,
        )

    owner = to_column(owner_lane)
    position = to_column(position_lane)
    slot = jnp.sum(flag((owner == owner_lane) & (row < col)), axis=1, keepdims=True)
    remote = owner != me.astype(F32)
    near_at = jnp.where(remote, -1.0, position)
    far_at = jnp.where(remote, owner * float(CAP) + slot, -1.0).astype(I32)
    near = flag(row.astype(F32) == near_at).astype(BF16)
    near_ref[...] = dot(near, table_ref[...]).astype(BF16)
    at_ref[...] = jnp.broadcast_to(far_at, (ROWS, LANES))
    goal_w_ref[...] = w_in_ref[S:, :]


def main_kernel(
    scale,
    place_ref,
    b_out_ref,
    fetched_ref,
    goal_w_ref,
    near_ref,
    at_ref,
    table_ref,
    state_ref,
    w_in_ref,
    b_in_ref,
    w_out_ref,
    td_ref,
    send_ref,
    keep_ref,
    slope_ref,
    hidden_ref,
    inputs_ref,
    state_w_ref,
    wide_ref,
    total_ref,
    td_rows_ref,
    even_ref,
    odd_ref,
    sems,
    td_sem,
):
    def load(n):
        at = pl.ds(pl.multiple_of(n * CHUNK, CHUNK), CHUNK)
        return pltpu.make_async_copy(
            w_in_ref.at[pl.ds(0, S), at], state_w_ref.at[:, at], sems.at[n]
        )

    def begin(n, carry):
        load(n).start()
        return carry

    lax.fori_loop(0, H // CHUNK, begin, 0)
    core = place_ref[1:2, 0:1]
    far_at = at_ref[:, 0:1]
    far = flag(iota((ROWS, N_TM * CAP), 1) == far_at).astype(BF16)
    inputs_ref[:, :S] = state_ref[...]
    wide_ref[: N_TM * 16, :] = fetched_ref[...].astype(F32)
    gap = jnp.zeros((ROWS, LANES), F32)
    for j in range(G // LANES):
        at = slice(j * LANES, (j + 1) * LANES)
        fetched = wide_ref[pl.ds(j, N_TM * CAP, stride=G // LANES), :].astype(BF16)
        goal = dot(far, fetched) + near_ref[:, at].astype(F32)
        diff = table_ref[:, at].astype(F32) - goal
        gap = gap + diff * diff
        inputs_ref[:, S + j * LANES : S + (j + 1) * LANES] = goal.astype(BF16)
    reward = -(jnp.sum(gap, axis=1, keepdims=True) * (1.0 / G))
    inputs = inputs_ref[...]

    kept = dot(half_rows(core), inputs, (((1,), (1,)), ((), ())))
    keep_ref[...] = kept.astype(BF16)
    sent = dot(half_rows(1 - core), inputs, (((1,), (1,)), ((), ()))).astype(BF16)
    for b in range(H // ROWS):
        send_ref[ROWS : ROWS + 48, b * ROWS : (b + 1) * ROWS] = sent[b * 48 : (b + 1) * 48, :]

    total_ref[...] = jnp.zeros((ROWS, LANES), F32)

    def product(n, buffer_ref):
        at = pl.ds(pl.multiple_of(n * CHUNK, CHUNK), CHUNK)
        buffer_ref[...] = dot(inputs[:, :S], state_w_ref[:, at]) + dot(
            inputs[:, S:], goal_w_ref[:, at]
        )

    def activate(n, buffer_ref):
        at = pl.ds(pl.multiple_of(n * CHUNK, CHUNK), CHUNK)
        pre = buffer_ref[...] + b_in_ref[:, at]
        sig = 0.5 * jnp.tanh(0.5 * pre) + 0.5
        head = w_out_ref[:, at]
        act = pre * sig
        hidden = act.astype(BF16)
        hidden_ref[:, at] = hidden
        slope_ref[:, at] = head * (sig + act * (1.0 - sig))
        term = hidden.astype(F32) * head
        total_ref[...] += term[:, :LANES] + term[:, LANES:]

    count = H // CHUNK
    load(0).wait()
    product(0, even_ref)

    def forward(m, carry):
        load(2 * m + 1).wait()

        @pl.when(2 * m + 2 < count)
        def _():
            load(2 * m + 2).wait()

        product(2 * m + 1, odd_ref)
        activate(2 * m, even_ref)
        product(jnp.minimum(2 * m + 2, count - 1), even_ref)
        activate(2 * m + 1, odd_ref)
        return carry

    lax.fori_loop(0, count // 2, forward, 0)
    value = jnp.sum(total_ref[...], axis=1, keepdims=True) + b_out_ref[:, 0:1]
    error = value - reward
    grad_value = error * scale

    each = (STEPS * iota((ROWS, ROWS // STEPS), 1)) - iota((ROWS, ROWS // STEPS), 0)
    for s in range(STEPS):
        td_rows_ref[s : s + 1, :] = jnp.sum(
            jnp.where(each + s == 0, error, 0.0), axis=0, keepdims=True
        )

    td_copy = pltpu.make_async_copy(td_rows_ref, td_ref, td_sem)
    td_copy.start()

    total_value = jnp.sum(grad_value, axis=0, keepdims=True)

    def backward(n, carry):
        at = pl.ds(pl.multiple_of(n * CHUNK, CHUNK), CHUNK)
        grad_pre = grad_value * slope_ref[:, at]
        send_ref[:ROWS, at] = grad_pre.astype(BF16)
        first = jnp.sum(grad_pre, axis=0, keepdims=True)
        second = jnp.sum(grad_value * hidden_ref[:, at].astype(F32), axis=0, keepdims=True)
        third = jnp.broadcast_to(total_value, (1, CHUNK))
        rows = stack_rows(three(first) + three(second) + three(third), 16)
        send_ref[ROWS + 48 : ROWS + 64, at] = rows.astype(BF16)
        return carry

    lax.fori_loop(0, H // CHUNK, backward, 0)
    td_copy.wait()


PACK = 424
BLOCK = 88


def product_kernel(own_ref, other_ref, keep_ref, out_ref, left_ref):
    for b in range(H // ROWS):
        left_ref[b * 48 : (b + 1) * 48, :] = other_ref[
            ROWS : ROWS + 48, b * ROWS : (b + 1) * ROWS
        ]
    keep = keep_ref[...]
    left = left_ref[...]
    for n in range(H // CHUNK):
        at = slice(n * CHUNK, (n + 1) * CHUNK)
        part = dot(keep, own_ref[:ROWS, at]) + dot(left, other_ref[:ROWS, at])
        for p in range(N_PLANE):
            for i in range(3):
                tile = part[p * SLAB + 8 * i : p * SLAB + 8 * i + 8]
                pair = jnp.concatenate([tile[:, :LANES], tile[:, LANES:]], axis=0)
                start = p * PACK + (16 * i + 2 * n) * 8
                out_ref[start : start + 16, :] = pair.astype(BF16)
    mine = own_ref[ROWS + 48 : ROWS + 64, :].astype(F32)
    theirs = other_ref[ROWS + 48 : ROWS + 64, :].astype(F32)
    rows = []
    for q in range(3):
        a = mine[3 * q : 3 * q + 1] + mine[3 * q + 1 : 3 * q + 2] + mine[3 * q + 2 : 3 * q + 3]
        b = theirs[3 * q : 3 * q + 1] + theirs[3 * q + 1 : 3 * q + 2] + theirs[3 * q + 2 : 3 * q + 3]
        rows.append(a + b)
    blocks = []
    for r in rows[:2]:
        pieces = [r[:, b * LANES : (b + 1) * LANES] for b in range(H // LANES)]
        blocks.append(jnp.concatenate(pieces, axis=0))
    blocks.append(stack_rows(two(rows[2][:, :LANES]), 8))
    small = jnp.concatenate(blocks, axis=0).astype(BF16)
    for p in range(N_PLANE):
        out_ref[p * PACK + HALF : (p + 1) * PACK, :] = small


def plane_kernel(got_ref, out_ref, sum_ref, wide_ref):
    for b in range(PACK // 8):
        total = got_ref[b * 8 : b * 8 + 8, :].astype(F32)
        for p in range(1, N_PLANE):
            total = total + got_ref[p * PACK + b * 8 : p * PACK + b * 8 + 8, :].astype(F32)
        sum_ref[b * 8 : b * 8 + 8, :] = total
    for n in range(48):
        wide_ref[pl.ds(n, N_LINE, stride=48), :] = sum_ref[8 * n : 8 * n + 8, :]
    last = sum_ref[416:417, :] + sum_ref[417:418, :]
    small = jnp.concatenate(
        (sum_ref[384:416, :], stack_rows(two(last), 8)),
        axis=0,
    ).astype(BF16)
    for z in range(N_LINE):
        out_ref[z * BLOCK : z * BLOCK + 48, :] = wide_ref[z * 48 : z * 48 + 48, :].astype(BF16)
        out_ref[z * BLOCK + 48 : (z + 1) * BLOCK, :] = small


def line_kernel(got_ref, w_ref, b_in_ref, w_out_ref, b_out_ref, sum_ref):
    for b in range(BLOCK // 8):
        total = got_ref[b * 8 : b * 8 + 8, :].astype(F32)
        for z in range(1, N_LINE):
            total = total + got_ref[z * BLOCK + b * 8 : z * BLOCK + b * 8 + 8, :].astype(F32)
        sum_ref[b * 8 : b * 8 + 8, :] = total
    for i in range(3):
        for b in range(H // LANES):
            w_ref[i : i + 1, b * LANES : (b + 1) * LANES] = sum_ref[i * 16 + b : i * 16 + b + 1, :]
    b_in_ref[...] = sum_ref[48:64, :]
    w_out_ref[...] = sum_ref[64:80, :]
    b_out_ref[...] = sum_ref[80:81, :] + sum_ref[81:82, :]


def call(kernel, shapes, operands, scratch, flops, grant, in_hbm=(), out_hbm=()):
    specs = [pl.BlockSpec(memory_space=pltpu.VMEM)] * len(operands)
    for n in in_hbm:
        specs[n] = pl.BlockSpec(memory_space=pltpu.HBM)
    back = [pl.BlockSpec(memory_space=pltpu.VMEM)] * len(shapes)
    for n in out_hbm:
        back[n] = pl.BlockSpec(memory_space=pltpu.HBM)
    outs = [jax.ShapeDtypeStruct(shape, kind) for shape, kind in shapes]
    return pl.pallas_call(
        kernel,
        out_shape=outs,
        in_specs=specs,
        out_specs=back,
        scratch_shapes=scratch,
        compiler_params=pltpu.CompilerParams(vmem_limit_bytes=grant << 20),
        cost_estimate=pl.CostEstimate(flops=flops, bytes_accessed=1 << 20, transcendentals=0),
    )(*operands)


def body(state_feats, achieved, offsets, w_in, b_in, w_out, b_out):
    place = jnp.stack([lax.axis_index(TM), lax.axis_index("dp")]).astype(I32)
    place = jnp.broadcast_to(place[:, None], (2, LANES))
    table = achieved.reshape(ROWS, G)
    state = state_feats.reshape(ROWS, S)
    many, offs = call(
        spread_kernel,
        [((N_TM, 1, ROWS), I32), ((1, ROWS), I32)],
        (offsets.T,),
        [],
        10**6,
        60,
    )
    known = lax.all_to_all(many, TM, split_axis=0, concat_axis=0, tiled=True)
    (picked,) = call(
        pick_kernel,
        [((N_TM * 16, LANES), BF16)],
        (place, known, table),
        [
            pltpu.VMEM((N_TM * 16 + 16, LANES), F32),
            pltpu.VMEM((N_TM * 16, LANES), BF16),
            pltpu.SemaphoreType.DMA((2,)),
        ],
        10**8,
        8,
        (),
        (0,),
    )
    goal_w, near, at = call(
        ahead_kernel,
        [((G, H), BF16), ((ROWS, G), BF16), ((ROWS, LANES), I32)],
        (place, offs, table, w_in),
        [],
        10**9,
        12,
    )
    fetched = lax.all_to_all(
        picked.reshape(N_TM, 16, LANES), TM, split_axis=0, concat_axis=0, tiled=True
    ).reshape(N_TM * 16, LANES)
    head_bias = jnp.broadcast_to(b_out[None], (1, LANES))
    scale = 1.0 / math.sqrt(ROWS * N_TM * 2)
    td, send, keep = call(
        functools.partial(main_kernel, scale),
        [((STEPS, ROWS // STEPS), F32), ((ROWS + 64, H), BF16), ((HALF, ROWS), BF16)],
        (
            place,
            head_bias,
            fetched,
            goal_w,
            near,
            at,
            table,
            state,
            w_in,
            b_in.reshape(1, H),
            w_out.reshape(1, H),
        ),
        [
            pltpu.VMEM((ROWS, H), F32),
            pltpu.VMEM((ROWS, H), BF16),
            pltpu.VMEM((ROWS, S + G), BF16),
            pltpu.VMEM((S, H), BF16),
            pltpu.VMEM((N_TM * 16 + 16, LANES), F32),
            pltpu.VMEM((ROWS, LANES), F32),
            pltpu.VMEM((STEPS, ROWS // STEPS), F32),
            pltpu.VMEM((ROWS, CHUNK), F32),
            pltpu.VMEM((ROWS, CHUNK), F32),
            pltpu.SemaphoreType.DMA((H // CHUNK,)),
            pltpu.SemaphoreType.DMA,
        ],
        2 * 10**9,
        48,
        (8,),
        (0,),
    )
    other = lax.ppermute(send, "dp", [(0, 1), (1, 0)])
    (packs,) = call(
        product_kernel,
        [((N_PLANE * PACK, LANES), BF16)],
        (send, other, keep),
        [pltpu.VMEM((HALF, ROWS), BF16)],
        10**9,
        12,
    )
    got = lax.all_to_all(
        packs.reshape(N_PLANE, PACK, LANES), PLANE, split_axis=0, concat_axis=0, tiled=True
    ).reshape(N_PLANE * PACK, LANES)
    (lines,) = call(
        plane_kernel,
        [((N_LINE * BLOCK, LANES), BF16)],
        (got,),
        [pltpu.VMEM((PACK, LANES), F32), pltpu.VMEM((N_LINE * 48 + 48, LANES), F32)],
        10**7,
        6,
    )
    got = lax.all_to_all(
        lines.reshape(N_LINE, BLOCK, LANES), LINE, split_axis=0, concat_axis=0, tiled=True
    ).reshape(N_LINE * BLOCK, LANES)
    grad_w_in, grad_b_in, grad_w_out, grad_b_out = call(
        line_kernel,
        [((3, H), F32), ((16, LANES), F32), ((16, LANES), F32), ((1, LANES), F32)],
        (got,),
        [pltpu.VMEM((BLOCK, LANES), F32)],
        10**6,
        4,
    )
    return td.T, grad_w_in, grad_b_in.reshape(H), grad_w_out.reshape(H), grad_b_out[0, :1]


def solution(mesh):
    split = Mesh(mesh.devices.reshape(4, 4, 8, mesh.shape["dp"]), TM_DP)
    placed = (P("dp", TM, None), P("dp", TM, None), P("dp", TM), P(), P(), P(), P())
    return jax.shard_map(
        body,
        mesh=split,
        in_specs=placed,
        out_specs=(P("dp", TM), P(TM_DP, None), P(), P(), P()),
        check_vma=False,
    )
```

```python
import functools
import math

import jax
import jax.numpy as jnp
from jax import lax
from jax.experimental import pallas as pl
from jax.experimental.pallas import tpu as pltpu
from jax.sharding import Mesh
from jax.sharding import PartitionSpec as P

CAP = 4
TM = ("tm_0", "tm_1", "tm_2")
TM_DP = ("tm_0", "tm_1", "tm_2", "dp")
PLANE = ("tm_0", "tm_1")
LINE = "tm_2"
N_TM = 128
N_PLANE = 16
N_LINE = 8
ROWS = 256
STEPS = 4
S = 256
G = 512
H = 2048
LANES = 128
HALF = (S + G) // 2
SLAB = HALF // N_PLANE
CHUNK = 256
F32 = jnp.float32
BF16 = jnp.bfloat16
I32 = jnp.int32


def iota(shape, dim):
    return lax.broadcasted_iota(I32, shape, dim)


def dot(a, b, dims=(((1,), (0,)), ((), ()))):
    return lax.dot_general(a, b, dims, preferred_element_type=F32)


def flag(mask):
    return jnp.where(mask, 1.0, 0.0)


def spread_kernel(offs_ref, many_ref, row_ref):
    offs = offs_ref[...]
    parts = jnp.concatenate([offs >> 4, offs & 15], axis=0).astype(F32).astype(BF16)
    episode = flag((iota((ROWS // STEPS, ROWS), 1) >> 2) == iota((ROWS // STEPS, ROWS), 0))
    wide = dot(parts, episode.astype(BF16))
    step = iota((2 * STEPS, ROWS), 1) & (STEPS - 1)
    which = iota((2 * STEPS, ROWS), 0)
    mine = (which & (STEPS - 1)) == step
    weight = jnp.where(which < STEPS, 16.0, 1.0)
    row = jnp.sum(jnp.where(mine, wide * weight, 0.0), axis=0, keepdims=True).astype(I32)
    row_ref[...] = row
    many_ref[...] = jnp.broadcast_to(row[None], (N_TM, 1, ROWS))


def pick_kernel(place_ref, offs_ref, table_ref, out_ref, wide_ref, ready_ref, sems):
    me = place_ref[0:1, 0:1]
    offs = offs_ref[...].reshape(N_TM, ROWS)
    peer = iota((N_TM, ROWS), 0)
    row = iota((N_TM, ROWS), 1)
    target = peer * STEPS + (row & (STEPS - 1)) + offs
    hit = ((target >> 2) == me) & (peer != me)
    earlier = flag(iota((ROWS, ROWS), 0) < iota((ROWS, ROWS), 1)).astype(BF16)
    rank = dot(flag(hit).astype(BF16), earlier)
    position = ((row - (row & (STEPS - 1))) + (target & (STEPS - 1)) + 1).astype(F32)
    wanted = []
    for c in range(CAP):
        place = jnp.sum(
            jnp.where(hit & (rank == float(c)), position, 0.0), axis=1, keepdims=True
        )
        wanted.append(flag(row.astype(F32) + 1.0 == place).astype(BF16))
    half = N_TM // 2
    copies = []
    for h in range(2):
        part = jnp.concatenate([w[h * half : (h + 1) * half] for w in wanted], axis=0)
        picked = dot(part, table_ref[...])
        for c in range(CAP):
            for j in range(G // LANES):
                at = pl.ds(h * half * 16 + c * (G // LANES) + j, half, stride=16)
                wide_ref[at, :] = picked[
                    c * half : (c + 1) * half, j * LANES : (j + 1) * LANES
                ]
        rows = slice(h * half * 16, (h + 1) * half * 16)
        ready_ref[rows, :] = wide_ref[rows, :].astype(BF16)
        there = pl.ds(h * half * 16, half * 16)
        copies.append(
            pltpu.make_async_copy(ready_ref.at[there, :], out_ref.at[there, :], sems.at[h])
        )
        copies[-1].start()
    for copy in copies:
        copy.wait()


def half_rows(core):
    k = iota((HALF, S + G), 0)
    eighth = k >> 3
    plane = (eighth * 171) >> 9
    within = eighth - plane * 3
    feature = (plane * N_LINE + (k & 7)) * 6 + core * 3 + within
    return flag(iota((HALF, S + G), 1) == feature).astype(BF16)


def three(x):
    high = x.astype(BF16).astype(F32)
    rest = x - high
    middle = rest.astype(BF16).astype(F32)
    return high, middle, rest - middle


def two(x):
    high = x.astype(BF16).astype(F32)
    return high, x - high


def stack_rows(rows, count):
    width = rows[0].shape[1]
    at = iota((count, width), 0)
    total = jnp.zeros((count, width), F32)
    for n, r in enumerate(rows):
        total = jnp.where(at == n, jnp.broadcast_to(r, (count, width)), total)
    return total


def ahead_kernel(
    place_ref,
    offs_ref,
    table_ref,
    w_in_ref,
    goal_w_ref,
    near_ref,
    at_ref,
):
    me = place_ref[0:1, 0:1]
    row = iota((ROWS, ROWS), 1)
    col = iota((ROWS, ROWS), 0)
    lane = iota((1, ROWS), 1)
    target = me * STEPS + (lane & (STEPS - 1)) + offs_ref[...]
    owner_lane = (target >> 2).astype(F32)
    position_lane = ((lane - (lane & (STEPS - 1))) + (target & (STEPS - 1))).astype(F32)

    def to_column(x):
        return jnp.sum(
            jnp.where(row == col, jnp.broadcast_to(x, (ROWS, ROWS)), 0.0),
            axis=1,
            keepdims=True,
        )

    owner = to_column(owner_lane)
    position = to_column(position_lane)
    slot = jnp.sum(flag((owner == owner_lane) & (row < col)), axis=1, keepdims=True)
    remote = owner != me.astype(F32)
    near_at = jnp.where(remote, -1.0, position)
    far_at = jnp.where(remote, owner * float(CAP) + slot, -1.0).astype(I32)
    near = flag(row.astype(F32) == near_at).astype(BF16)
    near_ref[...] = dot(near, table_ref[...]).astype(BF16)
    at_ref[...] = jnp.broadcast_to(far_at, (ROWS, LANES))
    goal_w_ref[...] = w_in_ref[S:, :]


def main_kernel(
    scale,
    place_ref,
    b_out_ref,
    fetched_ref,
    goal_w_ref,
    near_ref,
    at_ref,
    table_ref,
    state_ref,
    w_in_ref,
    b_in_ref,
    w_out_ref,
    td_ref,
    send_ref,
    inputs_ref,
    slope_ref,
    hidden_ref,
    state_w_ref,
    wide_ref,
    total_ref,
    td_rows_ref,
    even_ref,
    odd_ref,
    sums_ref,
    sems,
    td_sem,
):
    def load(n):
        at = pl.ds(pl.multiple_of(n * CHUNK, CHUNK), CHUNK)
        return pltpu.make_async_copy(
            w_in_ref.at[pl.ds(0, S), at], state_w_ref.at[:, at], sems.at[n]
        )

    def begin(n, carry):
        load(n).start()
        return carry

    lax.fori_loop(0, H // CHUNK, begin, 0)
    core = place_ref[1:2, 0:1]
    far_at = at_ref[:, 0:1]
    far = flag(iota((ROWS, N_TM * CAP), 1) == far_at).astype(BF16)
    inputs_ref[:, :S] = state_ref[...]
    wide_ref[: N_TM * 16, :] = fetched_ref[...].astype(F32)
    gap = jnp.zeros((ROWS, LANES), F32)
    for j in range(G // LANES):
        at = slice(j * LANES, (j + 1) * LANES)
        fetched = wide_ref[pl.ds(j, N_TM * CAP, stride=G // LANES), :].astype(BF16)
        goal = dot(far, fetched) + near_ref[:, at].astype(F32)
        diff = table_ref[:, at].astype(F32) - goal
        gap = gap + diff * diff
        inputs_ref[:, S + j * LANES : S + (j + 1) * LANES] = goal.astype(BF16)
    reward = -(jnp.sum(gap, axis=1, keepdims=True) * (1.0 / G))
    inputs = inputs_ref[...]

    sent = dot(half_rows(1 - core), inputs, (((1,), (1,)), ((), ()))).astype(BF16)
    for b in range(H // ROWS):
        send_ref[ROWS : ROWS + 48, b * ROWS : (b + 1) * ROWS] = sent[b * 48 : (b + 1) * 48, :]

    total_ref[...] = jnp.zeros((ROWS, LANES), F32)

    def product(n, buffer_ref):
        at = pl.ds(pl.multiple_of(n * CHUNK, CHUNK), CHUNK)
        buffer_ref[...] = dot(inputs[:, :S], state_w_ref[:, at]) + dot(
            inputs[:, S:], goal_w_ref[:, at]
        )

    def activate(n, buffer_ref):
        at = pl.ds(pl.multiple_of(n * CHUNK, CHUNK), CHUNK)
        pre = buffer_ref[...] + b_in_ref[:, at]
        sig = 0.5 * jnp.tanh(0.5 * pre) + 0.5
        head = w_out_ref[:, at]
        act = pre * sig
        hidden = act.astype(BF16)
        hidden_ref[:, at] = hidden
        slope_ref[:, at] = head * (sig + act * (1.0 - sig))
        term = hidden.astype(F32) * head
        total_ref[...] += term[:, :LANES] + term[:, LANES:]

    count = H // CHUNK
    load(0).wait()
    product(0, even_ref)

    def forward(m, carry):
        load(2 * m + 1).wait()

        @pl.when(2 * m + 2 < count)
        def _():
            load(2 * m + 2).wait()

        product(2 * m + 1, odd_ref)
        activate(2 * m, even_ref)
        product(jnp.minimum(2 * m + 2, count - 1), even_ref)
        activate(2 * m + 1, odd_ref)
        return carry

    lax.fori_loop(0, count // 2, forward, 0)
    value = jnp.sum(total_ref[...], axis=1, keepdims=True) + b_out_ref[:, 0:1]
    error = value - reward
    grad_value = error * scale

    each = (STEPS * iota((ROWS, ROWS // STEPS), 1)) - iota((ROWS, ROWS // STEPS), 0)
    for s in range(STEPS):
        td_rows_ref[s : s + 1, :] = jnp.sum(
            jnp.where(each + s == 0, error, 0.0), axis=0, keepdims=True
        )

    td_copy = pltpu.make_async_copy(td_rows_ref, td_ref, td_sem)
    td_copy.start()

    total_value = jnp.sum(grad_value, axis=0, keepdims=True)

    def backward(n, carry):
        at = pl.ds(pl.multiple_of(n * CHUNK, CHUNK), CHUNK)
        grad_pre = grad_value * slope_ref[:, at]
        send_ref[:ROWS, at] = grad_pre.astype(BF16)
        first = jnp.sum(grad_pre, axis=0, keepdims=True)
        second = jnp.sum(grad_value * hidden_ref[:, at].astype(F32), axis=0, keepdims=True)
        sums_ref[0:1, at] = first
        sums_ref[1:2, at] = second
        return carry

    lax.fori_loop(0, H // CHUNK, backward, 0)
    third = jnp.broadcast_to(total_value, (1, H))
    rows = three(sums_ref[0:1, :]) + three(sums_ref[1:2, :]) + three(third)
    send_ref[ROWS + 48 : ROWS + 64, :] = stack_rows(rows, 16).astype(BF16)
    td_copy.wait()


def keep_kernel(place_ref, inputs_ref, keep_ref):
    core = place_ref[1:2, 0:1]
    keep_ref[...] = dot(half_rows(core), inputs_ref[...], (((1,), (1,)), ((), ()))).astype(BF16)


PACK = 424
BLOCK = 88


def product_kernel(own_ref, other_ref, keep_ref, out_ref, left_ref):
    for b in range(H // ROWS):
        left_ref[b * 48 : (b + 1) * 48, :] = other_ref[
            ROWS : ROWS + 48, b * ROWS : (b + 1) * ROWS
        ]
    keep = keep_ref[...]
    left = left_ref[...]
    for n in range(H // CHUNK):
        at = slice(n * CHUNK, (n + 1) * CHUNK)
        part = dot(keep, own_ref[:ROWS, at]) + dot(left, other_ref[:ROWS, at])
        for p in range(N_PLANE):
            for i in range(3):
                tile = part[p * SLAB + 8 * i : p * SLAB + 8 * i + 8]
                pair = jnp.concatenate([tile[:, :LANES], tile[:, LANES:]], axis=0)
                start = p * PACK + (16 * i + 2 * n) * 8
                out_ref[start : start + 16, :] = pair.astype(BF16)
    mine = own_ref[ROWS + 48 : ROWS + 64, :].astype(F32)
    theirs = other_ref[ROWS + 48 : ROWS + 64, :].astype(F32)
    rows = []
    for q in range(3):
        a = mine[3 * q : 3 * q + 1] + mine[3 * q + 1 : 3 * q + 2] + mine[3 * q + 2 : 3 * q + 3]
        b = theirs[3 * q : 3 * q + 1] + theirs[3 * q + 1 : 3 * q + 2] + theirs[3 * q + 2 : 3 * q + 3]
        rows.append(a + b)
    blocks = []
    for r in rows[:2]:
        pieces = [r[:, b * LANES : (b + 1) * LANES] for b in range(H // LANES)]
        blocks.append(jnp.concatenate(pieces, axis=0))
    blocks.append(stack_rows(two(rows[2][:, :LANES]), 8))
    small = jnp.concatenate(blocks, axis=0).astype(BF16)
    for p in range(N_PLANE):
        out_ref[p * PACK + HALF : (p + 1) * PACK, :] = small


def plane_kernel(got_ref, out_ref, sum_ref, wide_ref):
    for b in range(PACK // 8):
        total = got_ref[b * 8 : b * 8 + 8, :].astype(F32)
        for p in range(1, N_PLANE):
            total = total + got_ref[p * PACK + b * 8 : p * PACK + b * 8 + 8, :].astype(F32)
        sum_ref[b * 8 : b * 8 + 8, :] = total
    for n in range(48):
        wide_ref[pl.ds(n, N_LINE, stride=48), :] = sum_ref[8 * n : 8 * n + 8, :]
    last = sum_ref[416:417, :] + sum_ref[417:418, :]
    small = jnp.concatenate(
        (sum_ref[384:416, :], stack_rows(two(last), 8)),
        axis=0,
    ).astype(BF16)
    for z in range(N_LINE):
        out_ref[z * BLOCK : z * BLOCK + 48, :] = wide_ref[z * 48 : z * 48 + 48, :].astype(BF16)
        out_ref[z * BLOCK + 48 : (z + 1) * BLOCK, :] = small


def line_kernel(got_ref, w_ref, b_in_ref, w_out_ref, b_out_ref, sum_ref):
    for b in range(BLOCK // 8):
        total = got_ref[b * 8 : b * 8 + 8, :].astype(F32)
        for z in range(1, N_LINE):
            total = total + got_ref[z * BLOCK + b * 8 : z * BLOCK + b * 8 + 8, :].astype(F32)
        sum_ref[b * 8 : b * 8 + 8, :] = total
    for i in range(3):
        for b in range(H // LANES):
            w_ref[i : i + 1, b * LANES : (b + 1) * LANES] = sum_ref[i * 16 + b : i * 16 + b + 1, :]
    b_in_ref[...] = sum_ref[48:64, :]
    w_out_ref[...] = sum_ref[64:80, :]
    b_out_ref[...] = sum_ref[80:81, :] + sum_ref[81:82, :]


def call(kernel, shapes, operands, scratch, flops, grant, in_hbm=(), out_hbm=()):
    specs = [pl.BlockSpec(memory_space=pltpu.VMEM)] * len(operands)
    for n in in_hbm:
        specs[n] = pl.BlockSpec(memory_space=pltpu.HBM)
    back = [pl.BlockSpec(memory_space=pltpu.VMEM)] * len(shapes)
    for n in out_hbm:
        back[n] = pl.BlockSpec(memory_space=pltpu.HBM)
    outs = [jax.ShapeDtypeStruct(shape, kind) for shape, kind in shapes]
    return pl.pallas_call(
        kernel,
        out_shape=outs,
        in_specs=specs,
        out_specs=back,
        scratch_shapes=scratch,
        compiler_params=pltpu.CompilerParams(vmem_limit_bytes=grant << 20),
        cost_estimate=pl.CostEstimate(flops=flops, bytes_accessed=1 << 20, transcendentals=0),
    )(*operands)


def body(state_feats, achieved, offsets, w_in, b_in, w_out, b_out):
    place = jnp.stack([lax.axis_index(TM), lax.axis_index("dp")]).astype(I32)
    place = jnp.broadcast_to(place[:, None], (2, LANES))
    table = achieved.reshape(ROWS, G)
    state = state_feats.reshape(ROWS, S)
    many, offs = call(
        spread_kernel,
        [((N_TM, 1, ROWS), I32), ((1, ROWS), I32)],
        (offsets.T,),
        [],
        10**6,
        60,
    )
    known = lax.all_to_all(many, TM, split_axis=0, concat_axis=0, tiled=True)
    (picked,) = call(
        pick_kernel,
        [((N_TM * 16, LANES), BF16)],
        (place, known, table),
        [
            pltpu.VMEM((N_TM * 16 + 16, LANES), F32),
            pltpu.VMEM((N_TM * 16, LANES), BF16),
            pltpu.SemaphoreType.DMA((2,)),
        ],
        10**8,
        8,
        (),
        (0,),
    )
    goal_w, near, at = call(
        ahead_kernel,
        [((G, H), BF16), ((ROWS, G), BF16), ((ROWS, LANES), I32)],
        (place, offs, table, w_in),
        [],
        10**9,
        12,
    )
    fetched = lax.all_to_all(
        picked.reshape(N_TM, 16, LANES), TM, split_axis=0, concat_axis=0, tiled=True
    ).reshape(N_TM * 16, LANES)
    head_bias = jnp.broadcast_to(b_out[None], (1, LANES))
    scale = 1.0 / math.sqrt(ROWS * N_TM * 2)
    td, send, inputs = call(
        functools.partial(main_kernel, scale),
        [((STEPS, ROWS // STEPS), F32), ((ROWS + 64, H), BF16), ((ROWS, S + G), BF16)],
        (
            place,
            head_bias,
            fetched,
            goal_w,
            near,
            at,
            table,
            state,
            w_in,
            b_in.reshape(1, H),
            w_out.reshape(1, H),
        ),
        [
            pltpu.VMEM((ROWS, H), F32),
            pltpu.VMEM((ROWS, H), BF16),
            pltpu.VMEM((S, H), BF16),
            pltpu.VMEM((N_TM * 16 + 16, LANES), F32),
            pltpu.VMEM((ROWS, LANES), F32),
            pltpu.VMEM((STEPS, ROWS // STEPS), F32),
            pltpu.VMEM((ROWS, CHUNK), F32),
            pltpu.VMEM((ROWS, CHUNK), F32),
            pltpu.VMEM((8, H), F32),
            pltpu.SemaphoreType.DMA((H // CHUNK,)),
            pltpu.SemaphoreType.DMA,
        ],
        2 * 10**9,
        48,
        (8,),
        (0,),
    )
    other = lax.ppermute(send, "dp", [(0, 1), (1, 0)])
    (keep,) = call(
        keep_kernel, [((HALF, ROWS), BF16)], (place, inputs), [], 10**9, 8
    )
    (packs,) = call(
        product_kernel,
        [((N_PLANE * PACK, LANES), BF16)],
        (send, other, keep),
        [pltpu.VMEM((HALF, ROWS), BF16)],
        10**9,
        12,
    )
    got = lax.all_to_all(
        packs.reshape(N_PLANE, PACK, LANES), PLANE, split_axis=0, concat_axis=0, tiled=True
    ).reshape(N_PLANE * PACK, LANES)
    (lines,) = call(
        plane_kernel,
        [((N_LINE * BLOCK, LANES), BF16)],
        (got,),
        [pltpu.VMEM((PACK, LANES), F32), pltpu.VMEM((N_LINE * 48 + 48, LANES), F32)],
        10**7,
        6,
    )
    got = lax.all_to_all(
        lines.reshape(N_LINE, BLOCK, LANES), LINE, split_axis=0, concat_axis=0, tiled=True
    ).reshape(N_LINE * BLOCK, LANES)
    grad_w_in, grad_b_in, grad_w_out, grad_b_out = call(
        line_kernel,
        [((3, H), F32), ((16, LANES), F32), ((16, LANES), F32), ((1, LANES), F32)],
        (got,),
        [pltpu.VMEM((BLOCK, LANES), F32)],
        10**6,
        4,
    )
    return td.T, grad_w_in, grad_b_in.reshape(H), grad_w_out.reshape(H), grad_b_out[0, :1]


def solution(mesh):
    split = Mesh(mesh.devices.reshape(4, 4, 8, mesh.shape["dp"]), TM_DP)
    placed = (P("dp", TM, None), P("dp", TM, None), P("dp", TM), P(), P(), P(), P())
    return jax.shard_map(
        body,
        mesh=split,
        in_specs=placed,
        out_specs=(P("dp", TM), P(TM_DP, None), P(), P(), P()),
        check_vma=False,
    )
```

```python
import functools
import math

import jax
import jax.numpy as jnp
from jax import lax
from jax.experimental import pallas as pl
from jax.experimental.pallas import tpu as pltpu
from jax.sharding import Mesh
from jax.sharding import PartitionSpec as P

CAP = 4
TM = ("tm_0", "tm_1", "tm_2")
TM_DP = ("tm_0", "tm_1", "tm_2", "dp")
PLANE = ("tm_0", "tm_1")
LINE = "tm_2"
N_TM = 128
N_PLANE = 16
N_LINE = 8
ROWS = 256
STEPS = 4
S = 256
G = 512
H = 2048
LANES = 128
HALF = (S + G) // 2
SLAB = HALF // N_PLANE
CHUNK = 256
F32 = jnp.float32
BF16 = jnp.bfloat16
I32 = jnp.int32


def iota(shape, dim):
    return lax.broadcasted_iota(I32, shape, dim)


def dot(a, b, dims=(((1,), (0,)), ((), ()))):
    return lax.dot_general(a, b, dims, preferred_element_type=F32)


def flag(mask):
    return jnp.where(mask, 1.0, 0.0)


def spread_kernel(offs_ref, many_ref, row_ref):
    offs = offs_ref[...]
    parts = jnp.concatenate([offs >> 4, offs & 15], axis=0).astype(F32).astype(BF16)
    episode = flag((iota((ROWS // STEPS, ROWS), 1) >> 2) == iota((ROWS // STEPS, ROWS), 0))
    wide = dot(parts, episode.astype(BF16))
    step = iota((2 * STEPS, ROWS), 1) & (STEPS - 1)
    which = iota((2 * STEPS, ROWS), 0)
    mine = (which & (STEPS - 1)) == step
    weight = jnp.where(which < STEPS, 16.0, 1.0)
    row = jnp.sum(jnp.where(mine, wide * weight, 0.0), axis=0, keepdims=True).astype(I32)
    row_ref[...] = row
    many_ref[...] = jnp.broadcast_to(row[None], (N_TM, 1, ROWS))


def pick_kernel(place_ref, offs_ref, table_ref, out_ref, wide_ref, ready_ref, sems):
    me = place_ref[0:1, 0:1]
    offs = offs_ref[...].reshape(N_TM, ROWS)
    peer = iota((N_TM, ROWS), 0)
    row = iota((N_TM, ROWS), 1)
    target = peer * STEPS + (row & (STEPS - 1)) + offs
    hit = ((target >> 2) == me) & (peer != me)
    earlier = flag(iota((ROWS, ROWS), 0) < iota((ROWS, ROWS), 1)).astype(BF16)
    rank = dot(flag(hit).astype(BF16), earlier)
    position = ((row - (row & (STEPS - 1))) + (target & (STEPS - 1)) + 1).astype(F32)
    wanted = []
    for c in range(CAP):
        place = jnp.sum(
            jnp.where(hit & (rank == float(c)), position, 0.0), axis=1, keepdims=True
        )
        wanted.append(flag(row.astype(F32) + 1.0 == place).astype(BF16))
    half = N_TM // 4
    copies = []
    for h in range(4):
        part = jnp.concatenate([w[h * half : (h + 1) * half] for w in wanted], axis=0)
        picked = dot(part, table_ref[...])
        for c in range(CAP):
            for j in range(G // LANES):
                at = pl.ds(h * half * 16 + c * (G // LANES) + j, half, stride=16)
                wide_ref[at, :] = picked[
                    c * half : (c + 1) * half, j * LANES : (j + 1) * LANES
                ]
        rows = slice(h * half * 16, (h + 1) * half * 16)
        ready_ref[rows, :] = wide_ref[rows, :].astype(BF16)
        there = pl.ds(h * half * 16, half * 16)
        copies.append(
            pltpu.make_async_copy(ready_ref.at[there, :], out_ref.at[there, :], sems.at[h])
        )
        copies[-1].start()
    for copy in copies:
        copy.wait()


def half_rows(core):
    k = iota((HALF, S + G), 0)
    eighth = k >> 3
    plane = (eighth * 171) >> 9
    within = eighth - plane * 3
    feature = (plane * N_LINE + (k & 7)) * 6 + core * 3 + within
    return flag(iota((HALF, S + G), 1) == feature).astype(BF16)


def three(x):
    high = x.astype(BF16).astype(F32)
    rest = x - high
    middle = rest.astype(BF16).astype(F32)
    return high, middle, rest - middle


def two(x):
    high = x.astype(BF16).astype(F32)
    return high, x - high


def stack_rows(rows, count):
    width = rows[0].shape[1]
    at = iota((count, width), 0)
    total = jnp.zeros((count, width), F32)
    for n, r in enumerate(rows):
        total = jnp.where(at == n, jnp.broadcast_to(r, (count, width)), total)
    return total


def ahead_kernel(
    place_ref,
    offs_ref,
    table_ref,
    w_in_ref,
    goal_w_ref,
    near_ref,
    at_ref,
):
    me = place_ref[0:1, 0:1]
    row = iota((ROWS, ROWS), 1)
    col = iota((ROWS, ROWS), 0)
    lane = iota((1, ROWS), 1)
    target = me * STEPS + (lane & (STEPS - 1)) + offs_ref[...]
    owner_lane = (target >> 2).astype(F32)
    position_lane = ((lane - (lane & (STEPS - 1))) + (target & (STEPS - 1))).astype(F32)

    def to_column(x):
        return jnp.sum(
            jnp.where(row == col, jnp.broadcast_to(x, (ROWS, ROWS)), 0.0),
            axis=1,
            keepdims=True,
        )

    owner = to_column(owner_lane)
    position = to_column(position_lane)
    slot = jnp.sum(flag((owner == owner_lane) & (row < col)), axis=1, keepdims=True)
    remote = owner != me.astype(F32)
    near_at = jnp.where(remote, -1.0, position)
    far_at = jnp.where(remote, owner * float(CAP) + slot, -1.0).astype(I32)
    near = flag(row.astype(F32) == near_at).astype(BF16)
    near_ref[...] = dot(near, table_ref[...]).astype(BF16)
    at_ref[...] = jnp.broadcast_to(far_at, (ROWS, LANES))
    goal_w_ref[...] = w_in_ref[S:, :]


def main_kernel(
    scale,
    place_ref,
    b_out_ref,
    fetched_ref,
    goal_w_ref,
    near_ref,
    at_ref,
    table_ref,
    state_ref,
    w_in_ref,
    b_in_ref,
    w_out_ref,
    td_ref,
    send_ref,
    keep_ref,
    slope_ref,
    hidden_ref,
    inputs_ref,
    state_w_ref,
    wide_ref,
    total_ref,
    td_rows_ref,
    even_ref,
    odd_ref,
    sems,
    td_sem,
):
    def load(n):
        at = pl.ds(pl.multiple_of(n * CHUNK, CHUNK), CHUNK)
        return pltpu.make_async_copy(
            w_in_ref.at[pl.ds(0, S), at], state_w_ref.at[:, at], sems.at[n]
        )

    def begin(n, carry):
        load(n).start()
        return carry

    lax.fori_loop(0, H // CHUNK, begin, 0)
    core = place_ref[1:2, 0:1]
    far_at = at_ref[:, 0:1]
    far = flag(iota((ROWS, N_TM * CAP), 1) == far_at).astype(BF16)
    inputs_ref[:, :S] = state_ref[...]
    wide_ref[: N_TM * 16, :] = fetched_ref[...].astype(F32)
    gap = jnp.zeros((ROWS, LANES), F32)
    for j in range(G // LANES):
        at = slice(j * LANES, (j + 1) * LANES)
        fetched = wide_ref[pl.ds(j, N_TM * CAP, stride=G // LANES), :].astype(BF16)
        goal = dot(far, fetched) + near_ref[:, at].astype(F32)
        diff = table_ref[:, at].astype(F32) - goal
        gap = gap + diff * diff
        inputs_ref[:, S + j * LANES : S + (j + 1) * LANES] = goal.astype(BF16)
    reward = -(jnp.sum(gap, axis=1, keepdims=True) * (1.0 / G))
    inputs = inputs_ref[...]

    kept = dot(half_rows(core), inputs, (((1,), (1,)), ((), ())))
    keep_ref[...] = kept.astype(BF16)
    sent = dot(half_rows(1 - core), inputs, (((1,), (1,)), ((), ()))).astype(BF16)
    for b in range(H // ROWS):
        send_ref[ROWS : ROWS + 48, b * ROWS : (b + 1) * ROWS] = sent[b * 48 : (b + 1) * 48, :]

    total_ref[...] = jnp.zeros((ROWS, LANES), F32)

    def product(n, buffer_ref):
        at = pl.ds(pl.multiple_of(n * CHUNK, CHUNK), CHUNK)
        buffer_ref[...] = dot(inputs[:, :S], state_w_ref[:, at]) + dot(
            inputs[:, S:], goal_w_ref[:, at]
        )

    def activate(n, buffer_ref):
        at = pl.ds(pl.multiple_of(n * CHUNK, CHUNK), CHUNK)
        pre = buffer_ref[...] + b_in_ref[:, at]
        sig = 0.5 * jnp.tanh(0.5 * pre) + 0.5
        head = w_out_ref[:, at]
        act = pre * sig
        hidden = act.astype(BF16)
        hidden_ref[:, at] = hidden
        slope_ref[:, at] = head * (sig + act * (1.0 - sig))
        term = hidden.astype(F32) * head
        total_ref[...] += term[:, :LANES] + term[:, LANES:]

    count = H // CHUNK
    load(0).wait()
    product(0, even_ref)

    def forward(m, carry):
        load(2 * m + 1).wait()

        @pl.when(2 * m + 2 < count)
        def _():
            load(2 * m + 2).wait()

        product(2 * m + 1, odd_ref)
        activate(2 * m, even_ref)
        product(jnp.minimum(2 * m + 2, count - 1), even_ref)
        activate(2 * m + 1, odd_ref)
        return carry

    lax.fori_loop(0, count // 2, forward, 0)
    value = jnp.sum(total_ref[...], axis=1, keepdims=True) + b_out_ref[:, 0:1]
    error = value - reward
    grad_value = error * scale

    each = (STEPS * iota((ROWS, ROWS // STEPS), 1)) - iota((ROWS, ROWS // STEPS), 0)
    for s in range(STEPS):
        td_rows_ref[s : s + 1, :] = jnp.sum(
            jnp.where(each + s == 0, error, 0.0), axis=0, keepdims=True
        )

    td_copy = pltpu.make_async_copy(td_rows_ref, td_ref, td_sem)
    td_copy.start()

    total_value = jnp.sum(grad_value, axis=0, keepdims=True)

    def backward(n, carry):
        at = pl.ds(pl.multiple_of(n * CHUNK, CHUNK), CHUNK)
        grad_pre = grad_value * slope_ref[:, at]
        send_ref[:ROWS, at] = grad_pre.astype(BF16)
        first = jnp.sum(grad_pre, axis=0, keepdims=True)
        second = jnp.sum(grad_value * hidden_ref[:, at].astype(F32), axis=0, keepdims=True)
        third = jnp.broadcast_to(total_value, (1, CHUNK))
        rows = stack_rows(three(first) + three(second) + three(third), 16)
        send_ref[ROWS + 48 : ROWS + 64, at] = rows.astype(BF16)
        return carry

    lax.fori_loop(0, H // CHUNK, backward, 0)
    td_copy.wait()


PACK = 424
BLOCK = 88


def product_kernel(own_ref, other_ref, keep_ref, out_ref, left_ref):
    for b in range(H // ROWS):
        left_ref[b * 48 : (b + 1) * 48, :] = other_ref[
            ROWS : ROWS + 48, b * ROWS : (b + 1) * ROWS
        ]
    keep = keep_ref[...]
    left = left_ref[...]
    for n in range(H // CHUNK):
        at = slice(n * CHUNK, (n + 1) * CHUNK)
        part = dot(keep, own_ref[:ROWS, at]) + dot(left, other_ref[:ROWS, at])
        for p in range(N_PLANE):
            for i in range(3):
                tile = part[p * SLAB + 8 * i : p * SLAB + 8 * i + 8]
                pair = jnp.concatenate([tile[:, :LANES], tile[:, LANES:]], axis=0)
                start = p * PACK + (16 * i + 2 * n) * 8
                out_ref[start : start + 16, :] = pair.astype(BF16)
    mine = own_ref[ROWS + 48 : ROWS + 64, :].astype(F32)
    theirs = other_ref[ROWS + 48 : ROWS + 64, :].astype(F32)
    rows = []
    for q in range(3):
        a = mine[3 * q : 3 * q + 1] + mine[3 * q + 1 : 3 * q + 2] + mine[3 * q + 2 : 3 * q + 3]
        b = theirs[3 * q : 3 * q + 1] + theirs[3 * q + 1 : 3 * q + 2] + theirs[3 * q + 2 : 3 * q + 3]
        rows.append(a + b)
    blocks = []
    for r in rows[:2]:
        pieces = [r[:, b * LANES : (b + 1) * LANES] for b in range(H // LANES)]
        blocks.append(jnp.concatenate(pieces, axis=0))
    blocks.append(stack_rows(two(rows[2][:, :LANES]), 8))
    small = jnp.concatenate(blocks, axis=0).astype(BF16)
    for p in range(N_PLANE):
        out_ref[p * PACK + HALF : (p + 1) * PACK, :] = small


def plane_kernel(got_ref, out_ref, sum_ref, wide_ref):
    for b in range(PACK // 8):
        total = got_ref[b * 8 : b * 8 + 8, :].astype(F32)
        for p in range(1, N_PLANE):
            total = total + got_ref[p * PACK + b * 8 : p * PACK + b * 8 + 8, :].astype(F32)
        sum_ref[b * 8 : b * 8 + 8, :] = total
    for n in range(48):
        wide_ref[pl.ds(n, N_LINE, stride=48), :] = sum_ref[8 * n : 8 * n + 8, :]
    last = sum_ref[416:417, :] + sum_ref[417:418, :]
    small = jnp.concatenate(
        (sum_ref[384:416, :], stack_rows(two(last), 8)),
        axis=0,
    ).astype(BF16)
    for z in range(N_LINE):
        out_ref[z * BLOCK : z * BLOCK + 48, :] = wide_ref[z * 48 : z * 48 + 48, :].astype(BF16)
        out_ref[z * BLOCK + 48 : (z + 1) * BLOCK, :] = small


def line_kernel(got_ref, w_ref, b_in_ref, w_out_ref, b_out_ref, sum_ref):
    for b in range(BLOCK // 8):
        total = got_ref[b * 8 : b * 8 + 8, :].astype(F32)
        for z in range(1, N_LINE):
            total = total + got_ref[z * BLOCK + b * 8 : z * BLOCK + b * 8 + 8, :].astype(F32)
        sum_ref[b * 8 : b * 8 + 8, :] = total
    for i in range(3):
        for b in range(H // LANES):
            w_ref[i : i + 1, b * LANES : (b + 1) * LANES] = sum_ref[i * 16 + b : i * 16 + b + 1, :]
    b_in_ref[...] = sum_ref[48:64, :]
    w_out_ref[...] = sum_ref[64:80, :]
    b_out_ref[...] = sum_ref[80:81, :] + sum_ref[81:82, :]


def call(kernel, shapes, operands, scratch, flops, grant, in_hbm=(), out_hbm=()):
    specs = [pl.BlockSpec(memory_space=pltpu.VMEM)] * len(operands)
    for n in in_hbm:
        specs[n] = pl.BlockSpec(memory_space=pltpu.HBM)
    back = [pl.BlockSpec(memory_space=pltpu.VMEM)] * len(shapes)
    for n in out_hbm:
        back[n] = pl.BlockSpec(memory_space=pltpu.HBM)
    outs = [jax.ShapeDtypeStruct(shape, kind) for shape, kind in shapes]
    return pl.pallas_call(
        kernel,
        out_shape=outs,
        in_specs=specs,
        out_specs=back,
        scratch_shapes=scratch,
        compiler_params=pltpu.CompilerParams(vmem_limit_bytes=grant << 20),
        cost_estimate=pl.CostEstimate(flops=flops, bytes_accessed=1 << 20, transcendentals=0),
    )(*operands)


def body(state_feats, achieved, offsets, w_in, b_in, w_out, b_out):
    place = jnp.stack([lax.axis_index(TM), lax.axis_index("dp")]).astype(I32)
    place = jnp.broadcast_to(place[:, None], (2, LANES))
    table = achieved.reshape(ROWS, G)
    state = state_feats.reshape(ROWS, S)
    many, offs = call(
        spread_kernel,
        [((N_TM, 1, ROWS), I32), ((1, ROWS), I32)],
        (offsets.T,),
        [],
        10**6,
        60,
    )
    known = lax.all_to_all(many, TM, split_axis=0, concat_axis=0, tiled=True)
    (picked,) = call(
        pick_kernel,
        [((N_TM * 16, LANES), BF16)],
        (place, known, table),
        [
            pltpu.VMEM((N_TM * 16 + 16, LANES), F32),
            pltpu.VMEM((N_TM * 16, LANES), BF16),
            pltpu.SemaphoreType.DMA((4,)),
        ],
        10**8,
        8,
        (),
        (0,),
    )
    goal_w, near, at = call(
        ahead_kernel,
        [((G, H), BF16), ((ROWS, G), BF16), ((ROWS, LANES), I32)],
        (place, offs, table, w_in),
        [],
        10**9,
        12,
    )
    fetched = lax.all_to_all(
        picked.reshape(N_TM, 16, LANES), TM, split_axis=0, concat_axis=0, tiled=True
    ).reshape(N_TM * 16, LANES)
    head_bias = jnp.broadcast_to(b_out[None], (1, LANES))
    scale = 1.0 / math.sqrt(ROWS * N_TM * 2)
    td, send, keep = call(
        functools.partial(main_kernel, scale),
        [((STEPS, ROWS // STEPS), F32), ((ROWS + 64, H), BF16), ((HALF, ROWS), BF16)],
        (
            place,
            head_bias,
            fetched,
            goal_w,
            near,
            at,
            table,
            state,
            w_in,
            b_in.reshape(1, H),
            w_out.reshape(1, H),
        ),
        [
            pltpu.VMEM((ROWS, H), F32),
            pltpu.VMEM((ROWS, H), BF16),
            pltpu.VMEM((ROWS, S + G), BF16),
            pltpu.VMEM((S, H), BF16),
            pltpu.VMEM((N_TM * 16 + 16, LANES), F32),
            pltpu.VMEM((ROWS, LANES), F32),
            pltpu.VMEM((STEPS, ROWS // STEPS), F32),
            pltpu.VMEM((ROWS, CHUNK), F32),
            pltpu.VMEM((ROWS, CHUNK), F32),
            pltpu.SemaphoreType.DMA((H // CHUNK,)),
            pltpu.SemaphoreType.DMA,
        ],
        2 * 10**9,
        48,
        (8,),
        (0,),
    )
    other = lax.ppermute(send, "dp", [(0, 1), (1, 0)])
    (packs,) = call(
        product_kernel,
        [((N_PLANE * PACK, LANES), BF16)],
        (send, other, keep),
        [pltpu.VMEM((HALF, ROWS), BF16)],
        10**9,
        12,
    )
    got = lax.all_to_all(
        packs.reshape(N_PLANE, PACK, LANES), PLANE, split_axis=0, concat_axis=0, tiled=True
    ).reshape(N_PLANE * PACK, LANES)
    (lines,) = call(
        plane_kernel,
        [((N_LINE * BLOCK, LANES), BF16)],
        (got,),
        [pltpu.VMEM((PACK, LANES), F32), pltpu.VMEM((N_LINE * 48 + 48, LANES), F32)],
        10**7,
        6,
    )
    got = lax.all_to_all(
        lines.reshape(N_LINE, BLOCK, LANES), LINE, split_axis=0, concat_axis=0, tiled=True
    ).reshape(N_LINE * BLOCK, LANES)
    grad_w_in, grad_b_in, grad_w_out, grad_b_out = call(
        line_kernel,
        [((3, H), F32), ((16, LANES), F32), ((16, LANES), F32), ((1, LANES), F32)],
        (got,),
        [pltpu.VMEM((BLOCK, LANES), F32)],
        10**6,
        4,
    )
    return td.T, grad_w_in, grad_b_in.reshape(H), grad_w_out.reshape(H), grad_b_out[0, :1]


def solution(mesh):
    split = Mesh(mesh.devices.reshape(4, 4, 8, mesh.shape["dp"]), TM_DP)
    placed = (P("dp", TM, None), P("dp", TM, None), P("dp", TM), P(), P(), P(), P())
    return jax.shard_map(
        body,
        mesh=split,
        in_specs=placed,
        out_specs=(P("dp", TM), P(TM_DP, None), P(), P(), P()),
        check_vma=False,
    )
```
